32 devices in a mesh: dp: 1 (over z), tp: 4 (over y), sp: 8 (over x, core).
Axes of the slice: x: 4, y: 4, z: 1, core: 2. Of those that a mesh axis runs over, the one named last changes fastest.
The devices are a block of a 4x4x8 slice.
Arguments:
- hidden: bfloat16 [64, 8192], P('dp')
- norm_scale: bfloat16 [8192], replicated
- w_qkv: bfloat16 [8192, 10240], P(None, 'tp')
- w_out: bfloat16 [8192, 8192], P('tp')
- k_cache: bfloat16 [64, 1024, 8, 128], P('dp', 'sp', 'tp')
- v_cache: bfloat16 [64, 1024, 8, 128], P('dp', 'sp', 'tp')
- positions: int32 [64], P('dp')
Outputs:
- output 1: bfloat16 [64, 8192], P('dp')
- output 2: bfloat16 [64, 1024, 8, 128], P('dp', 'sp', 'tp')
- output 3: bfloat16 [64, 1024, 8, 128], P('dp', 'sp', 'tp')
All inputs are finite; a program needn't handle non-finite values.
Results may differ from the reference program's by a relative error of at most 0.00668127.
Values sent between devices are 32-bit elements.
A program may use at most 768 MiB of HBM per device.

```python
import math
import jax
import jax.numpy as jnp
from jax import lax

BATCH = 64
SEQ = 1024
D = 8192
HEADS = 64
KV_HEADS = 8
HEAD = 128


def rope_apply(head_vals, positions):
    half_dim = head_vals.shape[-1] // 2
    inv_freq = jnp.exp(jnp.arange(half_dim, dtype=jnp.float32) * (-2.0 * math.log(500000.0) / head_vals.shape[-1]))
    angles = positions.astype(jnp.float32)[:, None] * inv_freq[None, :]
    cos_part = jnp.cos(angles)[:, None, None, :]
    sin_part = jnp.sin(angles)[:, None, None, :]
    first_half = head_vals[..., :half_dim]
    second_half = head_vals[..., half_dim:]
    return jnp.concatenate([first_half * cos_part - second_half * sin_part, second_half * cos_part + first_half * sin_part], axis=-1)


def setup_inputs(seed: int = 0, part: int = 0) -> dict:
    part_keys = jax.random.split(jax.random.fold_in(jax.random.key(seed), part), 5)
    shared_keys = jax.random.split(jax.random.key(seed + 1), 4)
    qkv_width = (HEADS + 2 * KV_HEADS) * HEAD
    hidden = jax.random.normal(part_keys[0], (BATCH, D), jnp.float32)
    norm_scale = 1.0 + 0.5 * jax.random.normal(shared_keys[0], (D,), jnp.float32)
    col_boost = jnp.where(jax.random.randint(shared_keys[1], (qkv_width,), 0, 16) == 0, 10.0, 1.0)
    w_qkv = jax.random.normal(shared_keys[2], (D, qkv_width), jnp.float32) * col_boost * (D ** -0.5)
    w_out = jax.random.normal(shared_keys[3], (HEADS * HEAD, D), jnp.float32) * (2.0 * (HEADS * HEAD) ** -0.5)
    k_cache = 0.5 * jax.random.normal(part_keys[1], (BATCH, SEQ, KV_HEADS, HEAD), jnp.float32)
    coarse = jax.random.normal(part_keys[2], (BATCH, 8, 1, KV_HEADS, HEAD), jnp.float32)
    fine_part = jax.random.normal(part_keys[3], (BATCH, 8, SEQ // 8, KV_HEADS, HEAD), jnp.float32)
    v_cache = (coarse + 0.5 * fine_part).reshape(BATCH, SEQ, KV_HEADS, HEAD)
    positions = jax.random.randint(part_keys[4], (BATCH,), SEQ // 8, SEQ)
    positions = positions.at[0].set(SEQ - 1).at[1].set(SEQ // 8)
    return {
        'hidden': hidden.astype(jnp.bfloat16),
        'norm_scale': norm_scale.astype(jnp.bfloat16),
        'w_qkv': w_qkv.astype(jnp.bfloat16),
        'w_out': w_out.astype(jnp.bfloat16),
        'k_cache': k_cache.astype(jnp.bfloat16),
        'v_cache': v_cache.astype(jnp.bfloat16),
        'positions': positions.astype(jnp.int32),
    }


def reference(hidden, norm_scale, w_qkv, w_out, k_cache, v_cache, positions):
    q_per_kv = HEADS // KV_HEADS
    hidden_f32 = hidden.astype(jnp.float32)
    row_mean = jnp.mean(hidden_f32, axis=-1, keepdims=True)
    centered = hidden_f32 - row_mean
    row_var = jnp.mean(centered * centered, axis=-1, keepdims=True)
    normed = (centered * lax.rsqrt(row_var + 1e-5) * norm_scale.astype(jnp.float32)).astype(jnp.bfloat16)
    qkv_proj = jnp.clip(jnp.dot(normed, w_qkv, preferred_element_type=jnp.float32).astype(jnp.bfloat16), -8.0, 8.0)
    grouped = qkv_proj.reshape(BATCH, KV_HEADS, q_per_kv + 2, HEAD)
    rotated = rope_apply(grouped[:, :, : q_per_kv + 1].astype(jnp.float32), positions).astype(jnp.bfloat16)
    queries = rotated[:, :, :q_per_kv]
    new_row = (jnp.arange(SEQ)[None, :] == positions[:, None])[:, :, None, None]
    k_upd = jnp.where(new_row, rotated[:, :, q_per_kv][:, None], k_cache)
    v_upd = jnp.where(new_row, grouped[:, :, q_per_kv + 1][:, None], v_cache)

    def one_sequence(seq_args):
        q_seq, k_seq, v_seq, p_seq = seq_args
        scores = jnp.einsum('gqd,sgd->gqs', q_seq.astype(jnp.float32), k_seq.astype(jnp.float32)) * (HEAD ** -0.5)
        valid_mask = jnp.arange(SEQ) <= p_seq
        scores = jnp.where(valid_mask[None, None, :], scores, -jnp.inf)
        weights_bf = jax.nn.softmax(scores, axis=-1).astype(jnp.bfloat16)
        return jnp.einsum('gqs,sgd->gqd', weights_bf.astype(jnp.float32), v_seq.astype(jnp.float32))

    attn_out = lax.map(one_sequence, (queries, k_upd, v_upd, positions))
    attn_flat = attn_out.reshape(BATCH, HEADS * HEAD).astype(jnp.bfloat16)
    h_out = (hidden_f32 + jnp.dot(attn_flat, w_out, preferred_element_type=jnp.float32)).astype(jnp.bfloat16)
    return (h_out, k_upd, v_upd)
```

```python
import functools
import math

import jax
import jax.numpy as jnp
from jax import lax
from jax.experimental import pallas as pl
from jax.experimental.pallas import tpu as pltpu
from jax.sharding import PartitionSpec as P

MESH = pl.DeviceIdType.MESH
F32 = jnp.float32
BF16 = jnp.bfloat16
ANY = pl.BlockSpec(memory_space=pl.ANY)
VMEM = pl.BlockSpec(memory_space=pltpu.VMEM)
SMEM = pl.BlockSpec(memory_space=pltpu.SMEM)
CORES = 2
VMEM_LIMIT = 60 * 1024 * 1024


def ds(start, size, align):
    return pl.ds(pl.multiple_of(start, align), size)


def rcopy(src, dst, send_sem, recv_sem, **where):
    return pltpu.make_async_remote_copy(
        src_ref=src, dst_ref=dst, send_sem=send_sem, recv_sem=recv_sem,
        device_id=where, device_id_type=MESH,
    )


def qkv_kernel(dims, h_ref, scale_ref, pos_ref, w_ref, out_ref, wbuf, u_ref, acc, mine, wsem, send_sem, recv_sem):
    n_seq, d_model = h_ref.shape
    q_per_kv, head = dims
    n_blk, blk, cols = wbuf.shape
    s = lax.axis_index('sp')
    core = lax.rem(s, CORES)
    partner = s + 1 - 2 * core

    def wcopy(i):
        return pltpu.make_async_copy(
            w_ref.at[ds(i * blk, blk, blk), ds(core * cols, cols, 128)], wbuf.at[i], wsem.at[i])

    for i in range(n_blk):
        wcopy(i).start()
    barrier = pltpu.get_barrier_semaphore()
    pl.semaphore_signal(barrier, inc=1, device_id={'sp': partner}, device_id_type=MESH)

    lanes = 128
    zero = jnp.zeros((n_seq, lanes), F32)

    def add_sum(i, tot):
        return tot + h_ref[:, ds(i * lanes, lanes, lanes)].astype(F32)

    mean = jnp.sum(lax.fori_loop(0, d_model // lanes, add_sum, zero, unroll=8), axis=1, keepdims=True) / d_model

    def add_sq(i, tot):
        cent = h_ref[:, ds(i * lanes, lanes, lanes)].astype(F32) - mean
        return tot + cent * cent

    var = jnp.sum(lax.fori_loop(0, d_model // lanes, add_sq, zero, unroll=8), axis=1, keepdims=True) / d_model
    inv = lax.rsqrt(var + 1e-5)

    def norm(i, carry):
        cut = ds(i * lanes, lanes, lanes)
        cent = h_ref[:, cut].astype(F32) - mean
        u_ref[:, cut] = (cent * inv * scale_ref[:, cut].astype(F32)).astype(BF16)
        return carry

    lax.fori_loop(0, d_model // lanes, norm, 0, unroll=8)

    eye = lax.broadcasted_iota(jnp.int32, (n_seq, n_seq), 0) == lax.broadcasted_iota(jnp.int32, (n_seq, n_seq), 1)
    pos_col = jnp.sum(jnp.where(eye, pos_ref[...].astype(F32), 0.0), axis=1, keepdims=True)
    lane = lax.broadcasted_iota(jnp.int32, (n_seq, head), 1)
    half = head // 2
    inv_freq = jnp.exp(lax.rem(lane, half).astype(F32) * (-2.0 * math.log(500000.0) / head))
    angle = pos_col * inv_freq
    cos_t = jnp.cos(angle)
    sin_t = jnp.where(lane < half, -jnp.sin(angle), jnp.sin(angle))

    acc[...] = jnp.zeros_like(acc)

    def mm(i, carry):
        wcopy(i).wait()
        acc[...] += jnp.dot(u_ref[:, ds(i * blk, blk, blk)], wbuf[i], preferred_element_type=F32)
        return carry

    lax.fori_loop(0, n_blk, mm, 0)

    for j in range(q_per_kv + 2):
        val = jnp.clip(acc[:, j * head:(j + 1) * head].astype(BF16), -8.0, 8.0).astype(F32)
        if j < q_per_kv + 1:
            val = (val * cos_t + pltpu.roll(val, half, 1) * sin_t).astype(BF16).astype(F32)
        if j < q_per_kv:
            mine[pl.ds(j, n_seq, stride=q_per_kv), :] = val
        else:
            mine[pl.ds((j * n_seq), n_seq), :] = val
    pl.semaphore_wait(barrier, 1)
    give = rcopy(mine, out_ref.at[core], send_sem, recv_sem, sp=partner)
    give.start()
    out_ref[core] = mine[...]
    give.wait()


def attn_kernel(dims, pos_ref, qkv_ref, k_ref, v_ref, o_ref, ko_ref, vo_ref, kbuf, vbuf, isem, osem):
    q_per_kv, head = dims
    n_seq, rows2, _ = kbuf.shape
    n_grp = rows2 // qkv_ref.shape[0]
    groups = qkv_ref.shape[0]
    n_ch = o_ref.shape[0]
    per = n_seq // n_ch
    heads = groups * q_per_kv
    base = lax.axis_index('sp') * n_grp

    def cin(i, which):
        src, dst = ((k_ref, kbuf), (v_ref, vbuf))[which]
        return pltpu.make_async_copy(src.at[pl.ds(i * per, per)], dst.at[pl.ds(i * per, per)], isem.at[which, i])

    def cout(i, which):
        src, dst = ((kbuf, ko_ref), (vbuf, vo_ref))[which]
        return pltpu.make_async_copy(src.at[pl.ds(i * per, per)], dst.at[pl.ds(i * per, per)], osem.at[which, i])

    for i in range(n_ch):
        cin(i, 0).start()
        cin(i, 1).start()

    colj = lax.broadcasted_iota(jnp.int32, (heads, rows2), 1)
    rown = lax.broadcasted_iota(jnp.int32, (heads, rows2), 0)
    same = lax.rem(colj, groups) == rown // q_per_kv
    tile = 8 * groups
    trow = lax.broadcasted_iota(jnp.int32, (tile, head), 0)
    n_rows = per * heads
    eye = lax.broadcasted_iota(jnp.int32, (n_rows, n_rows), 0) == lax.broadcasted_iota(jnp.int32, (n_rows, n_rows), 1)
    q_rows = n_seq * q_per_kv

    def step(i, carry):
        cin(i, 0).wait()
        cin(i, 1).wait()
        scores = []
        for t in range(per):
            b = i * per + t
            rel = pos_ref[b] - base
            here = jnp.logical_and(rel >= 0, rel < n_grp)
            at = jnp.clip(rel, 0, n_grp - 1)
            start = (at // 8) * tile
            hit = jnp.logical_and(trow // groups == at % 8, here)
            for buf, off in ((kbuf, q_rows), (vbuf, q_rows + n_seq)):
                cut = ds(start, tile, tile)
                new = qkv_ref[0, pl.ds(off + b, 1), :]
                for g in range(1, groups):
                    new = jnp.where(trow % groups == g, qkv_ref[g, pl.ds(off + b, 1), :], new)
                buf[b, cut, :] = jnp.where(hit, new, buf[b, cut, :].astype(F32)).astype(BF16)
            q = jnp.concatenate([qkv_ref[g, ds(b * q_per_kv, q_per_kv, 8), :] for g in range(groups)], axis=0)
            sc = lax.dot_general(q.astype(BF16), kbuf[b], (((1,), (1,)), ((), ())), preferred_element_type=F32)
            ok = jnp.logical_and(same, colj < groups * (rel + 1))
            scores.append(jnp.where(ok, sc * (head ** -0.5), -1e30))
        sc = jnp.concatenate(scores, axis=0)
        top = jnp.max(sc, axis=1, keepdims=True)
        wt = jnp.exp(sc - top)
        tot = jnp.sum(wt, axis=1, keepdims=True)
        wt = wt.astype(BF16)
        for t in range(per):
            o_ref[i, t * heads:(t + 1) * heads, :] = jnp.dot(
                wt[t * heads:(t + 1) * heads], vbuf[i * per + t], preferred_element_type=F32)
        top_row = jnp.sum(jnp.where(eye, top, 0.0), axis=0, keepdims=True)
        tot_row = jnp.sum(jnp.where(eye, tot, 0.0), axis=0, keepdims=True)
        pad = jnp.zeros((6, n_rows), F32)
        o_ref[i, n_rows:n_rows + 8, :] = jnp.concatenate([top_row, tot_row, pad], axis=0)
        cout(i, 0).start()
        cout(i, 1).start()
        return carry

    lax.fori_loop(0, n_ch, step, 0)
    for i in range(n_ch):
        cout(i, 0).wait()
        cout(i, 1).wait()


def out_kernel(dims, o_ref, h_ref, w_ref, out_ref, rbuf, abuf, attn, lhs, wbuf, pbuf, ybuf, hbuf,
               wsem, hsem, rs_s, rs_r, ab_s, ab_r, y_s, y_r, a_s, a_r, b_s, b_r, d_s, d_r):
    n_tp, n_sp, heads = dims
    nx = n_sp // CORES
    y = lax.axis_index('tp')
    s = lax.axis_index('sp')
    core = lax.rem(s, CORES)
    x = s // CORES
    partner = s + 1 - 2 * core
    _, n_rows, head = attn.shape
    per = n_rows // heads
    depth, cols = wbuf.shape[1:]
    seqs = CORES * per

    def yat(d):
        return lax.rem(y + d, n_tp)

    def xat(d):
        return lax.rem(x + d, nx) * CORES + core

    def wcopy(j):
        return pltpu.make_async_copy(
            w_ref.at[:, ds((core * n_tp + yat(j)) * cols, cols, cols)], wbuf.at[j], wsem.at[j])

    hcopy = pltpu.make_async_copy(
        h_ref.at[ds(x * seqs, seqs, seqs), ds((core * n_tp + y) * cols, cols, cols)], hbuf, hsem)
    order = [d for d in range(1, n_tp)] + [0]
    for j in order:
        wcopy(j).start()
    hcopy.start()

    barrier = pltpu.get_barrier_semaphore()
    for d in range(1, n_sp):
        pl.semaphore_signal(barrier, inc=1, device_id={'sp': lax.rem(s + d, n_sp)}, device_id_type=MESH)
    for d in range(1, n_tp):
        pl.semaphore_signal(barrier, inc=1, device_id={'tp': yat(d)}, device_id_type=MESH)
    pl.semaphore_wait(barrier, n_sp + n_tp - 2)

    def rs(d):
        to = lax.rem(s + d, n_sp)
        return rcopy(o_ref.at[to], rbuf.at[d], rs_s.at[d], rs_r.at[d], sp=to)

    for d in range(1, n_sp):
        rs(d).start()
    parts = [o_ref.at[s]]
    for d in range(1, n_sp):
        rs(d).wait_recv()
        parts.append(rbuf.at[d])
    tops = [p[n_rows:n_rows + 1, :] for p in parts]
    sums = [p[n_rows + 1:n_rows + 2, :] for p in parts]
    top = functools.reduce(jnp.maximum, tops)
    facs = [jnp.exp(t - top) for t in tops]
    tot = functools.reduce(jnp.add, [f * l for f, l in zip(facs, sums)])
    fac = jnp.concatenate([f / tot for f in facs], axis=0)
    pad = jnp.zeros((n_rows - n_sp, n_rows), F32)
    fac = jnp.transpose(jnp.concatenate([fac, pad], axis=0))
    val = parts[0][0:n_rows, :] * fac[:, 0:1]
    for j in range(1, n_sp):
        val = val + parts[j][0:n_rows, :] * fac[:, j:j + 1]
    attn[0] = val

    swap = rcopy(attn.at[0], abuf.at[core], ab_s, ab_r, sp=partner)
    swap.start()
    abuf[core] = val
    swap.wait()
    flat = abuf.reshape(CORES * n_rows, head)
    for n in range(heads):
        lhs[:, n * head:(n + 1) * head] = flat[pl.ds(n, seqs, stride=heads), :].astype(BF16)

    def ysend(d):
        return rcopy(pbuf.at[d], ybuf.at[d], y_s.at[d], y_r.at[d], tp=yat(d))

    def proj(j):
        wcopy(j).wait()
        pbuf[j] = jnp.dot(lhs[...], wbuf[j], preferred_element_type=F32)

    for j in order:
        proj(j)
        if j:
            ysend(j).start()
    hcopy.wait()
    tot = pbuf[0]
    for d in range(1, n_tp):
        ysend(d).wait_recv()
        tot = tot + ybuf[d]
    out_ref[ds(x * seqs, seqs, seqs), ds((core * n_tp + y) * cols, cols, cols)] = hbuf[...].astype(F32) + tot

    def block(dy, dx, part):
        by = lax.rem(y + n_tp - dy, n_tp)
        bx = lax.rem(x + nx - dx, nx)
        return out_ref.at[ds(bx * seqs + part * per, per, per), ds((core * n_tp + by) * cols, cols, cols)]

    sends = []

    def go(dy, dx, part, sems, where, ty, tx):
        ref = block(dy, dx, part)
        cp = rcopy(ref, ref, sems[0].at[ty, tx], sems[1].at[ty, tx], **where)
        cp.start()
        sends.append(cp)

    def fwd(dy, dx, part):
        if part == 0 and dx == 0:
            for e in range(1, nx):
                go(dy, 0, 0, (a_s, a_r), {'sp': xat(e)}, dy, e)
        if part == 1 and dy == 0:
            for e in range(1, n_tp):
                go(0, dx, 1, (b_s, b_r), {'tp': yat(e)}, e, dx)
        ref = block(dy, dx, part)
        cp = rcopy(ref, ref, d_s.at[part, dy, dx], d_r.at[part, dy, dx], sp=partner)
        cp.start()
        sends.append(cp)

    for e in range(1, n_tp):
        go(0, 0, 0, (a_s, a_r), {'tp': yat(e)}, e, 0)
    for e in range(1, nx):
        go(0, 0, 1, (b_s, b_r), {'sp': xat(e)}, 0, e)
    fwd(0, 0, 0)
    fwd(0, 0, 1)

    def arrive(dy, dx, part):
        ref = block(dy, dx, part)
        r = (a_r, b_r)[part].at[dy, dx]
        q = (a_s, b_s)[part].at[dy, dx]
        rcopy(ref, ref, q, r, sp=partner).wait_recv()
        fwd(dy, dx, part)

    for e in range(1, max(n_tp, nx)):
        if e < n_tp:
            arrive(e, 0, 0)
        if e < nx:
            arrive(0, e, 1)
    for dy in range(n_tp):
        for e in range(1, nx):
            arrive(dy, e, 0)
    for dx in range(nx):
        for e in range(1, n_tp):
            arrive(e, dx, 1)
    for part in range(2):
        for dy in range(n_tp):
            for dx in range(nx):
                by = lax.rem(y + n_tp - dy, n_tp)
                bx = lax.rem(x + nx - dx, nx)
                ref = out_ref.at[ds(bx * seqs + part * per, per, per),
                                 ds(((1 - core) * n_tp + by) * cols, cols, cols)]
                rcopy(ref, ref, d_s.at[part, dy, dx], d_r.at[part, dy, dx], sp=partner).wait_recv()
    for cp in sends:
        cp.wait_send()
    for d in range(1, n_sp):
        rs(d).wait_send()
    for d in range(1, n_tp):
        ysend(d).wait_send()


def solution(mesh):
    n_tp, n_sp = mesh.shape['tp'], mesh.shape['sp']
    cache_spec = P('dp', 'sp', 'tp', None)
    DMA = pltpu.SemaphoreType.DMA

    def local_step(hidden, norm_scale, w_qkv, w_out, k_cache, v_cache, positions):
        n_seq, seq_local, kv_local, head = k_cache.shape
        d_model = hidden.shape[1]
        q_per_kv = w_qkv.shape[1] // (kv_local * head) - 2
        heads = kv_local * q_per_kv
        grp_cols = (q_per_kv + 2) * head
        n_blk = 8
        blk = d_model // n_blk
        per = n_seq // n_sp
        n_rows = per * heads

        qkv = pl.pallas_call(
            functools.partial(qkv_kernel, (q_per_kv, head)),
            out_shape=jax.ShapeDtypeStruct((kv_local, n_seq * (q_per_kv + 2), head), F32),
            in_specs=[VMEM, VMEM, VMEM, ANY],
            out_specs=VMEM,
            scratch_shapes=[
                pltpu.VMEM((n_blk, blk, grp_cols), BF16),
                pltpu.VMEM((n_seq, d_model), BF16),
                pltpu.VMEM((n_seq, grp_cols), F32),
                pltpu.VMEM((n_seq * (q_per_kv + 2), head), F32),
                DMA((n_blk,)), DMA, DMA,
            ],
            compiler_params=pltpu.CompilerParams(
                collective_id=0, has_side_effects=True, vmem_limit_bytes=VMEM_LIMIT),
            name='qkv',
        )(hidden, norm_scale.reshape(1, d_model), positions.reshape(1, n_seq), w_qkv)

        flat = (n_seq, seq_local * kv_local, head)
        cache_out = jax.ShapeDtypeStruct(flat, BF16)
        part, k_out, v_out = pl.pallas_call(
            functools.partial(attn_kernel, (q_per_kv, head)),
            out_shape=(jax.ShapeDtypeStruct((n_sp, n_rows + 8, head), F32), cache_out, cache_out),
            in_specs=[SMEM, VMEM, ANY, ANY],
            out_specs=(VMEM, ANY, ANY),
            scratch_shapes=[
                pltpu.VMEM(flat, BF16), pltpu.VMEM(flat, BF16),
                DMA((2, n_sp)), DMA((2, n_sp)),
            ],
            compiler_params=pltpu.CompilerParams(vmem_limit_bytes=VMEM_LIMIT),
            name='attn',
        )(positions, qkv, k_cache.reshape(flat), v_cache.reshape(flat))

        nx = n_sp // CORES
        cols = d_model // (CORES * n_tp)
        depth = w_out.shape[0]
        h_out = pl.pallas_call(
            functools.partial(out_kernel, (n_tp, n_sp, heads)),
            out_shape=jax.ShapeDtypeStruct((n_seq, d_model), F32),
            in_specs=[VMEM, ANY, ANY],
            out_specs=VMEM,
            scratch_shapes=[
                pltpu.VMEM((n_sp, n_rows + 8, head), F32),
                pltpu.VMEM((CORES, n_rows, head), F32),
                pltpu.VMEM((1, n_rows, head), F32),
                pltpu.VMEM((CORES * per, depth), BF16),
                pltpu.VMEM((n_tp, depth, cols), BF16),
                pltpu.VMEM((n_tp, CORES * per, cols), F32),
                pltpu.VMEM((n_tp, CORES * per, cols), F32),
                pltpu.VMEM((CORES * per, cols), BF16),
                DMA((n_tp,)), DMA,
                DMA((n_sp,)), DMA((n_sp,)), DMA, DMA, DMA((n_tp,)), DMA((n_tp,)),
                DMA((n_tp, nx)), DMA((n_tp, nx)), DMA((n_tp, nx)), DMA((n_tp, nx)),
                DMA((2, n_tp, nx)), DMA((2, n_tp, nx)),
            ],
            compiler_params=pltpu.CompilerParams(
                collective_id=1, has_side_effects=True, vmem_limit_bytes=VMEM_LIMIT),
            name='outproj',
        )(part, hidden, w_out)
        return h_out.astype(BF16), k_out.reshape(k_cache.shape), v_out.reshape(v_cache.shape)

    return jax.shard_map(
        local_step,
        mesh=mesh,
        in_specs=(P('dp', None), P(None), P(None, 'tp'), P('tp', None), cache_spec, cache_spec, P('dp')),
        out_specs=(P('dp', None), cache_spec, cache_spec),
        check_vma=False,
    )
```

```python
import functools
import math

import jax
import jax.numpy as jnp
from jax import lax
from jax.experimental import pallas as pl
from jax.experimental.pallas import tpu as pltpu
from jax.sharding import PartitionSpec as P

MESH = pl.DeviceIdType.MESH
F32 = jnp.float32
BF16 = jnp.bfloat16
HBM = pl.BlockSpec(memory_space=pltpu.HBM)
VMEM = pl.BlockSpec(memory_space=pltpu.VMEM)
SMEM = pl.BlockSpec(memory_space=pltpu.SMEM)
CORES = 2
MIB = 1024 * 1024


def in_vmem(val):
    return pltpu.with_memory_space_constraint(val, pltpu.VMEM)


def in_hbm(val):
    return pltpu.with_memory_space_constraint(val, pltpu.HBM)


def ds(start, size, align):
    return pl.ds(pl.multiple_of(start, align), size)


def rcopy(src, dst, send_sem, recv_sem, **where):
    return pltpu.make_async_remote_copy(
        src_ref=src, dst_ref=dst, send_sem=send_sem, recv_sem=recv_sem,
        device_id=where, device_id_type=MESH,
    )


def qkv_kernel(dims, h_hbm, scale_hbm, pos_hbm, w_ref, out_ref, h_ref, scale_ref, pos_ref, wbuf, u_ref, acc, mine,
               gain, hsem, wsem, send_sem, recv_sem):
    n_seq, d_model = h_ref.shape
    q_per_kv, head = dims
    n_blk, blk, cols = wbuf.shape
    s = lax.axis_index('sp')
    core = lax.rem(s, CORES)
    partner = s + 1 - 2 * core

    def wcopy(i):
        return pltpu.make_async_copy(
            w_ref.at[ds(i * blk, blk, blk), ds(core * cols, cols, 128)], wbuf.at[i], wsem.at[i])

    loads = [
        pltpu.make_async_copy(src, dst, hsem.at[i])
        for i, (src, dst) in enumerate(((h_hbm, h_ref), (scale_hbm, scale_ref), (pos_hbm, pos_ref)))
    ]
    for load in loads:
        load.start()
    for i in range(n_blk):
        wcopy(i).start()
    barrier = pltpu.get_barrier_semaphore()
    pl.semaphore_signal(barrier, inc=1, device_id={'sp': partner}, device_id_type=MESH)

    for load in loads:
        load.wait()

    lanes = 128
    zero = jnp.zeros((n_seq, lanes), F32)

    def add_sum(i, tot):
        return tot + h_ref[:, ds(i * lanes, lanes, lanes)].astype(F32)

    mean = jnp.sum(lax.fori_loop(0, d_model // lanes, add_sum, zero, unroll=8), axis=1, keepdims=True) / d_model

    def add_sq(i, tot):
        cent = h_ref[:, ds(i * lanes, lanes, lanes)].astype(F32) - mean
        return tot + cent * cent

    var = jnp.sum(lax.fori_loop(0, d_model // lanes, add_sq, zero, unroll=8), axis=1, keepdims=True) / d_model
    inv = lax.rsqrt(var + 1e-5)

    gain[...] = scale_ref[...].astype(F32)

    def norm(i, carry):
        cut = ds(i * lanes, lanes, lanes)
        cent = h_ref[:, cut].astype(F32) - mean
        u_ref[:, cut] = (cent * inv * gain[pl.ds(i, 1), :]).astype(BF16)
        return carry

    lax.fori_loop(0, d_model // lanes, norm, 0, unroll=8)

    eye = lax.broadcasted_iota(jnp.int32, (n_seq, n_seq), 0) == lax.broadcasted_iota(jnp.int32, (n_seq, n_seq), 1)
    pos_col = jnp.sum(jnp.where(eye, pos_ref[...].astype(F32), 0.0), axis=1, keepdims=True)
    lane = lax.broadcasted_iota(jnp.int32, (n_seq, head), 1)
    half = head // 2
    inv_freq = jnp.exp(lax.rem(lane, half).astype(F32) * (-2.0 * math.log(500000.0) / head))
    angle = pos_col * inv_freq
    cos_t = jnp.cos(angle)
    sin_t = jnp.where(lane < half, -jnp.sin(angle), jnp.sin(angle))

    acc[...] = jnp.zeros_like(acc)

    def mm(i, carry):
        wcopy(i).wait()
        acc[...] += jnp.dot(u_ref[:, ds(i * blk, blk, blk)], wbuf[i], preferred_element_type=F32)
        return carry

    lax.fori_loop(0, n_blk, mm, 0)

    for j in range(q_per_kv + 2):
        val = jnp.clip(acc[:, j * head:(j + 1) * head].astype(BF16), -8.0, 8.0).astype(F32)
        if j < q_per_kv + 1:
            val = (val * cos_t + pltpu.roll(val, half, 1) * sin_t).astype(BF16).astype(F32)
        if j < q_per_kv:
            mine[pl.ds(j, n_seq, stride=q_per_kv), :] = val
        else:
            mine[pl.ds((j * n_seq), n_seq), :] = val
    pl.semaphore_wait(barrier, 1)
    give = rcopy(mine, out_ref.at[core], send_sem, recv_sem, sp=partner)
    give.start()
    out_ref[core] = mine[...]
    give.wait()


def attn_kernel(dims, pos_ref, qkv_ref, k_ref, v_ref, o_ref, ko_ref, vo_ref, kp, vp, osem, psem):
    q_per_kv, head = dims
    n_seq, rows2, _ = k_ref.shape
    groups = qkv_ref.shape[0]
    n_grp = rows2 // groups
    n_ch = o_ref.shape[0]
    per = n_seq // n_ch
    heads = groups * q_per_kv
    base = lax.axis_index('sp') * n_grp
    tile = 8 * groups
    pairs = ((k_ref, ko_ref, kp), (v_ref, vo_ref, vp))

    def bulk(i, which):
        src, dst, _ = pairs[which]
        cut = pl.ds(i * per, per)
        return pltpu.make_async_copy(src.at[cut], dst.at[cut], osem.at[which, i])

    for i in range(n_ch):
        bulk(i, 0).start()
        bulk(i, 1).start()

    colj = lax.broadcasted_iota(jnp.int32, (heads, rows2), 1)
    rown = lax.broadcasted_iota(jnp.int32, (heads, rows2), 0)
    same = lax.rem(colj, groups) == rown // q_per_kv
    trow = lax.broadcasted_iota(jnp.int32, (tile, head), 0)
    n_rows = per * heads
    eye = lax.broadcasted_iota(jnp.int32, (n_rows, n_rows), 0) == lax.broadcasted_iota(jnp.int32, (n_rows, n_rows), 1)
    q_rows = n_seq * q_per_kv

    def locate(b):
        rel = pos_ref[b] - base
        at = jnp.clip(rel, 0, n_grp - 1)
        return rel, at, jnp.logical_and(rel >= 0, rel < n_grp)

    def patch(i):
        for which in range(2):
            bulk(i, which).wait()
        for t in range(per):
            b = i * per + t
            _, at, _ = locate(b)
            cut = ds((at // 8) * tile, tile, tile)
            for which in range(2):
                _, dst, new = pairs[which]
                pltpu.make_async_copy(new.at[b], dst.at[b, cut], psem.at[which]).start()

    def step(i, carry):
        scores, fresh, vals = [], [], []
        for t in range(per):
            b = i * per + t
            rel, at, here = locate(b)
            hit = jnp.logical_and(trow // groups == at % 8, here)
            cut = ds((at // 8) * tile, tile, tile)
            rows = []
            for (src, _, dst), off in zip(pairs, (q_rows, q_rows + n_seq)):
                mine = [qkv_ref[g, pl.ds(off + b, 1), :] for g in range(groups)]
                new = mine[0]
                for g in range(1, groups):
                    new = jnp.where(trow % groups == g, mine[g], new)
                dst[b] = jnp.where(hit, new, src[b, cut, :].astype(F32)).astype(BF16)
                rows.append(jnp.concatenate(
                    [jnp.broadcast_to(m, (q_per_kv, head)) for m in mine], axis=0))
            q = jnp.concatenate([qkv_ref[g, ds(b * q_per_kv, q_per_kv, 8), :] for g in range(groups)], axis=0)
            sc = lax.dot_general(q.astype(BF16), k_ref[b], (((1,), (1,)), ((), ())), preferred_element_type=F32)
            ok = jnp.logical_and(same, colj < groups * rel)
            scores.append(jnp.where(ok, sc * (head ** -0.5), -1e30))
            own = jnp.sum(q * rows[0], axis=1, keepdims=True) * (head ** -0.5)
            fresh.append(jnp.where(here, own, -1e30))
            vals.append(rows[1])
        sc = jnp.concatenate(scores, axis=0)
        own = jnp.concatenate(fresh, axis=0)
        top = jnp.maximum(jnp.max(sc, axis=1, keepdims=True), own)
        wt = jnp.exp(sc - top)
        own = jnp.exp(own - top)
        tot = jnp.sum(wt, axis=1, keepdims=True) + own
        wt = wt.astype(BF16)
        own = own.astype(BF16).astype(F32)
        for t in range(per):
            cut = slice(t * heads, (t + 1) * heads)
            o_ref[i, cut, :] = jnp.dot(
                wt[cut], v_ref[i * per + t], preferred_element_type=F32) + own[cut] * vals[t]
        top_row = jnp.sum(jnp.where(eye, top, 0.0), axis=0, keepdims=True)
        tot_row = jnp.sum(jnp.where(eye, tot, 0.0), axis=0, keepdims=True)
        pad = jnp.zeros((6, n_rows), F32)
        o_ref[i, n_rows:n_rows + 8, :] = jnp.concatenate([top_row, tot_row, pad], axis=0)

        @pl.when(i > 0)
        def _():
            patch(i - 1)

        return carry

    lax.fori_loop(0, n_ch, step, 0)
    patch(n_ch - 1)
    for which in range(2):
        _, dst, new = pairs[which]
        pltpu.make_async_copy(new, dst.at[:, pl.ds(0, tile)], psem.at[which]).wait()


def out_kernel(dims, o_ref, h_ref, w_ref, out_ref, rbuf, abuf, attn, lhs, wbuf, pbuf, ybuf, hbuf,
               wsem, hsem, rs_s, rs_r, ab_s, ab_r, y_s, y_r, a_s, a_r, b_s, b_r, d_s, d_r):
    n_tp, n_sp, heads = dims
    nx = n_sp // CORES
    y = lax.axis_index('tp')
    s = lax.axis_index('sp')
    core = lax.rem(s, CORES)
    x = s // CORES
    partner = s + 1 - 2 * core
    _, n_rows, head = attn.shape
    per = n_rows // heads
    depth, cols = wbuf.shape[1:]
    seqs = CORES * per

    def yat(d):
        return lax.rem(y + d, n_tp)

    def xat(d):
        return lax.rem(x + d, nx) * CORES + core

    def wcopy(j):
        return pltpu.make_async_copy(
            w_ref.at[:, ds((core * n_tp + yat(j)) * cols, cols, cols)], wbuf.at[j], wsem.at[j])

    hcopy = pltpu.make_async_copy(
        h_ref.at[ds(x * seqs, seqs, seqs), ds((core * n_tp + y) * cols, cols, cols)], hbuf, hsem)
    order = [d for d in range(1, n_tp)] + [0]
    for j in order:
        wcopy(j).start()
    hcopy.start()

    barrier = pltpu.get_barrier_semaphore()
    for d in range(1, n_sp):
        pl.semaphore_signal(barrier, inc=1, device_id={'sp': lax.rem(s + d, n_sp)}, device_id_type=MESH)
    for d in range(1, n_tp):
        pl.semaphore_signal(barrier, inc=1, device_id={'tp': yat(d)}, device_id_type=MESH)
    pl.semaphore_wait(barrier, n_sp + n_tp - 2)

    def rs(d):
        to = lax.rem(s + d, n_sp)
        return rcopy(o_ref.at[to], rbuf.at[d], rs_s.at[d], rs_r.at[d], sp=to)

    for d in range(1, n_sp):
        rs(d).start()
    parts = [o_ref.at[s]]
    for d in range(1, n_sp):
        rs(d).wait_recv()
        parts.append(rbuf.at[d])
    tops = [p[n_rows:n_rows + 1, :] for p in parts]
    sums = [p[n_rows + 1:n_rows + 2, :] for p in parts]
    top = functools.reduce(jnp.maximum, tops)
    facs = [jnp.exp(t - top) for t in tops]
    tot = functools.reduce(jnp.add, [f * l for f, l in zip(facs, sums)])
    fac = jnp.concatenate([f / tot for f in facs], axis=0)
    pad = jnp.zeros((n_rows - n_sp, n_rows), F32)
    fac = jnp.transpose(jnp.concatenate([fac, pad], axis=0))
    val = parts[0][0:n_rows, :] * fac[:, 0:1]
    for j in range(1, n_sp):
        val = val + parts[j][0:n_rows, :] * fac[:, j:j + 1]
    attn[0] = val

    swap = rcopy(attn.at[0], abuf.at[core], ab_s, ab_r, sp=partner)
    swap.start()
    abuf[core] = val
    swap.wait()
    flat = abuf.reshape(CORES * n_rows, head)
    for n in range(heads):
        lhs[:, n * head:(n + 1) * head] = flat[pl.ds(n, seqs, stride=heads), :].astype(BF16)

    def ysend(d):
        return rcopy(pbuf.at[d], ybuf.at[d], y_s.at[d], y_r.at[d], tp=yat(d))

    def proj(j):
        wcopy(j).wait()
        pbuf[j] = jnp.dot(lhs[...], wbuf[j], preferred_element_type=F32)

    for j in order:
        proj(j)
        if j:
            ysend(j).start()
    hcopy.wait()
    tot = pbuf[0]
    for d in range(1, n_tp):
        ysend(d).wait_recv()
        tot = tot + ybuf[d]
    out_ref[ds(x * seqs, seqs, seqs), ds((core * n_tp + y) * cols, cols, cols)] = hbuf[...].astype(F32) + tot

    def block(dy, dx, part):
        by = lax.rem(y + n_tp - dy, n_tp)
        bx = lax.rem(x + nx - dx, nx)
        return out_ref.at[ds(bx * seqs + part * per, per, per), ds((core * n_tp + by) * cols, cols, cols)]

    sends = []

    def go(dy, dx, part, sems, where, ty, tx):
        ref = block(dy, dx, part)
        cp = rcopy(ref, ref, sems[0].at[ty, tx], sems[1].at[ty, tx], **where)
        cp.start()
        sends.append(cp)

    def fwd(dy, dx, part):
        if part == 0 and dx == 0:
            for e in range(1, nx):
                go(dy, 0, 0, (a_s, a_r), {'sp': xat(e)}, dy, e)
        if part == 1 and dy == 0:
            for e in range(1, n_tp):
                go(0, dx, 1, (b_s, b_r), {'tp': yat(e)}, e, dx)
        ref = block(dy, dx, part)
        cp = rcopy(ref, ref, d_s.at[part, dy, dx], d_r.at[part, dy, dx], sp=partner)
        cp.start()
        sends.append(cp)

    for e in range(1, n_tp):
        go(0, 0, 0, (a_s, a_r), {'tp': yat(e)}, e, 0)
    for e in range(1, nx):
        go(0, 0, 1, (b_s, b_r), {'sp': xat(e)}, 0, e)
    fwd(0, 0, 0)
    fwd(0, 0, 1)

    def arrive(dy, dx, part):
        ref = block(dy, dx, part)
        r = (a_r, b_r)[part].at[dy, dx]
        q = (a_s, b_s)[part].at[dy, dx]
        rcopy(ref, ref, q, r, sp=partner).wait_recv()
        fwd(dy, dx, part)

    for e in range(1, max(n_tp, nx)):
        if e < n_tp:
            arrive(e, 0, 0)
        if e < nx:
            arrive(0, e, 1)
    for dy in range(n_tp):
        for e in range(1, nx):
            arrive(dy, e, 0)
    for dx in range(nx):
        for e in range(1, n_tp):
            arrive(e, dx, 1)
    for part in range(2):
        for dy in range(n_tp):
            for dx in range(nx):
                by = lax.rem(y + n_tp - dy, n_tp)
                bx = lax.rem(x + nx - dx, nx)
                ref = out_ref.at[ds(bx * seqs + part * per, per, per),
                                 ds(((1 - core) * n_tp + by) * cols, cols, cols)]
                rcopy(ref, ref, d_s.at[part, dy, dx], d_r.at[part, dy, dx], sp=partner).wait_recv()
    for cp in sends:
        cp.wait_send()
    for d in range(1, n_sp):
        rs(d).wait_send()
    for d in range(1, n_tp):
        ysend(d).wait_send()


def solution(mesh):
    n_tp, n_sp = mesh.shape['tp'], mesh.shape['sp']
    cache_spec = P('dp', 'sp', 'tp', None)
    DMA = pltpu.SemaphoreType.DMA

    def local_step(hidden, norm_scale, w_qkv, w_out, k_cache, v_cache, positions):
        n_seq, seq_local, kv_local, head = k_cache.shape
        d_model = hidden.shape[1]
        q_per_kv = w_qkv.shape[1] // (kv_local * head) - 2
        heads = kv_local * q_per_kv
        grp_cols = (q_per_kv + 2) * head
        n_blk = 8
        blk = d_model // n_blk
        per = n_seq // n_sp
        n_rows = per * heads

        qkv = pl.pallas_call(
            functools.partial(qkv_kernel, (q_per_kv, head)),
            out_shape=pltpu.VMEM((kv_local, n_seq * (q_per_kv + 2), head), F32),
            in_specs=[HBM, HBM, HBM, HBM],
            out_specs=VMEM,
            scratch_shapes=[
                pltpu.VMEM(hidden.shape, BF16),
                pltpu.VMEM((d_model // 128, 128), BF16),
                pltpu.VMEM((1, n_seq), jnp.int32),
                pltpu.VMEM((n_blk, blk, grp_cols), BF16),
                pltpu.VMEM((n_seq, d_model), BF16),
                pltpu.VMEM((n_seq, grp_cols), F32),
                pltpu.VMEM((n_seq * (q_per_kv + 2), head), F32),
                pltpu.VMEM((d_model // 128, 128), F32),
                DMA((3,)), DMA((n_blk,)), DMA, DMA,
            ],
            compiler_params=pltpu.CompilerParams(
                collective_id=0, has_side_effects=True, vmem_limit_bytes=28 * MIB),
            name='qkv',
        )(in_hbm(hidden), in_hbm(norm_scale.reshape(d_model // 128, 128)),
          in_hbm(positions.reshape(1, n_seq)), in_hbm(w_qkv))

        flat = (n_seq, seq_local * kv_local, head)
        cache_out = jax.ShapeDtypeStruct(flat, BF16)
        tile = 8 * kv_local
        part, k_out, v_out = pl.pallas_call(
            functools.partial(attn_kernel, (q_per_kv, head)),
            out_shape=(pltpu.VMEM((n_sp, n_rows + 8, head), F32), cache_out, cache_out),
            in_specs=[SMEM, VMEM, VMEM, VMEM],
            out_specs=(VMEM, HBM, HBM),
            scratch_shapes=[
                pltpu.VMEM((n_seq, tile, head), BF16), pltpu.VMEM((n_seq, tile, head), BF16),
                DMA((2, n_sp)), DMA((2,)),
            ],
            compiler_params=pltpu.CompilerParams(vmem_limit_bytes=4 * MIB),
            name='attn',
        )(positions, qkv, in_vmem(k_cache.reshape(flat)), in_vmem(v_cache.reshape(flat)))

        nx = n_sp // CORES
        cols = d_model // (CORES * n_tp)
        depth = w_out.shape[0]
        h_out = pl.pallas_call(
            functools.partial(out_kernel, (n_tp, n_sp, heads)),
            out_shape=jax.ShapeDtypeStruct((n_seq, d_model), F32),
            in_specs=[VMEM, HBM, HBM],
            out_specs=VMEM,
            scratch_shapes=[
                pltpu.VMEM((n_sp, n_rows + 8, head), F32),
                pltpu.VMEM((CORES, n_rows, head), F32),
                pltpu.VMEM((1, n_rows, head), F32),
                pltpu.VMEM((CORES * per, depth), BF16),
                pltpu.VMEM((n_tp, depth, cols), BF16),
                pltpu.VMEM((n_tp, CORES * per, cols), F32),
                pltpu.VMEM((n_tp, CORES * per, cols), F32),
                pltpu.VMEM((CORES * per, cols), BF16),
                DMA((n_tp,)), DMA,
                DMA((n_sp,)), DMA((n_sp,)), DMA, DMA, DMA((n_tp,)), DMA((n_tp,)),
                DMA((n_tp, nx)), DMA((n_tp, nx)), DMA((n_tp, nx)), DMA((n_tp, nx)),
                DMA((2, n_tp, nx)), DMA((2, n_tp, nx)),
            ],
            compiler_params=pltpu.CompilerParams(
                collective_id=1, has_side_effects=True, vmem_limit_bytes=28 * MIB),
            name='outproj',
        )(part, in_hbm(hidden), in_hbm(w_out))
        return h_out.astype(BF16), k_out.reshape(k_cache.shape), v_out.reshape(v_cache.shape)

    return jax.shard_map(
        local_step,
        mesh=mesh,
        in_specs=(P('dp', None), P(None), P(None, 'tp'), P('tp', None), cache_spec, cache_spec, P('dp')),
        out_specs=(P('dp', None), cache_spec, cache_spec),
        check_vma=False,
    )
```

```python
import functools
import math

import jax
import jax.numpy as jnp
from jax import lax
from jax.experimental import pallas as pl
from jax.experimental.pallas import tpu as pltpu
from jax.sharding import PartitionSpec as P

MESH = pl.DeviceIdType.MESH
F32 = jnp.float32
BF16 = jnp.bfloat16
HBM = pl.BlockSpec(memory_space=pltpu.HBM)
VMEM = pl.BlockSpec(memory_space=pltpu.VMEM)
SMEM = pl.BlockSpec(memory_space=pltpu.SMEM)
CORES = 2
RING_HEADS = 1
MIB = 1024 * 1024


def in_hbm(val):
    return pltpu.with_memory_space_constraint(val, pltpu.HBM)


def ds(start, size, align):
    return pl.ds(pl.multiple_of(start, align), size)


def rcopy(src, dst, send_sem, recv_sem, **where):
    return pltpu.make_async_remote_copy(
        src_ref=src, dst_ref=dst, send_sem=send_sem, recv_sem=recv_sem,
        device_id=where, device_id_type=MESH,
    )


def qkv_kernel(dims, h_hbm, scale_hbm, pos_hbm, w_ref, k_hbm, v_hbm, out_ref, kbuf, vbuf, h_ref, scale_ref, pos_ref,
               wring, wloc, u_ref, acc, gain, hsem, rsem, wsem, csem, s_ring, r_ring, s_part, r_part):
    n_seq, d_model = h_ref.shape
    q_per_kv, head, n_sp = dims
    nx = n_sp // CORES
    n_rblk, rblk, rcols = wring.shape
    n_blk, blk, lcols = wloc.shape
    rh = rcols // head
    grp = (q_per_kv + 2) * head
    s = lax.axis_index('sp')
    core = lax.rem(s, CORES)
    x = s // CORES
    partner = s + 1 - 2 * core

    def rload(i):
        return pltpu.make_async_copy(
            w_ref.at[ds(i * rblk, rblk, rblk), ds(core * grp + x * rcols, rcols, 128)], wring.at[i], rsem.at[i])

    def wload(i):
        return pltpu.make_async_copy(
            w_ref.at[ds(i * blk, blk, blk), ds(core * grp + nx * rcols, lcols, 128)], wloc.at[i], wsem.at[i])

    loads = [
        pltpu.make_async_copy(src, dst, hsem.at[i])
        for i, (src, dst) in enumerate(((h_hbm, h_ref), (scale_hbm, scale_ref), (pos_hbm, pos_ref)))
    ]
    caches = [
        pltpu.make_async_copy(src, dst, csem.at[i]) for i, (src, dst) in enumerate(((k_hbm, kbuf), (v_hbm, vbuf)))
    ]
    for load in loads:
        load.start()
    for i in range(n_rblk):
        rload(i).start()
    for i in range(n_blk):
        wload(i).start()
    barrier = pltpu.get_barrier_semaphore()
    pl.semaphore_signal(barrier, inc=1, device_id={'sp': partner}, device_id_type=MESH)
    for d in range(1, nx):
        pl.semaphore_signal(
            barrier, inc=1, device_id={'sp': lax.rem(x + d, nx) * CORES + core}, device_id_type=MESH)
    for load in loads:
        load.wait()

    lanes = 128
    zero = jnp.zeros((n_seq, lanes), F32)

    def add_sum(i, tot):
        return tot + h_ref[:, ds(i * lanes, lanes, lanes)].astype(F32)

    mean = jnp.sum(lax.fori_loop(0, d_model // lanes, add_sum, zero, unroll=8), axis=1, keepdims=True) / d_model

    def add_sq(i, tot):
        cent = h_ref[:, ds(i * lanes, lanes, lanes)].astype(F32) - mean
        return tot + cent * cent

    var = jnp.sum(lax.fori_loop(0, d_model // lanes, add_sq, zero, unroll=8), axis=1, keepdims=True) / d_model
    inv = lax.rsqrt(var + 1e-5)

    gain[...] = scale_ref[...].astype(F32)

    def norm(i, carry):
        cut = ds(i * lanes, lanes, lanes)
        cent = h_ref[:, cut].astype(F32) - mean
        u_ref[:, cut] = (cent * inv * gain[pl.ds(i, 1), :]).astype(BF16)
        return carry

    lax.fori_loop(0, d_model // lanes, norm, 0, unroll=8)

    eye = lax.broadcasted_iota(jnp.int32, (n_seq, n_seq), 0) == lax.broadcasted_iota(jnp.int32, (n_seq, n_seq), 1)
    pos_col = jnp.sum(jnp.where(eye, pos_ref[...].astype(F32), 0.0), axis=1, keepdims=True)
    lane = lax.broadcasted_iota(jnp.int32, (n_seq, head), 1)
    half = head // 2
    inv_freq = jnp.exp(lax.rem(lane, half).astype(F32) * (-2.0 * math.log(500000.0) / head))
    angle = pos_col * inv_freq
    cos_t = jnp.cos(angle)
    sin_t = jnp.where(lane < half, -jnp.sin(angle), jnp.sin(angle))

    def finish(val, rotate):
        val = jnp.clip(val.astype(BF16), -8.0, 8.0).astype(F32)
        if rotate:
            val = (val * cos_t + pltpu.roll(val, half, 1) * sin_t).astype(BF16).astype(F32)
        return val

    def slab(cx):
        return out_ref.at[core, ds(cx * rh * n_seq, rh * n_seq, 8)]

    def rsend(d):
        return rcopy(slab(x), slab(x), s_ring.at[d], r_ring.at[d], sp=lax.rem(x + d, nx) * CORES + core)

    def psend(d):
        ref = slab(lax.rem(x + nx - d, nx)) if d < nx else out_ref.at[core, pl.ds(nx * rh * n_seq, lcols // head * n_seq)]
        return rcopy(ref, ref, s_part.at[d], r_part.at[d], sp=partner)

    tot = None
    for i in range(n_rblk):
        rload(i).wait()
        prod = jnp.dot(u_ref[:, i * rblk:(i + 1) * rblk], wring[i], preferred_element_type=F32)
        tot = prod if tot is None else tot + prod
    for j in range(rh):
        out_ref[core, ds((x * rh + j) * n_seq, n_seq, n_seq), :] = finish(tot[:, j * head:(j + 1) * head], True)
    pl.semaphore_wait(barrier, nx)
    order = [2, 1, 3] if nx == 4 else list(range(1, nx))
    for d in order:
        rsend(d).start()
    psend(0).start()
    for cp in caches:
        cp.start()

    acc[...] = jnp.zeros_like(acc)

    def mm(i, carry):
        wload(i).wait()
        acc[...] += jnp.dot(u_ref[:, ds(i * blk, blk, blk)], wloc[i], preferred_element_type=F32)
        return carry

    lax.fori_loop(0, n_blk, mm, 0)
    for j in range(lcols // head):
        at = nx * rh + j
        out_ref[core, at * n_seq:(at + 1) * n_seq, :] = finish(acc[:, j * head:(j + 1) * head], at < q_per_kv + 1)
    psend(nx).start()
    for d in list(reversed(order)):
        rsend(d).wait_recv()
        psend(d).start()
    for d in range(nx + 1):
        psend(d).wait()
    for d in order:
        rsend(d).wait_send()
    for cp in caches:
        cp.wait()


def attn_kernel(dims, pos_ref, qkv_ref, k_ref, v_ref, o_ref, ko_ref, vo_ref, kp, vp, osem, psem):
    q_per_kv, head = dims
    n_seq, rows2, _ = k_ref.shape
    groups = qkv_ref.shape[0]
    n_grp = rows2 // groups
    n_ch = o_ref.shape[0]
    per = n_seq // n_ch
    heads = groups * q_per_kv
    base = lax.axis_index('sp') * n_grp
    tile = 8 * groups
    pairs = ((k_ref, ko_ref, kp), (v_ref, vo_ref, vp))

    def bulk(i, which):
        src, dst, _ = pairs[which]
        cut = pl.ds(i * per, per)
        return pltpu.make_async_copy(src.at[cut], dst.at[cut], osem.at[which, i])

    for i in range(n_ch):
        bulk(i, 0).start()
        bulk(i, 1).start()

    colj = lax.broadcasted_iota(jnp.int32, (heads, rows2), 1)
    rown = lax.broadcasted_iota(jnp.int32, (heads, rows2), 0)
    same = lax.rem(colj, groups) == rown // q_per_kv
    trow = lax.broadcasted_iota(jnp.int32, (tile, head), 0)
    n_rows = per * heads
    eye = lax.broadcasted_iota(jnp.int32, (n_rows, n_rows), 0) == lax.broadcasted_iota(jnp.int32, (n_rows, n_rows), 1)
    q_rows = n_seq * q_per_kv

    def locate(b):
        rel = pos_ref[b] - base
        at = jnp.clip(rel, 0, n_grp - 1)
        return rel, at, jnp.logical_and(rel >= 0, rel < n_grp)

    def fresh_row(off, b):
        return [qkv_ref[g, pl.ds(off + b, 1), :] for g in range(groups)]

    def patch(b, which):
        _, at, _ = locate(b)
        _, dst, new = pairs[which]
        return pltpu.make_async_copy(new.at[b], dst.at[b, ds((at // 8) * tile, tile, tile)], psem.at[which])

    def build(b, carry):
        _, at, here = locate(b)

        @pl.when(here)
        def _():
            for (src, _, dst), off in zip(pairs, (q_rows, q_rows + n_seq)):
                mine = fresh_row(off, b)
                new = mine[0]
                for g in range(1, groups):
                    new = jnp.where(trow % groups == g, mine[g], new)
                old = src[b, ds((at // 8) * tile, tile, tile), :].astype(F32)
                dst[b] = jnp.where(trow // groups == at % 8, new, old).astype(BF16)

        return carry

    def send(b, carry):
        @pl.when(locate(b)[2])
        def _():
            patch(b, 0).start()
            patch(b, 1).start()

        return carry

    def drain(b, carry):
        @pl.when(locate(b)[2])
        def _():
            patch(b, 0).wait()
            patch(b, 1).wait()

        return carry

    def step(i, carry):
        scores, fresh, vals = [], [], []
        for t in range(per):
            b = i * per + t
            rel, at, here = locate(b)
            rows = [
                jnp.concatenate([jnp.broadcast_to(m, (q_per_kv, head)) for m in fresh_row(off, b)], axis=0)
                for off in (q_rows, q_rows + n_seq)
            ]
            q = jnp.concatenate([qkv_ref[g, pl.ds(b, q_per_kv, stride=n_seq), :] for g in range(groups)], axis=0)
            sc = lax.dot_general(q.astype(BF16), k_ref[b], (((1,), (1,)), ((), ())), preferred_element_type=F32)
            ok = jnp.logical_and(same, colj < groups * rel)
            scores.append(jnp.where(ok, sc * (head ** -0.5), -1e30))
            own = jnp.sum(q * rows[0], axis=1, keepdims=True) * (head ** -0.5)
            fresh.append(jnp.where(here, own, -1e30))
            vals.append(rows[1])
        sc = jnp.concatenate(scores, axis=0)
        own = jnp.concatenate(fresh, axis=0)
        top = jnp.maximum(jnp.max(sc, axis=1, keepdims=True), own)
        wt = jnp.exp(sc - top)
        own = jnp.exp(own - top)
        tot = jnp.sum(wt, axis=1, keepdims=True) + own
        wt = wt.astype(BF16)
        own = own.astype(BF16).astype(F32)
        for t in range(per):
            cut = slice(t * heads, (t + 1) * heads)
            o_ref[i, cut, :] = jnp.dot(
                wt[cut], v_ref[i * per + t], preferred_element_type=F32) + own[cut] * vals[t]
        top_row = jnp.sum(jnp.where(eye, top, 0.0), axis=0, keepdims=True)
        tot_row = jnp.sum(jnp.where(eye, tot, 0.0), axis=0, keepdims=True)
        pad = jnp.zeros((6, n_rows), F32)
        o_ref[i, n_rows:n_rows + 8, :] = jnp.concatenate([top_row, tot_row, pad], axis=0)
        return carry

    lax.fori_loop(0, n_seq, build, 0)
    lax.fori_loop(0, n_ch, step, 0)
    for i in range(n_ch):
        bulk(i, 0).wait()
        bulk(i, 1).wait()
    lax.fori_loop(0, n_seq, send, 0)
    lax.fori_loop(0, n_seq, drain, 0)


def out_kernel(dims, o_ref, h_ref, w_ref, out_ref, rbuf, abuf, attn, lhs, wbuf, pbuf, ybuf, hbuf,
               wsem, hsem, rs_s, rs_r, ab_s, ab_r, y_s, y_r, a_s, a_r, b_s, b_r, d_s, d_r):
    n_tp, n_sp, heads = dims
    nx = n_sp // CORES
    y = lax.axis_index('tp')
    s = lax.axis_index('sp')
    core = lax.rem(s, CORES)
    x = s // CORES
    partner = s + 1 - 2 * core
    _, n_rows, head = attn.shape
    per = n_rows // heads
    depth, cols = wbuf.shape[1:]
    seqs = CORES * per

    def yat(d):
        return lax.rem(y + d, n_tp)

    def xat(d):
        return lax.rem(x + d, nx) * CORES + core

    def wcopy(j):
        return pltpu.make_async_copy(
            w_ref.at[:, ds((core * n_tp + yat(j)) * cols, cols, cols)], wbuf.at[j], wsem.at[j])

    hcopy = pltpu.make_async_copy(
        h_ref.at[ds(x * seqs, seqs, seqs), ds((core * n_tp + y) * cols, cols, cols)], hbuf, hsem)
    order = [d for d in range(1, n_tp)] + [0]
    for j in order:
        wcopy(j).start()
    hcopy.start()

    barrier = pltpu.get_barrier_semaphore()
    for d in range(1, n_sp):
        pl.semaphore_signal(barrier, inc=1, device_id={'sp': lax.rem(s + d, n_sp)}, device_id_type=MESH)
    for d in range(1, n_tp):
        pl.semaphore_signal(barrier, inc=1, device_id={'tp': yat(d)}, device_id_type=MESH)
    pl.semaphore_wait(barrier, n_sp + n_tp - 2)

    def rs(d):
        to = lax.rem(s + d, n_sp)
        return rcopy(o_ref.at[to], rbuf.at[d], rs_s.at[d], rs_r.at[d], sp=to)

    for d in range(1, n_sp):
        rs(d).start()
    parts = [o_ref.at[s]]
    for d in range(1, n_sp):
        rs(d).wait_recv()
        parts.append(rbuf.at[d])
    tops = [p[n_rows:n_rows + 1, :] for p in parts]
    sums = [p[n_rows + 1:n_rows + 2, :] for p in parts]
    top = functools.reduce(jnp.maximum, tops)
    facs = [jnp.exp(t - top) for t in tops]
    tot = functools.reduce(jnp.add, [f * l for f, l in zip(facs, sums)])
    fac = jnp.concatenate([f / tot for f in facs], axis=0)
    pad = jnp.zeros((n_rows - n_sp, n_rows), F32)
    fac = jnp.transpose(jnp.concatenate([fac, pad], axis=0))
    val = parts[0][0:n_rows, :] * fac[:, 0:1]
    for j in range(1, n_sp):
        val = val + parts[j][0:n_rows, :] * fac[:, j:j + 1]
    attn[0] = val

    swap = rcopy(attn.at[0], abuf.at[core], ab_s, ab_r, sp=partner)
    swap.start()
    abuf[core] = val
    swap.wait()
    flat = abuf.reshape(CORES * n_rows, head)
    for n in range(heads):
        lhs[:, n * head:(n + 1) * head] = flat[pl.ds(n, seqs, stride=heads), :].astype(BF16)

    def ysend(d):
        return rcopy(pbuf.at[d], ybuf.at[d], y_s.at[d], y_r.at[d], tp=yat(d))

    def proj(j):
        wcopy(j).wait()
        pbuf[j] = jnp.dot(lhs[...], wbuf[j], preferred_element_type=F32)

    for j in order:
        proj(j)
        if j:
            ysend(j).start()
    hcopy.wait()
    tot = pbuf[0]
    for d in range(1, n_tp):
        ysend(d).wait_recv()
        tot = tot + ybuf[d]
    out_ref[ds(x * seqs, seqs, seqs), ds((core * n_tp + y) * cols, cols, cols)] = hbuf[...].astype(F32) + tot

    def block(dy, dx, part):
        by = lax.rem(y + n_tp - dy, n_tp)
        bx = lax.rem(x + nx - dx, nx)
        return out_ref.at[ds(bx * seqs + part * per, per, per), ds((core * n_tp + by) * cols, cols, cols)]

    sends = []

    def go(dy, dx, part, sems, where, ty, tx):
        ref = block(dy, dx, part)
        cp = rcopy(ref, ref, sems[0].at[ty, tx], sems[1].at[ty, tx], **where)
        cp.start()
        sends.append(cp)

    def fwd(dy, dx, part):
        if part == 0 and dx == 0:
            for e in range(1, nx):
                go(dy, 0, 0, (a_s, a_r), {'sp': xat(e)}, dy, e)
        if part == 1 and dy == 0:
            for e in range(1, n_tp):
                go(0, dx, 1, (b_s, b_r), {'tp': yat(e)}, e, dx)
        ref = block(dy, dx, part)
        cp = rcopy(ref, ref, d_s.at[part, dy, dx], d_r.at[part, dy, dx], sp=partner)
        cp.start()
        sends.append(cp)

    for e in range(1, n_tp):
        go(0, 0, 0, (a_s, a_r), {'tp': yat(e)}, e, 0)
    for e in range(1, nx):
        go(0, 0, 1, (b_s, b_r), {'sp': xat(e)}, 0, e)
    fwd(0, 0, 0)
    fwd(0, 0, 1)

    def arrive(dy, dx, part):
        ref = block(dy, dx, part)
        r = (a_r, b_r)[part].at[dy, dx]
        q = (a_s, b_s)[part].at[dy, dx]
        rcopy(ref, ref, q, r, sp=partner).wait_recv()
        fwd(dy, dx, part)

    for e in range(1, max(n_tp, nx)):
        if e < n_tp:
            arrive(e, 0, 0)
        if e < nx:
            arrive(0, e, 1)
    for dy in range(n_tp):
        for e in range(1, nx):
            arrive(dy, e, 0)
    for dx in range(nx):
        for e in range(1, n_tp):
            arrive(e, dx, 1)
    for part in range(2):
        for dy in range(n_tp):
            for dx in range(nx):
                by = lax.rem(y + n_tp - dy, n_tp)
                bx = lax.rem(x + nx - dx, nx)
                ref = out_ref.at[ds(bx * seqs + part * per, per, per),
                                 ds(((1 - core) * n_tp + by) * cols, cols, cols)]
                rcopy(ref, ref, d_s.at[part, dy, dx], d_r.at[part, dy, dx], sp=partner).wait_recv()
    for cp in sends:
        cp.wait_send()
    for d in range(1, n_sp):
        rs(d).wait_send()
    for d in range(1, n_tp):
        ysend(d).wait_send()


def solution(mesh):
    n_tp, n_sp = mesh.shape['tp'], mesh.shape['sp']
    cache_spec = P('dp', 'sp', 'tp', None)
    DMA = pltpu.SemaphoreType.DMA

    def local_step(hidden, norm_scale, w_qkv, w_out, k_cache, v_cache, positions):
        n_seq, seq_local, kv_local, head = k_cache.shape
        d_model = hidden.shape[1]
        q_per_kv = w_qkv.shape[1] // (kv_local * head) - 2
        heads = kv_local * q_per_kv
        grp_cols = (q_per_kv + 2) * head
        n_blk, n_rblk = 8, 2
        nx = n_sp // CORES
        ring_cols = RING_HEADS * head
        local_cols = grp_cols - nx * ring_cols
        per = n_seq // n_sp
        n_rows = per * heads
        flat = (n_seq, seq_local * kv_local, head)

        qkv, k_now, v_now = pl.pallas_call(
            functools.partial(qkv_kernel, (q_per_kv, head, n_sp)),
            out_shape=(pltpu.VMEM((kv_local, n_seq * (q_per_kv + 2), head), F32),
                       pltpu.VMEM(flat, BF16), pltpu.VMEM(flat, BF16)),
            in_specs=[HBM] * 6,
            out_specs=(VMEM, VMEM, VMEM),
            scratch_shapes=[
                pltpu.VMEM(hidden.shape, BF16),
                pltpu.VMEM((d_model // 128, 128), BF16),
                pltpu.VMEM((1, n_seq), jnp.int32),
                pltpu.VMEM((n_rblk, d_model // n_rblk, ring_cols), BF16),
                pltpu.VMEM((n_blk, d_model // n_blk, local_cols), BF16),
                pltpu.VMEM((n_seq, d_model), BF16),
                pltpu.VMEM((n_seq, local_cols), F32),
                pltpu.VMEM((d_model // 128, 128), F32),
                DMA((3,)), DMA((n_rblk,)), DMA((n_blk,)), DMA((2,)),
                DMA((nx,)), DMA((nx,)), DMA((nx + 1,)), DMA((nx + 1,)),
            ],
            compiler_params=pltpu.CompilerParams(
                collective_id=0, has_side_effects=True, vmem_limit_bytes=24 * MIB),
            name='qkv',
        )(in_hbm(hidden), in_hbm(norm_scale.reshape(d_model // 128, 128)),
          in_hbm(positions.reshape(1, n_seq)), in_hbm(w_qkv), in_hbm(k_cache.reshape(flat)),
          in_hbm(v_cache.reshape(flat)))

        cache_out = jax.ShapeDtypeStruct(flat, BF16)
        tile = 8 * kv_local
        part, k_out, v_out = pl.pallas_call(
            functools.partial(attn_kernel, (q_per_kv, head)),
            out_shape=(pltpu.VMEM((n_sp, n_rows + 8, head), F32), cache_out, cache_out),
            in_specs=[SMEM, VMEM, VMEM, VMEM],
            out_specs=(VMEM, HBM, HBM),
            scratch_shapes=[
                pltpu.VMEM((n_seq, tile, head), BF16), pltpu.VMEM((n_seq, tile, head), BF16),
                DMA((2, n_sp)), DMA((2,)),
            ],
            compiler_params=pltpu.CompilerParams(vmem_limit_bytes=4 * MIB),
            name='attn',
        )(positions, qkv, k_now, v_now)

        cols = d_model // (CORES * n_tp)
        depth = w_out.shape[0]
        h_out = pl.pallas_call(
            functools.partial(out_kernel, (n_tp, n_sp, heads)),
            out_shape=jax.ShapeDtypeStruct((n_seq, d_model), F32),
            in_specs=[VMEM, HBM, HBM],
            out_specs=VMEM,
            scratch_shapes=[
                pltpu.VMEM((n_sp, n_rows + 8, head), F32),
                pltpu.VMEM((CORES, n_rows, head), F32),
                pltpu.VMEM((1, n_rows, head), F32),
                pltpu.VMEM((CORES * per, depth), BF16),
                pltpu.VMEM((n_tp, depth, cols), BF16),
                pltpu.VMEM((n_tp, CORES * per, cols), F32),
                pltpu.VMEM((n_tp, CORES * per, cols), F32),
                pltpu.VMEM((CORES * per, cols), BF16),
                DMA((n_tp,)), DMA,
                DMA((n_sp,)), DMA((n_sp,)), DMA, DMA, DMA((n_tp,)), DMA((n_tp,)),
                DMA((n_tp, nx)), DMA((n_tp, nx)), DMA((n_tp, nx)), DMA((n_tp, nx)),
                DMA((2, n_tp, nx)), DMA((2, n_tp, nx)),
            ],
            compiler_params=pltpu.CompilerParams(
                collective_id=1, has_side_effects=True, vmem_limit_bytes=28 * MIB),
            name='outproj',
        )(part, in_hbm(hidden), in_hbm(w_out))
        return h_out.astype(BF16), k_out.reshape(k_cache.shape), v_out.reshape(v_cache.shape)

    return jax.shard_map(
        local_step,
        mesh=mesh,
        in_specs=(P('dp', None), P(None), P(None, 'tp'), P('tp', None), cache_spec, cache_spec, P('dp')),
        out_specs=(P('dp', None), cache_spec, cache_spec),
        check_vma=False,
    )
```

```python
import functools
import math

import jax
import jax.numpy as jnp
from jax import lax
from jax.experimental import pallas as pl
from jax.experimental.pallas import tpu as pltpu
from jax.sharding import PartitionSpec as P

MESH = pl.DeviceIdType.MESH
F32 = jnp.float32
BF16 = jnp.bfloat16
HBM = pl.BlockSpec(memory_space=pltpu.HBM)
VMEM = pl.BlockSpec(memory_space=pltpu.VMEM)
SMEM = pl.BlockSpec(memory_space=pltpu.SMEM)
CORES = 2
MIB = 1024 * 1024


def in_hbm(val):
    return pltpu.with_memory_space_constraint(val, pltpu.HBM)


def ds(start, size, align):
    return pl.ds(pl.multiple_of(start, align), size)


def rcopy(src, dst, send_sem, recv_sem, **where):
    return pltpu.make_async_remote_copy(
        src_ref=src, dst_ref=dst, send_sem=send_sem, recv_sem=recv_sem,
        device_id=where, device_id_type=MESH,
    )


def qkv_kernel(dims, h_hbm, scale_hbm, pos_hbm, w_ref, k_hbm, v_hbm, out_ref, kbuf, vbuf, h_ref, scale_ref, pos_ref,
               wbuf, u_ref, gain, hsem, wsem, csem, s_part, r_part):
    n_seq, d_model = h_ref.shape
    q_per_kv, head, pitch = dims
    n_blk, n_half, blk, cols = wbuf.shape
    grp = (q_per_kv + 2) * head
    s = lax.axis_index('sp')
    core = lax.rem(s, CORES)
    partner = s + 1 - 2 * core

    def wload(i, k):
        return pltpu.make_async_copy(
            w_ref.at[pl.ds(k * blk, blk), ds(core * grp + i * cols, cols, 128)], wbuf.at[i, k], wsem.at[i, k])

    loads = [
        pltpu.make_async_copy(src, dst, hsem.at[i])
        for i, (src, dst) in enumerate(((h_hbm, h_ref), (scale_hbm, scale_ref), (pos_hbm, pos_ref)))
    ]
    caches = [
        pltpu.make_async_copy(src, dst, csem.at[i]) for i, (src, dst) in enumerate(((k_hbm, kbuf), (v_hbm, vbuf)))
    ]
    for load in loads:
        load.start()
    for i in range(n_blk):
        for k in range(n_half):
            wload(i, k).start()
    barrier = pltpu.get_barrier_semaphore()
    pl.semaphore_signal(barrier, inc=1, device_id={'sp': partner}, device_id_type=MESH)
    for load in loads:
        load.wait()

    lanes = 128
    zero = jnp.zeros((n_seq, lanes), F32)

    def add_sum(i, tot):
        return tot + h_ref[:, ds(i * lanes, lanes, lanes)].astype(F32)

    mean = jnp.sum(lax.fori_loop(0, d_model // lanes, add_sum, zero, unroll=8), axis=1, keepdims=True) / d_model

    def add_sq(i, tot):
        cent = h_ref[:, ds(i * lanes, lanes, lanes)].astype(F32) - mean
        return tot + cent * cent

    var = jnp.sum(lax.fori_loop(0, d_model // lanes, add_sq, zero, unroll=8), axis=1, keepdims=True) / d_model
    inv = lax.rsqrt(var + 1e-5)

    gain[...] = scale_ref[...].astype(F32)

    def norm(i, carry):
        cut = ds(i * lanes, lanes, lanes)
        cent = h_ref[:, cut].astype(F32) - mean
        u_ref[:, cut] = (cent * inv * gain[pl.ds(i, 1), :]).astype(BF16)
        return carry

    lax.fori_loop(0, d_model // lanes, norm, 0, unroll=8)

    eye = lax.broadcasted_iota(jnp.int32, (n_seq, n_seq), 0) == lax.broadcasted_iota(jnp.int32, (n_seq, n_seq), 1)
    pos_col = jnp.sum(jnp.where(eye, pos_ref[...].astype(F32), 0.0), axis=1, keepdims=True)
    lane = lax.broadcasted_iota(jnp.int32, (n_seq, head), 1)
    half = head // 2
    inv_freq = jnp.exp(lax.rem(lane, half).astype(F32) * (-2.0 * math.log(500000.0) / head))
    angle = pos_col * inv_freq
    cos_t = jnp.cos(angle)
    sin_t = jnp.where(lane < half, -jnp.sin(angle), jnp.sin(angle))

    def psend(j):
        ref = out_ref.at[core, pl.ds(j * pitch, n_seq)]
        return rcopy(ref, ref, s_part.at[j], r_part.at[j], sp=partner)

    for i in range(n_blk):
        tot = None
        for k in range(n_half):
            wload(i, k).wait()
            prod = jnp.dot(u_ref[:, k * blk:(k + 1) * blk], wbuf[i, k], preferred_element_type=F32)
            tot = prod if tot is None else tot + prod
        per_blk = cols // head
        for t in range(per_blk):
            j = i * per_blk + t
            val = jnp.clip(tot[:, t * head:(t + 1) * head].astype(BF16), -8.0, 8.0).astype(F32)
            if j < q_per_kv + 1:
                val = (val * cos_t + pltpu.roll(val, half, 1) * sin_t).astype(BF16).astype(F32)
            out_ref[core, j * pitch:j * pitch + n_seq, :] = val
        if i == 0:
            pl.semaphore_wait(barrier, 1)
        for t in range(per_blk):
            psend(i * per_blk + t).start()
        if i == 1:
            caches[0].start()
        if i == 2:
            caches[1].start()
    for j in range(q_per_kv + 2):
        psend(j).wait()
    for cp in caches:
        cp.wait()


def attn_kernel(dims, pos_ref, qkv_ref, k_ref, v_ref, o_ref, ko_ref, vo_ref, kbuf, vbuf, osem):
    q_per_kv, head, pitch = dims
    n_seq, rows2, _ = kbuf.shape
    groups = qkv_ref.shape[0]
    n_grp = rows2 // groups
    n_ch = o_ref.shape[0]
    per = n_seq // n_ch
    heads = groups * q_per_kv
    base = lax.axis_index('sp') * n_grp

    def bulk(i, which):
        src, dst = ((kbuf, ko_ref), (vbuf, vo_ref))[which]
        cut = pl.ds(i * per, per)
        return pltpu.make_async_copy(src.at[cut], dst.at[cut], osem.at[which, i])

    colj = lax.broadcasted_iota(jnp.int32, (heads, rows2), 1)
    rown = lax.broadcasted_iota(jnp.int32, (heads, rows2), 0)
    same = lax.rem(colj, groups) == rown // q_per_kv
    tile = 8 * groups
    trow = lax.broadcasted_iota(jnp.int32, (tile, head), 0)
    n_rows = per * heads
    eye = lax.broadcasted_iota(jnp.int32, (n_rows, n_rows), 0) == lax.broadcasted_iota(jnp.int32, (n_rows, n_rows), 1)

    def step(i, carry):
        @pl.when(i > 0)
        def _():
            bulk(i - 1, 0).start()
            bulk(i - 1, 1).start()

        scores = []
        for t in range(per):
            b = i * per + t
            rel = pos_ref[b] - base
            here = jnp.logical_and(rel >= 0, rel < n_grp)
            at = jnp.clip(rel, 0, n_grp - 1)
            cut = ds((at // 8) * tile, tile, tile)
            hit = jnp.logical_and(trow // groups == at % 8, here)
            for src, buf, off in ((k_ref, kbuf, q_per_kv * pitch), (v_ref, vbuf, (q_per_kv + 1) * pitch)):
                new = qkv_ref[0, pl.ds(off + b, 1), :]
                for g in range(1, groups):
                    new = jnp.where(trow % groups == g, qkv_ref[g, pl.ds(off + b, 1), :], new)
                buf[b, cut, :] = jnp.where(hit, new, src[b, cut, :].astype(F32)).astype(BF16)
            q = jnp.concatenate([qkv_ref[g, pl.ds(b, q_per_kv, stride=pitch), :] for g in range(groups)], axis=0)
            sc = lax.dot_general(q.astype(BF16), kbuf[b], (((1,), (1,)), ((), ())), preferred_element_type=F32)
            ok = jnp.logical_and(same, colj < groups * (rel + 1))
            scores.append(jnp.where(ok, sc * (head ** -0.5), -1e30))
        sc = jnp.concatenate(scores, axis=0)
        top = jnp.max(sc, axis=1, keepdims=True)
        wt = jnp.exp(sc - top)
        tot = jnp.sum(wt, axis=1, keepdims=True)
        wt = wt.astype(BF16)
        for t in range(per):
            o_ref[i, t * heads:(t + 1) * heads, :] = jnp.dot(
                wt[t * heads:(t + 1) * heads], vbuf[i * per + t], preferred_element_type=F32)
        top_row = jnp.sum(jnp.where(eye, top, 0.0), axis=0, keepdims=True)
        tot_row = jnp.sum(jnp.where(eye, tot, 0.0), axis=0, keepdims=True)
        pad = jnp.zeros((6, n_rows), F32)
        o_ref[i, n_rows:n_rows + 8, :] = jnp.concatenate([top_row, tot_row, pad], axis=0)
        return carry

    lax.fori_loop(0, n_ch, step, 0)
    bulk(n_ch - 1, 0).start()
    bulk(n_ch - 1, 1).start()
    for i in range(n_ch):
        bulk(i, 0).wait()
        bulk(i, 1).wait()


def out_kernel(dims, o_ref, h_ref, w_ref, out_ref, rbuf, abuf, attn, lhs, wbuf, pbuf, ybuf, hbuf,
               wsem, hsem, rs_s, rs_r, ab_s, ab_r, y_s, y_r, a_s, a_r, b_s, b_r, d_s, d_r):
    n_tp, n_sp, heads = dims
    nx = n_sp // CORES
    y = lax.axis_index('tp')
    s = lax.axis_index('sp')
    core = lax.rem(s, CORES)
    x = s // CORES
    partner = s + 1 - 2 * core
    _, n_rows, head = attn.shape
    per = n_rows // heads
    depth, cols = wbuf.shape[1:]
    seqs = CORES * per

    def yat(d):
        return lax.rem(y + d, n_tp)

    def xat(d):
        return lax.rem(x + d, nx) * CORES + core

    def wcopy(j):
        return pltpu.make_async_copy(
            w_ref.at[:, ds((core * n_tp + yat(j)) * cols, cols, cols)], wbuf.at[j], wsem.at[j])

    hcopy = pltpu.make_async_copy(
        h_ref.at[ds(x * seqs, seqs, seqs), ds((core * n_tp + y) * cols, cols, cols)], hbuf, hsem)
    order = [d for d in range(1, n_tp)] + [0]
    for j in order:
        wcopy(j).start()
    hcopy.start()

    barrier = pltpu.get_barrier_semaphore()
    for d in range(1, n_sp):
        pl.semaphore_signal(barrier, inc=1, device_id={'sp': lax.rem(s + d, n_sp)}, device_id_type=MESH)
    for d in range(1, n_tp):
        pl.semaphore_signal(barrier, inc=1, device_id={'tp': yat(d)}, device_id_type=MESH)
    pl.semaphore_wait(barrier, n_sp + n_tp - 2)

    def rs(d):
        to = lax.rem(s + d, n_sp)
        return rcopy(o_ref.at[to], rbuf.at[d], rs_s.at[d], rs_r.at[d], sp=to)

    for d in range(1, n_sp):
        rs(d).start()
    parts = [o_ref.at[s]]
    for d in range(1, n_sp):
        rs(d).wait_recv()
        parts.append(rbuf.at[d])
    tops = [p[n_rows:n_rows + 1, :] for p in parts]
    sums = [p[n_rows + 1:n_rows + 2, :] for p in parts]
    top = functools.reduce(jnp.maximum, tops)
    facs = [jnp.exp(t - top) for t in tops]
    tot = functools.reduce(jnp.add, [f * l for f, l in zip(facs, sums)])
    fac = jnp.concatenate([f / tot for f in facs], axis=0)
    pad = jnp.zeros((n_rows - n_sp, n_rows), F32)
    fac = jnp.transpose(jnp.concatenate([fac, pad], axis=0))
    val = parts[0][0:n_rows, :] * fac[:, 0:1]
    for j in range(1, n_sp):
        val = val + parts[j][0:n_rows, :] * fac[:, j:j + 1]
    attn[0] = val

    swap = rcopy(attn.at[0], abuf.at[core], ab_s, ab_r, sp=partner)
    swap.start()
    abuf[core] = val
    swap.wait()
    flat = abuf.reshape(CORES * n_rows, head)
    for n in range(heads):
        lhs[:, n * head:(n + 1) * head] = flat[pl.ds(n, seqs, stride=heads), :].astype(BF16)

    def ysend(d):
        return rcopy(pbuf.at[d], ybuf.at[d], y_s.at[d], y_r.at[d], tp=yat(d))

    def proj(j):
        wcopy(j).wait()
        pbuf[j] = jnp.dot(lhs[...], wbuf[j], preferred_element_type=F32)

    for j in order:
        proj(j)
        if j:
            ysend(j).start()
    hcopy.wait()
    tot = pbuf[0]
    for d in range(1, n_tp):
        ysend(d).wait_recv()
        tot = tot + ybuf[d]
    out_ref[ds(x * seqs, seqs, seqs), ds((core * n_tp + y) * cols, cols, cols)] = hbuf[...].astype(F32) + tot

    def block(dy, dx, part):
        by = lax.rem(y + n_tp - dy, n_tp)
        bx = lax.rem(x + nx - dx, nx)
        return out_ref.at[ds(bx * seqs + part * per, per, per), ds((core * n_tp + by) * cols, cols, cols)]

    sends = []

    def go(dy, dx, part, sems, where, ty, tx):
        ref = block(dy, dx, part)
        cp = rcopy(ref, ref, sems[0].at[ty, tx], sems[1].at[ty, tx], **where)
        cp.start()
        sends.append(cp)

    def fwd(dy, dx, part):
        if part == 0 and dx == 0:
            for e in range(1, nx):
                go(dy, 0, 0, (a_s, a_r), {'sp': xat(e)}, dy, e)
        if part == 1 and dy == 0:
            for e in range(1, n_tp):
                go(0, dx, 1, (b_s, b_r), {'tp': yat(e)}, e, dx)
        ref = block(dy, dx, part)
        cp = rcopy(ref, ref, d_s.at[part, dy, dx], d_r.at[part, dy, dx], sp=partner)
        cp.start()
        sends.append(cp)

    for e in range(1, n_tp):
        go(0, 0, 0, (a_s, a_r), {'tp': yat(e)}, e, 0)
    for e in range(1, nx):
        go(0, 0, 1, (b_s, b_r), {'sp': xat(e)}, 0, e)
    fwd(0, 0, 0)
    fwd(0, 0, 1)

    def arrive(dy, dx, part):
        ref = block(dy, dx, part)
        r = (a_r, b_r)[part].at[dy, dx]
        q = (a_s, b_s)[part].at[dy, dx]
        rcopy(ref, ref, q, r, sp=partner).wait_recv()
        fwd(dy, dx, part)

    for e in range(1, max(n_tp, nx)):
        if e < n_tp:
            arrive(e, 0, 0)
        if e < nx:
            arrive(0, e, 1)
    for dy in range(n_tp):
        for e in range(1, nx):
            arrive(dy, e, 0)
    for dx in range(nx):
        for e in range(1, n_tp):
            arrive(e, dx, 1)
    for part in range(2):
        for dy in range(n_tp):
            for dx in range(nx):
                by = lax.rem(y + n_tp - dy, n_tp)
                bx = lax.rem(x + nx - dx, nx)
                ref = out_ref.at[ds(bx * seqs + part * per, per, per),
                                 ds(((1 - core) * n_tp + by) * cols, cols, cols)]
                rcopy(ref, ref, d_s.at[part, dy, dx], d_r.at[part, dy, dx], sp=partner).wait_recv()
    for cp in sends:
        cp.wait_send()
    for d in range(1, n_sp):
        rs(d).wait_send()
    for d in range(1, n_tp):
        ysend(d).wait_send()


def solution(mesh):
    n_tp, n_sp = mesh.shape['tp'], mesh.shape['sp']
    cache_spec = P('dp', 'sp', 'tp', None)
    DMA = pltpu.SemaphoreType.DMA

    def local_step(hidden, norm_scale, w_qkv, w_out, k_cache, v_cache, positions):
        n_seq, seq_local, kv_local, head = k_cache.shape
        d_model = hidden.shape[1]
        q_per_kv = w_qkv.shape[1] // (kv_local * head) - 2
        heads = kv_local * q_per_kv
        grp_cols = (q_per_kv + 2) * head
        n_blk, n_half = (q_per_kv + 2) // 2, 2
        pitch = n_seq + 8
        per = n_seq // n_sp
        n_rows = per * heads
        flat = (n_seq, seq_local * kv_local, head)
        vmem_cache = pltpu.VMEM(flat, BF16)
        hbm_cache = jax.ShapeDtypeStruct(flat, BF16)

        qkv, k_now, v_now = pl.pallas_call(
            functools.partial(qkv_kernel, (q_per_kv, head, pitch)),
            out_shape=(pltpu.VMEM((kv_local, pitch * (q_per_kv + 2), head), F32), vmem_cache, vmem_cache),
            in_specs=[HBM] * 6,
            out_specs=(VMEM, VMEM, VMEM),
            scratch_shapes=[
                pltpu.VMEM(hidden.shape, BF16),
                pltpu.VMEM((d_model // 128, 128), BF16),
                pltpu.VMEM((1, n_seq), jnp.int32),
                pltpu.VMEM((n_blk, n_half, d_model // n_half, grp_cols // n_blk), BF16),
                pltpu.VMEM((n_seq, d_model), BF16),
                pltpu.VMEM((d_model // 128, 128), F32),
                DMA((3,)), DMA((n_blk, n_half)), DMA((2,)),
                DMA((q_per_kv + 2,)), DMA((q_per_kv + 2,)),
            ],
            compiler_params=pltpu.CompilerParams(
                collective_id=0, has_side_effects=True, vmem_limit_bytes=28 * MIB),
            name='qkv',
        )(in_hbm(hidden), in_hbm(norm_scale.reshape(d_model // 128, 128)),
          in_hbm(positions.reshape(1, n_seq)), in_hbm(w_qkv), in_hbm(k_cache.reshape(flat)),
          in_hbm(v_cache.reshape(flat)))

        part, k_out, v_out, _, _ = pl.pallas_call(
            functools.partial(attn_kernel, (q_per_kv, head, pitch)),
            out_shape=(pltpu.VMEM((n_sp, n_rows + 8, head), F32), hbm_cache, hbm_cache, vmem_cache, vmem_cache),
            in_specs=[SMEM, VMEM, VMEM, VMEM],
            out_specs=(VMEM, HBM, HBM, VMEM, VMEM),
            input_output_aliases={2: 3, 3: 4},
            scratch_shapes=[DMA((2, n_sp))],
            compiler_params=pltpu.CompilerParams(vmem_limit_bytes=4 * MIB),
            name='attn',
        )(positions, qkv, k_now, v_now)

        nx = n_sp // CORES
        cols = d_model // (CORES * n_tp)
        depth = w_out.shape[0]
        h_out = pl.pallas_call(
            functools.partial(out_kernel, (n_tp, n_sp, heads)),
            out_shape=jax.ShapeDtypeStruct((n_seq, d_model), F32),
            in_specs=[VMEM, HBM, HBM],
            out_specs=VMEM,
            scratch_shapes=[
                pltpu.VMEM((n_sp, n_rows + 8, head), F32),
                pltpu.VMEM((CORES, n_rows, head), F32),
                pltpu.VMEM((1, n_rows, head), F32),
                pltpu.VMEM((CORES * per, depth), BF16),
                pltpu.VMEM((n_tp, depth, cols), BF16),
                pltpu.VMEM((n_tp, CORES * per, cols), F32),
                pltpu.VMEM((n_tp, CORES * per, cols), F32),
                pltpu.VMEM((CORES * per, cols), BF16),
                DMA((n_tp,)), DMA,
                DMA((n_sp,)), DMA((n_sp,)), DMA, DMA, DMA((n_tp,)), DMA((n_tp,)),
                DMA((n_tp, nx)), DMA((n_tp, nx)), DMA((n_tp, nx)), DMA((n_tp, nx)),
                DMA((2, n_tp, nx)), DMA((2, n_tp, nx)),
            ],
            compiler_params=pltpu.CompilerParams(
                collective_id=1, has_side_effects=True, vmem_limit_bytes=28 * MIB),
            name='outproj',
        )(part, in_hbm(hidden), in_hbm(w_out))
        return h_out.astype(BF16), k_out.reshape(k_cache.shape), v_out.reshape(v_cache.shape)

    return jax.shard_map(
        local_step,
        mesh=mesh,
        in_specs=(P('dp', None), P(None), P(None, 'tp'), P('tp', None), cache_spec, cache_spec, P('dp')),
        out_specs=(P('dp', None), cache_spec, cache_spec),
        check_vma=False,
    )
```

```python
import functools
import math

import jax
import jax.numpy as jnp
from jax import lax
from jax.experimental import pallas as pl
from jax.experimental.pallas import tpu as pltpu
from jax.sharding import PartitionSpec as P

MESH = pl.DeviceIdType.MESH
F32 = jnp.float32
BF16 = jnp.bfloat16
HBM = pl.BlockSpec(memory_space=pltpu.HBM)
VMEM = pl.BlockSpec(memory_space=pltpu.VMEM)
SMEM = pl.BlockSpec(memory_space=pltpu.SMEM)
CORES = 2
CACHE_STEP = 4
MIB = 1024 * 1024


def in_hbm(val):
    return pltpu.with_memory_space_constraint(val, pltpu.HBM)


def ds(start, size, align):
    return pl.ds(pl.multiple_of(start, align), size)


def rcopy(src, dst, send_sem, recv_sem, **where):
    return pltpu.make_async_remote_copy(
        src_ref=src, dst_ref=dst, send_sem=send_sem, recv_sem=recv_sem,
        device_id=where, device_id_type=MESH,
    )


def qkv_kernel(dims, h_hbm, scale_hbm, pos_hbm, w_ref, k_hbm, v_hbm, out_ref, kbuf, vbuf, h_ref, scale_ref, pos_ref,
               wbuf, u_ref, acc, gain, hsem, wsem, csem, s_part, r_part):
    n_seq, d_model = h_ref.shape
    q_per_kv, head, pitch = dims
    n_blk, blk, grp = wbuf.shape
    s = lax.axis_index('sp')
    core = lax.rem(s, CORES)
    partner = s + 1 - 2 * core

    def wload(i):
        return pltpu.make_async_copy(
            w_ref.at[ds(i * blk, blk, blk), ds(core * grp, grp, 128)], wbuf.at[i], wsem.at[i])

    loads = [
        pltpu.make_async_copy(src, dst, hsem.at[i])
        for i, (src, dst) in enumerate(((h_hbm, h_ref), (scale_hbm, scale_ref), (pos_hbm, pos_ref)))
    ]
    caches = [
        pltpu.make_async_copy(src, dst, csem.at[i]) for i, (src, dst) in enumerate(((k_hbm, kbuf), (v_hbm, vbuf)))
    ]
    for load in loads:
        load.start()
    for i in range(n_blk):
        wload(i).start()
    barrier = pltpu.get_barrier_semaphore()
    pl.semaphore_signal(barrier, inc=1, device_id={'sp': partner}, device_id_type=MESH)
    for load in loads:
        load.wait()

    lanes = 128
    zero = jnp.zeros((n_seq, lanes), F32)

    def add_sum(i, tot):
        return tot + h_ref[:, ds(i * lanes, lanes, lanes)].astype(F32)

    mean = jnp.sum(lax.fori_loop(0, d_model // lanes, add_sum, zero, unroll=8), axis=1, keepdims=True) / d_model

    def add_sq(i, tot):
        cent = h_ref[:, ds(i * lanes, lanes, lanes)].astype(F32) - mean
        return tot + cent * cent

    var = jnp.sum(lax.fori_loop(0, d_model // lanes, add_sq, zero, unroll=8), axis=1, keepdims=True) / d_model
    inv = lax.rsqrt(var + 1e-5)

    gain[...] = scale_ref[...].astype(F32)

    def norm(i, carry):
        cut = ds(i * lanes, lanes, lanes)
        cent = h_ref[:, cut].astype(F32) - mean
        u_ref[:, cut] = (cent * inv * gain[pl.ds(i, 1), :]).astype(BF16)
        return carry

    lax.fori_loop(0, d_model // lanes, norm, 0, unroll=8)

    eye = lax.broadcasted_iota(jnp.int32, (n_seq, n_seq), 0) == lax.broadcasted_iota(jnp.int32, (n_seq, n_seq), 1)
    pos_col = jnp.sum(jnp.where(eye, pos_ref[...].astype(F32), 0.0), axis=1, keepdims=True)
    lane = lax.broadcasted_iota(jnp.int32, (n_seq, head), 1)
    half = head // 2
    inv_freq = jnp.exp(lax.rem(lane, half).astype(F32) * (-2.0 * math.log(500000.0) / head))
    angle = pos_col * inv_freq
    cos_t = jnp.cos(angle)
    sin_t = jnp.where(lane < half, -jnp.sin(angle), jnp.sin(angle))

    def psend(j):
        ref = out_ref.at[core, pl.ds(j * pitch, n_seq)]
        return rcopy(ref, ref, s_part.at[j], r_part.at[j], sp=partner)

    acc[...] = jnp.zeros_like(acc)

    def mm(i, carry):
        wload(i).wait()

        @pl.when(i == CACHE_STEP)
        def _():
            caches[0].start()
            caches[1].start()

        acc[...] += jnp.dot(u_ref[:, ds(i * blk, blk, blk)], wbuf[i], preferred_element_type=F32)
        return carry

    lax.fori_loop(0, n_blk, mm, 0)
    pl.semaphore_wait(barrier, 1)
    for j in range(q_per_kv + 2):
        val = jnp.clip(acc[:, j * head:(j + 1) * head].astype(BF16), -8.0, 8.0).astype(F32)
        if j < q_per_kv + 1:
            val = (val * cos_t + pltpu.roll(val, half, 1) * sin_t).astype(BF16).astype(F32)
        out_ref[core, j * pitch:j * pitch + n_seq, :] = val
        if j > 0:
            psend(j - 1).start()
    psend(q_per_kv + 1).start()
    for j in range(q_per_kv + 2):
        psend(j).wait()
    for cp in caches:
        cp.wait()


def attn_kernel(dims, pos_ref, qkv_ref, k_ref, v_ref, o_ref, ko_ref, vo_ref, kbuf, vbuf, osem):
    q_per_kv, head, pitch = dims
    n_seq, rows2, _ = kbuf.shape
    groups = qkv_ref.shape[0]
    n_grp = rows2 // groups
    n_ch = o_ref.shape[0]
    per = n_seq // n_ch
    heads = groups * q_per_kv
    base = lax.axis_index('sp') * n_grp

    def bulk(i, which):
        src, dst = ((kbuf, ko_ref), (vbuf, vo_ref))[which]
        cut = pl.ds(i * per, per)
        return pltpu.make_async_copy(src.at[cut], dst.at[cut], osem.at[which, i])

    colj = lax.broadcasted_iota(jnp.int32, (heads, rows2), 1)
    rown = lax.broadcasted_iota(jnp.int32, (heads, rows2), 0)
    same = lax.rem(colj, groups) == rown // q_per_kv
    tile = 8 * groups
    trow = lax.broadcasted_iota(jnp.int32, (tile, head), 0)
    n_rows = per * heads
    eye = lax.broadcasted_iota(jnp.int32, (n_rows, n_rows), 0) == lax.broadcasted_iota(jnp.int32, (n_rows, n_rows), 1)

    def step(i, carry):
        @pl.when(i > 0)
        def _():
            bulk(i - 1, 0).start()
            bulk(i - 1, 1).start()

        scores = []
        for t in range(per):
            b = i * per + t
            rel = pos_ref[b] - base
            here = jnp.logical_and(rel >= 0, rel < n_grp)
            at = jnp.clip(rel, 0, n_grp - 1)
            cut = ds((at // 8) * tile, tile, tile)
            hit = jnp.logical_and(trow // groups == at % 8, here)
            for src, buf, off in ((k_ref, kbuf, q_per_kv * pitch), (v_ref, vbuf, (q_per_kv + 1) * pitch)):
                new = qkv_ref[0, pl.ds(off + b, 1), :]
                for g in range(1, groups):
                    new = jnp.where(trow % groups == g, qkv_ref[g, pl.ds(off + b, 1), :], new)
                buf[b, cut, :] = jnp.where(hit, new, src[b, cut, :].astype(F32)).astype(BF16)
            q = jnp.concatenate([qkv_ref[g, pl.ds(b, q_per_kv, stride=pitch), :] for g in range(groups)], axis=0)
            sc = lax.dot_general(q.astype(BF16), kbuf[b], (((1,), (1,)), ((), ())), preferred_element_type=F32)
            ok = jnp.logical_and(same, colj < groups * (rel + 1))
            scores.append(jnp.where(ok, sc * (head ** -0.5), -1e30))
        sc = jnp.concatenate(scores, axis=0)
        top = jnp.max(sc, axis=1, keepdims=True)
        wt = jnp.exp(sc - top)
        tot = jnp.sum(wt, axis=1, keepdims=True)
        wt = wt.astype(BF16)
        for t in range(per):
            o_ref[i, t * heads:(t + 1) * heads, :] = jnp.dot(
                wt[t * heads:(t + 1) * heads], vbuf[i * per + t], preferred_element_type=F32)
        top_row = jnp.sum(jnp.where(eye, top, 0.0), axis=0, keepdims=True)
        tot_row = jnp.sum(jnp.where(eye, tot, 0.0), axis=0, keepdims=True)
        pad = jnp.zeros((6, n_rows), F32)
        o_ref[i, n_rows:n_rows + 8, :] = jnp.concatenate([top_row, tot_row, pad], axis=0)
        return carry

    lax.fori_loop(0, n_ch, step, 0)
    bulk(n_ch - 1, 0).start()
    bulk(n_ch - 1, 1).start()
    for i in range(n_ch):
        bulk(i, 0).wait()
        bulk(i, 1).wait()


def out_kernel(dims, o_ref, h_ref, w_ref, out_ref, rbuf, abuf, attn, lhs, wbuf, pbuf, ybuf, hbuf,
               wsem, hsem, rs_s, rs_r, ab_s, ab_r, y_s, y_r, a_s, a_r, b_s, b_r, d_s, d_r):
    n_tp, n_sp, heads = dims
    nx = n_sp // CORES
    y = lax.axis_index('tp')
    s = lax.axis_index('sp')
    core = lax.rem(s, CORES)
    x = s // CORES
    partner = s + 1 - 2 * core
    _, n_rows, head = attn.shape
    per = n_rows // heads
    depth, cols = wbuf.shape[1:]
    seqs = CORES * per

    def yat(d):
        return lax.rem(y + d, n_tp)

    def xat(d):
        return lax.rem(x + d, nx) * CORES + core

    def wcopy(j):
        return pltpu.make_async_copy(
            w_ref.at[:, ds((core * n_tp + yat(j)) * cols, cols, cols)], wbuf.at[j], wsem.at[j])

    hcopy = pltpu.make_async_copy(
        h_ref.at[ds(x * seqs, seqs, seqs), ds((core * n_tp + y) * cols, cols, cols)], hbuf, hsem)
    order = [d for d in range(1, n_tp)] + [0]
    for j in order:
        wcopy(j).start()
    hcopy.start()

    barrier = pltpu.get_barrier_semaphore()
    for d in range(1, n_sp):
        pl.semaphore_signal(barrier, inc=1, device_id={'sp': lax.rem(s + d, n_sp)}, device_id_type=MESH)
    for d in range(1, n_tp):
        pl.semaphore_signal(barrier, inc=1, device_id={'tp': yat(d)}, device_id_type=MESH)
    pl.semaphore_wait(barrier, n_sp + n_tp - 2)

    def rs(d):
        to = lax.rem(s + d, n_sp)
        return rcopy(o_ref.at[to], rbuf.at[d], rs_s.at[d], rs_r.at[d], sp=to)

    for d in range(1, n_sp):
        rs(d).start()
    parts = [o_ref.at[s]]
    for d in range(1, n_sp):
        rs(d).wait_recv()
        parts.append(rbuf.at[d])
    tops = [p[n_rows:n_rows + 1, :] for p in parts]
    sums = [p[n_rows + 1:n_rows + 2, :] for p in parts]
    top = functools.reduce(jnp.maximum, tops)
    facs = [jnp.exp(t - top) for t in tops]
    tot = functools.reduce(jnp.add, [f * l for f, l in zip(facs, sums)])
    fac = jnp.concatenate([f / tot for f in facs], axis=0)
    pad = jnp.zeros((n_rows - n_sp, n_rows), F32)
    fac = jnp.transpose(jnp.concatenate([fac, pad], axis=0))
    val = parts[0][0:n_rows, :] * fac[:, 0:1]
    for j in range(1, n_sp):
        val = val + parts[j][0:n_rows, :] * fac[:, j:j + 1]
    attn[0] = val

    swap = rcopy(attn.at[0], abuf.at[core], ab_s, ab_r, sp=partner)
    swap.start()
    abuf[core] = val
    swap.wait()
    flat = abuf.reshape(CORES * n_rows, head)
    for n in range(heads):
        lhs[:, n * head:(n + 1) * head] = flat[pl.ds(n, seqs, stride=heads), :].astype(BF16)

    def ysend(d):
        return rcopy(pbuf.at[d], ybuf.at[d], y_s.at[d], y_r.at[d], tp=yat(d))

    def proj(j):
        wcopy(j).wait()
        pbuf[j] = jnp.dot(lhs[...], wbuf[j], preferred_element_type=F32)

    for j in order:
        proj(j)
        if j:
            ysend(j).start()
    hcopy.wait()
    tot = pbuf[0]
    for d in range(1, n_tp):
        ysend(d).wait_recv()
        tot = tot + ybuf[d]
    out_ref[ds(x * seqs, seqs, seqs), ds((core * n_tp + y) * cols, cols, cols)] = hbuf[...].astype(F32) + tot

    def block(dy, dx, part):
        by = lax.rem(y + n_tp - dy, n_tp)
        bx = lax.rem(x + nx - dx, nx)
        return out_ref.at[ds(bx * seqs + part * per, per, per), ds((core * n_tp + by) * cols, cols, cols)]

    sends = []

    def go(dy, dx, part, sems, where, ty, tx):
        ref = block(dy, dx, part)
        cp = rcopy(ref, ref, sems[0].at[ty, tx], sems[1].at[ty, tx], **where)
        cp.start()
        sends.append(cp)

    def fwd(dy, dx, part):
        if part == 0 and dx == 0:
            for e in range(1, nx):
                go(dy, 0, 0, (a_s, a_r), {'sp': xat(e)}, dy, e)
        if part == 1 and dy == 0:
            for e in range(1, n_tp):
                go(0, dx, 1, (b_s, b_r), {'tp': yat(e)}, e, dx)
        ref = block(dy, dx, part)
        cp = rcopy(ref, ref, d_s.at[part, dy, dx], d_r.at[part, dy, dx], sp=partner)
        cp.start()
        sends.append(cp)

    for e in range(1, n_tp):
        go(0, 0, 0, (a_s, a_r), {'tp': yat(e)}, e, 0)
    for e in range(1, nx):
        go(0, 0, 1, (b_s, b_r), {'sp': xat(e)}, 0, e)
    fwd(0, 0, 0)
    fwd(0, 0, 1)

    def arrive(dy, dx, part):
        ref = block(dy, dx, part)
        r = (a_r, b_r)[part].at[dy, dx]
        q = (a_s, b_s)[part].at[dy, dx]
        rcopy(ref, ref, q, r, sp=partner).wait_recv()
        fwd(dy, dx, part)

    for e in range(1, max(n_tp, nx)):
        if e < n_tp:
            arrive(e, 0, 0)
        if e < nx:
            arrive(0, e, 1)
    for dy in range(n_tp):
        for e in range(1, nx):
            arrive(dy, e, 0)
    for dx in range(nx):
        for e in range(1, n_tp):
            arrive(e, dx, 1)
    for part in range(2):
        for dy in range(n_tp):
            for dx in range(nx):
                by = lax.rem(y + n_tp - dy, n_tp)
                bx = lax.rem(x + nx - dx, nx)
                ref = out_ref.at[ds(bx * seqs + part * per, per, per),
                                 ds(((1 - core) * n_tp + by) * cols, cols, cols)]
                rcopy(ref, ref, d_s.at[part, dy, dx], d_r.at[part, dy, dx], sp=partner).wait_recv()
    for cp in sends:
        cp.wait_send()
    for d in range(1, n_sp):
        rs(d).wait_send()
    for d in range(1, n_tp):
        ysend(d).wait_send()


def solution(mesh):
    n_tp, n_sp = mesh.shape['tp'], mesh.shape['sp']
    cache_spec = P('dp', 'sp', 'tp', None)
    DMA = pltpu.SemaphoreType.DMA

    def local_step(hidden, norm_scale, w_qkv, w_out, k_cache, v_cache, positions):
        n_seq, seq_local, kv_local, head = k_cache.shape
        d_model = hidden.shape[1]
        q_per_kv = w_qkv.shape[1] // (kv_local * head) - 2
        heads = kv_local * q_per_kv
        grp_cols = (q_per_kv + 2) * head
        n_blk = 8
        pitch = n_seq + 8
        per = n_seq // n_sp
        n_rows = per * heads
        flat = (n_seq, seq_local * kv_local, head)
        vmem_cache = pltpu.VMEM(flat, BF16)
        hbm_cache = jax.ShapeDtypeStruct(flat, BF16)

        qkv, k_now, v_now = pl.pallas_call(
            functools.partial(qkv_kernel, (q_per_kv, head, pitch)),
            out_shape=(pltpu.VMEM((kv_local, pitch * (q_per_kv + 2), head), F32), vmem_cache, vmem_cache),
            in_specs=[HBM] * 6,
            out_specs=(VMEM, VMEM, VMEM),
            scratch_shapes=[
                pltpu.VMEM(hidden.shape, BF16),
                pltpu.VMEM((d_model // 128, 128), BF16),
                pltpu.VMEM((1, n_seq), jnp.int32),
                pltpu.VMEM((n_blk, d_model // n_blk, grp_cols), BF16),
                pltpu.VMEM((n_seq, d_model), BF16),
                pltpu.VMEM((n_seq, grp_cols), F32),
                pltpu.VMEM((d_model // 128, 128), F32),
                DMA((3,)), DMA((n_blk,)), DMA((2,)),
                DMA((q_per_kv + 2,)), DMA((q_per_kv + 2,)),
            ],
            compiler_params=pltpu.CompilerParams(
                collective_id=0, has_side_effects=True, vmem_limit_bytes=28 * MIB),
            name='qkv',
        )(in_hbm(hidden), in_hbm(norm_scale.reshape(d_model // 128, 128)),
          in_hbm(positions.reshape(1, n_seq)), in_hbm(w_qkv), in_hbm(k_cache.reshape(flat)),
          in_hbm(v_cache.reshape(flat)))

        part, k_out, v_out, _, _ = pl.pallas_call(
            functools.partial(attn_kernel, (q_per_kv, head, pitch)),
            out_shape=(pltpu.VMEM((n_sp, n_rows + 8, head), F32), hbm_cache, hbm_cache, vmem_cache, vmem_cache),
            in_specs=[SMEM, VMEM, VMEM, VMEM],
            out_specs=(VMEM, HBM, HBM, VMEM, VMEM),
            input_output_aliases={2: 3, 3: 4},
            scratch_shapes=[DMA((2, n_sp))],
            compiler_params=pltpu.CompilerParams(vmem_limit_bytes=4 * MIB),
            name='attn',
        )(positions, qkv, k_now, v_now)

        nx = n_sp // CORES
        cols = d_model // (CORES * n_tp)
        depth = w_out.shape[0]
        h_out = pl.pallas_call(
            functools.partial(out_kernel, (n_tp, n_sp, heads)),
            out_shape=jax.ShapeDtypeStruct((n_seq, d_model), F32),
            in_specs=[VMEM, HBM, HBM],
            out_specs=VMEM,
            scratch_shapes=[
                pltpu.VMEM((n_sp, n_rows + 8, head), F32),
                pltpu.VMEM((CORES, n_rows, head), F32),
                pltpu.VMEM((1, n_rows, head), F32),
                pltpu.VMEM((CORES * per, depth), BF16),
                pltpu.VMEM((n_tp, depth, cols), BF16),
                pltpu.VMEM((n_tp, CORES * per, cols), F32),
                pltpu.VMEM((n_tp, CORES * per, cols), F32),
                pltpu.VMEM((CORES * per, cols), BF16),
                DMA((n_tp,)), DMA,
                DMA((n_sp,)), DMA((n_sp,)), DMA, DMA, DMA((n_tp,)), DMA((n_tp,)),
                DMA((n_tp, nx)), DMA((n_tp, nx)), DMA((n_tp, nx)), DMA((n_tp, nx)),
                DMA((2, n_tp, nx)), DMA((2, n_tp, nx)),
            ],
            compiler_params=pltpu.CompilerParams(
                collective_id=1, has_side_effects=True, vmem_limit_bytes=28 * MIB),
            name='outproj',
        )(part, in_hbm(hidden), in_hbm(w_out))
        return h_out.astype(BF16), k_out.reshape(k_cache.shape), v_out.reshape(v_cache.shape)

    return jax.shard_map(
        local_step,
        mesh=mesh,
        in_specs=(P('dp', None), P(None), P(None, 'tp'), P('tp', None), cache_spec, cache_spec, P('dp')),
        out_specs=(P('dp', None), cache_spec, cache_spec),
        check_vma=False,
    )
```

```python
import functools
import math

import jax
import jax.numpy as jnp
from jax import lax
from jax.experimental import pallas as pl
from jax.experimental.pallas import tpu as pltpu
from jax.sharding import PartitionSpec as P

MESH = pl.DeviceIdType.MESH
F32 = jnp.float32
BF16 = jnp.bfloat16
HBM = pl.BlockSpec(memory_space=pltpu.HBM)
VMEM = pl.BlockSpec(memory_space=pltpu.VMEM)
SMEM = pl.BlockSpec(memory_space=pltpu.SMEM)
CORES = 2
CACHE_STEP = 4
MIB = 1024 * 1024


def in_hbm(val):
    return pltpu.with_memory_space_constraint(val, pltpu.HBM)


def ds(start, size, align):
    return pl.ds(pl.multiple_of(start, align), size)


def rcopy(src, dst, send_sem, recv_sem, **where):
    return pltpu.make_async_remote_copy(
        src_ref=src, dst_ref=dst, send_sem=send_sem, recv_sem=recv_sem,
        device_id=where, device_id_type=MESH,
    )


def main_kernel(dims, pos_smem, h_hbm, scale_hbm, pos_hbm, w_ref, k_hbm, v_hbm, wo_ref, out_ref, kbuf, vbuf, res_ref,
                h_ref, scale_ref, pos_ref, wbuf, u_ref, acc, gain, o_ref, rbuf, abuf, attn, lhs, wobuf, pbuf, ybuf, hbuf,
                hsem, wsem, csem, s_part, r_part, wosem, hosem, rs_s, rs_r, ab_s, ab_r, y_s, y_r, a_s, a_r, b_s, b_r,
                d_s, d_r):
    n_seq, d_model = h_ref.shape
    q_per_kv, head, pitch, n_tp, n_sp = dims
    n_blk, blk, grp = wbuf.shape
    groups = out_ref.shape[0]
    heads = groups * q_per_kv
    rows2 = kbuf.shape[1]
    n_grp = rows2 // groups
    nx = n_sp // CORES
    y = lax.axis_index('tp')
    s = lax.axis_index('sp')
    core = lax.rem(s, CORES)
    x = s // CORES
    partner = s + 1 - 2 * core
    n_rows = attn.shape[1]
    per = n_rows // heads
    cols = wobuf.shape[2]
    seqs = CORES * per
    base = s * n_grp

    def yat(d):
        return lax.rem(y + d, n_tp)

    def xat(d):
        return lax.rem(x + d, nx) * CORES + core

    def wload(i):
        return pltpu.make_async_copy(
            w_ref.at[ds(i * blk, blk, blk), ds(core * grp, grp, 128)], wbuf.at[i], wsem.at[i])

    def wcopy(j):
        return pltpu.make_async_copy(
            wo_ref.at[:, ds((core * n_tp + yat(j)) * cols, cols, cols)], wobuf.at[j], wosem.at[j])

    def chunk_of(d):
        return lax.rem(s + d, n_sp)

    def ccopy(d, which):
        src, dst = ((k_hbm, kbuf), (v_hbm, vbuf))[which]
        cut = pl.ds(chunk_of(d) * per, per)
        return pltpu.make_async_copy(src.at[cut], dst.at[cut], csem.at[which, d])

    def owner(t):
        return 1 + (t + n_sp // 2 - 2) % (n_sp - 1)

    hcopy = pltpu.make_async_copy(
        h_hbm.at[ds(x * seqs, seqs, seqs), ds((core * n_tp + y) * cols, cols, cols)], hbuf, hosem)
    order = [d for d in range(1, n_tp)] + [0]
    loads = [
        pltpu.make_async_copy(src, dst, hsem.at[i])
        for i, (src, dst) in enumerate(((h_hbm, h_ref), (scale_hbm, scale_ref), (pos_hbm, pos_ref)))
    ]
    for load in loads:
        load.start()
    for i in range(n_blk):
        wload(i).start()
    barrier = pltpu.get_barrier_semaphore()
    for d in range(1, n_sp):
        pl.semaphore_signal(barrier, inc=1, device_id={'sp': lax.rem(s + d, n_sp)}, device_id_type=MESH)
    for d in range(1, n_tp):
        pl.semaphore_signal(barrier, inc=1, device_id={'tp': yat(d)}, device_id_type=MESH)
    for load in loads:
        load.wait()

    lanes = 128
    zero = jnp.zeros((n_seq, lanes), F32)

    def add_sum(i, tot):
        return tot + h_ref[:, ds(i * lanes, lanes, lanes)].astype(F32)

    mean = jnp.sum(lax.fori_loop(0, d_model // lanes, add_sum, zero, unroll=8), axis=1, keepdims=True) / d_model

    def add_sq(i, tot):
        cent = h_ref[:, ds(i * lanes, lanes, lanes)].astype(F32) - mean
        return tot + cent * cent

    var = jnp.sum(lax.fori_loop(0, d_model // lanes, add_sq, zero, unroll=8), axis=1, keepdims=True) / d_model
    inv = lax.rsqrt(var + 1e-5)

    gain[...] = scale_ref[...].astype(F32)

    def norm(i, carry):
        cut = ds(i * lanes, lanes, lanes)
        cent = h_ref[:, cut].astype(F32) - mean
        u_ref[:, cut] = (cent * inv * gain[pl.ds(i, 1), :]).astype(BF16)
        return carry

    lax.fori_loop(0, d_model // lanes, norm, 0, unroll=8)

    eye = lax.broadcasted_iota(jnp.int32, (n_seq, n_seq), 0) == lax.broadcasted_iota(jnp.int32, (n_seq, n_seq), 1)
    pos_col = jnp.sum(jnp.where(eye, pos_ref[...].astype(F32), 0.0), axis=1, keepdims=True)
    lane = lax.broadcasted_iota(jnp.int32, (n_seq, head), 1)
    half = head // 2
    inv_freq = jnp.exp(lax.rem(lane, half).astype(F32) * (-2.0 * math.log(500000.0) / head))
    angle = pos_col * inv_freq
    cos_t = jnp.cos(angle)
    sin_t = jnp.where(lane < half, -jnp.sin(angle), jnp.sin(angle))

    def psend(j):
        ref = out_ref.at[core, pl.ds(j * pitch, n_seq)]
        return rcopy(ref, ref, s_part.at[j], r_part.at[j], sp=partner)

    acc[...] = jnp.zeros_like(acc)

    def mm(i, carry):
        wload(i).wait()

        @pl.when(i == CACHE_STEP)
        def _():
            for d in [owner(t) for t in range(n_sp - 1)] + [0]:
                ccopy(d, 0).start()
                ccopy(d, 1).start()

        acc[...] += jnp.dot(u_ref[:, ds(i * blk, blk, blk)], wbuf[i], preferred_element_type=F32)
        return carry

    lax.fori_loop(0, n_blk, mm, 0)
    pl.semaphore_wait(barrier, n_sp + n_tp - 2)
    for j in order:
        wcopy(j).start()
    hcopy.start()
    for j in range(q_per_kv + 2):
        val = jnp.clip(acc[:, j * head:(j + 1) * head].astype(BF16), -8.0, 8.0).astype(F32)
        if j < q_per_kv + 1:
            val = (val * cos_t + pltpu.roll(val, half, 1) * sin_t).astype(BF16).astype(F32)
        out_ref[core, j * pitch:j * pitch + n_seq, :] = val
        if j > 0:
            psend(j - 1).start()
    psend(q_per_kv + 1).start()
    colj = lax.broadcasted_iota(jnp.int32, (heads, rows2), 1)
    rown = lax.broadcasted_iota(jnp.int32, (heads, rows2), 0)
    same = lax.rem(colj, groups) == rown // q_per_kv
    eye = lax.broadcasted_iota(jnp.int32, (n_rows, n_rows), 0) == lax.broadcasted_iota(jnp.int32, (n_rows, n_rows), 1)
    for j in range(q_per_kv + 2):
        psend(j).wait_recv()

    def rs(d):
        to = chunk_of(d)
        return rcopy(o_ref.at[d], rbuf.at[d], rs_s.at[d], rs_r.at[d], sp=to)

    def attend(d):
        i = chunk_of(d)
        ccopy(d, 0).wait()
        ccopy(d, 1).wait()
        scores, fresh, vals = [], [], []
        for t in range(per):
            b = i * per + t
            rel = pos_smem[b] - base
            rows = [
                jnp.concatenate([
                    jnp.broadcast_to(out_ref[g, pl.ds(off * pitch + b, 1), :], (q_per_kv, head)) for g in range(groups)
                ], axis=0) for off in (q_per_kv, q_per_kv + 1)
            ]
            q = jnp.concatenate([out_ref[g, pl.ds(b, q_per_kv, stride=pitch), :] for g in range(groups)], axis=0)
            sc = lax.dot_general(q.astype(BF16), kbuf[b], (((1,), (1,)), ((), ())), preferred_element_type=F32)
            ok = jnp.logical_and(same, colj < groups * rel)
            scores.append(jnp.where(ok, sc * (head ** -0.5), -1e30))
            own = jnp.sum(q * rows[0], axis=1, keepdims=True) * (head ** -0.5)
            at = jnp.full((heads, 1), rel, jnp.int32)
            fresh.append(jnp.where(jnp.logical_and(at >= 0, at < n_grp), own, -1e30))
            vals.append(rows[1])
        sc = jnp.concatenate(scores, axis=0)
        own = jnp.concatenate(fresh, axis=0)
        top = jnp.maximum(jnp.max(sc, axis=1, keepdims=True), own)
        wt = jnp.exp(sc - top)
        own = jnp.exp(own - top)
        tot = jnp.sum(wt, axis=1, keepdims=True) + own
        wt = wt.astype(BF16)
        own = own.astype(BF16).astype(F32)
        for t in range(per):
            cut = slice(t * heads, (t + 1) * heads)
            o_ref[d, cut, :] = jnp.dot(
                wt[cut], vbuf[i * per + t], preferred_element_type=F32) + own[cut] * vals[t]
        top_row = jnp.sum(jnp.where(eye, top, 0.0), axis=0, keepdims=True)
        tot_row = jnp.sum(jnp.where(eye, tot, 0.0), axis=0, keepdims=True)
        pad = jnp.zeros((6, n_rows), F32)
        o_ref[d, n_rows:n_rows + 8, :] = jnp.concatenate([top_row, tot_row, pad], axis=0)

    def sweep(t, carry):
        d = owner(t)
        attend(d)
        rs(d).start()
        return carry

    lax.fori_loop(0, n_sp - 1, sweep, 0)
    attend(0)
    parts = [o_ref.at[0]]
    for d in range(1, n_sp):
        rs(d).wait_recv()
        parts.append(rbuf.at[d])
    tops = [p[n_rows:n_rows + 1, :] for p in parts]
    sums = [p[n_rows + 1:n_rows + 2, :] for p in parts]
    top = functools.reduce(jnp.maximum, tops)
    facs = [jnp.exp(t - top) for t in tops]
    tot = functools.reduce(jnp.add, [f * l for f, l in zip(facs, sums)])
    fac = jnp.concatenate([f / tot for f in facs], axis=0)
    pad = jnp.zeros((n_rows - n_sp, n_rows), F32)
    fac = jnp.transpose(jnp.concatenate([fac, pad], axis=0))
    val = parts[0][0:n_rows, :] * fac[:, 0:1]
    for j in range(1, n_sp):
        val = val + parts[j][0:n_rows, :] * fac[:, j:j + 1]
    attn[0] = val

    swap = rcopy(attn.at[0], abuf.at[core], ab_s, ab_r, sp=partner)
    swap.start()
    abuf[core] = val
    swap.wait()
    flat = abuf.reshape(CORES * n_rows, head)
    for n in range(heads):
        lhs[:, n * head:(n + 1) * head] = flat[pl.ds(n, seqs, stride=heads), :].astype(BF16)

    def ysend(d):
        return rcopy(pbuf.at[d], ybuf.at[d], y_s.at[d], y_r.at[d], tp=yat(d))

    def proj(j):
        wcopy(j).wait()
        pbuf[j] = jnp.dot(lhs[...], wobuf[j], preferred_element_type=F32)

    for j in order:
        proj(j)
        if j:
            ysend(j).start()
    hcopy.wait()
    tot = pbuf[0]
    for d in range(1, n_tp):
        ysend(d).wait_recv()
        tot = tot + ybuf[d]
    res_ref[ds(x * seqs, seqs, seqs), ds((core * n_tp + y) * cols, cols, cols)] = hbuf[...].astype(F32) + tot

    def block(dy, dx, part):
        by = lax.rem(y + n_tp - dy, n_tp)
        bx = lax.rem(x + nx - dx, nx)
        return res_ref.at[ds(bx * seqs + part * per, per, per), ds((core * n_tp + by) * cols, cols, cols)]

    sends = []

    def go(dy, dx, part, sems, where, ty, tx):
        ref = block(dy, dx, part)
        cp = rcopy(ref, ref, sems[0].at[ty, tx], sems[1].at[ty, tx], **where)
        cp.start()
        sends.append(cp)

    def fwd(dy, dx, part):
        if part == 0 and dx == 0:
            for e in range(1, nx):
                go(dy, 0, 0, (a_s, a_r), {'sp': xat(e)}, dy, e)
        if part == 1 and dy == 0:
            for e in range(1, n_tp):
                go(0, dx, 1, (b_s, b_r), {'tp': yat(e)}, e, dx)
        ref = block(dy, dx, part)
        cp = rcopy(ref, ref, d_s.at[part, dy, dx], d_r.at[part, dy, dx], sp=partner)
        cp.start()
        sends.append(cp)

    for e in range(1, n_tp):
        go(0, 0, 0, (a_s, a_r), {'tp': yat(e)}, e, 0)
    for e in range(1, nx):
        go(0, 0, 1, (b_s, b_r), {'sp': xat(e)}, 0, e)
    fwd(0, 0, 0)
    fwd(0, 0, 1)

    def arrive(dy, dx, part):
        ref = block(dy, dx, part)
        r = (a_r, b_r)[part].at[dy, dx]
        q = (a_s, b_s)[part].at[dy, dx]
        rcopy(ref, ref, q, r, sp=partner).wait_recv()
        fwd(dy, dx, part)

    for e in range(1, max(n_tp, nx)):
        if e < n_tp:
            arrive(e, 0, 0)
        if e < nx:
            arrive(0, e, 1)
    for dy in range(n_tp):
        for e in range(1, nx):
            arrive(dy, e, 0)
    for dx in range(nx):
        for e in range(1, n_tp):
            arrive(e, dx, 1)
    for part in range(2):
        for dy in range(n_tp):
            for dx in range(nx):
                by = lax.rem(y + n_tp - dy, n_tp)
                bx = lax.rem(x + nx - dx, nx)
                ref = res_ref.at[ds(bx * seqs + part * per, per, per),
                                 ds(((1 - core) * n_tp + by) * cols, cols, cols)]
                rcopy(ref, ref, d_s.at[part, dy, dx], d_r.at[part, dy, dx], sp=partner).wait_recv()
    for cp in sends:
        cp.wait_send()
    for d in range(1, n_sp):
        rs(d).wait_send()
    for d in range(1, n_tp):
        ysend(d).wait_send()
    for j in range(q_per_kv + 2):
        psend(j).wait_send()


def write_kernel(dims, pos_ref, qkv_ref, res_ref, k_ref, v_ref, h_out, ko_ref, vo_ref, kbuf, vbuf, hbuf, osem, hsem):
    q_per_kv, head, pitch, n_ch = dims
    n_seq, rows2, _ = kbuf.shape
    groups = qkv_ref.shape[0]
    n_grp = rows2 // groups
    per = n_seq // n_ch
    base = lax.axis_index('sp') * n_grp
    tile = 8 * groups
    trow = lax.broadcasted_iota(jnp.int32, (tile, head), 0)

    def bulk(i, which):
        src, dst = ((kbuf, ko_ref), (vbuf, vo_ref))[which]
        cut = pl.ds(i * per, per)
        return pltpu.make_async_copy(src.at[cut], dst.at[cut], osem.at[which, i])

    def hwrite(i):
        cut = pl.ds(i * 16, 16)
        return pltpu.make_async_copy(hbuf.at[cut], h_out.at[cut], hsem.at[i])

    def step(i, carry):
        for t in range(per):
            b = i * per + t
            rel = pos_ref[b] - base
            here = jnp.logical_and(rel >= 0, rel < n_grp)
            at = jnp.clip(rel, 0, n_grp - 1)
            cut = ds((at // 8) * tile, tile, tile)
            hit = jnp.logical_and(trow // groups == at % 8, here)
            for src, buf, off in ((k_ref, kbuf, q_per_kv * pitch), (v_ref, vbuf, (q_per_kv + 1) * pitch)):
                new = qkv_ref[0, pl.ds(off + b, 1), :]
                for g in range(1, groups):
                    new = jnp.where(trow % groups == g, qkv_ref[g, pl.ds(off + b, 1), :], new)
                buf[b, cut, :] = jnp.where(hit, new, src[b, cut, :].astype(F32)).astype(BF16)

        @pl.when(i > 0)
        def _():
            bulk(i - 1, 0).start()
            bulk(i - 1, 1).start()

        return carry

    lax.fori_loop(0, n_ch, step, 0)
    bulk(n_ch - 1, 0).start()
    bulk(n_ch - 1, 1).start()
    n_h = n_seq // 16
    for i in range(n_h):
        hbuf[i * 16:(i + 1) * 16, :] = res_ref[i * 16:(i + 1) * 16, :].astype(BF16)
        if i > 0:
            hwrite(i - 1).start()
    hwrite(n_h - 1).start()
    for i in range(n_ch):
        bulk(i, 0).wait()
        bulk(i, 1).wait()
    for i in range(n_h):
        hwrite(i).wait()


def solution(mesh):
    n_tp, n_sp = mesh.shape['tp'], mesh.shape['sp']
    cache_spec = P('dp', 'sp', 'tp', None)
    DMA = pltpu.SemaphoreType.DMA

    def local_step(hidden, norm_scale, w_qkv, w_out, k_cache, v_cache, positions):
        n_seq, seq_local, kv_local, head = k_cache.shape
        d_model = hidden.shape[1]
        q_per_kv = w_qkv.shape[1] // (kv_local * head) - 2
        heads = kv_local * q_per_kv
        grp_cols = (q_per_kv + 2) * head
        n_blk = 8
        pitch = n_seq + 8
        per = n_seq // n_sp
        n_rows = per * heads
        flat = (n_seq, seq_local * kv_local, head)
        vmem_cache = pltpu.VMEM(flat, BF16)
        hbm_cache = jax.ShapeDtypeStruct(flat, BF16)

        nx = n_sp // CORES
        cols = d_model // (CORES * n_tp)
        depth = w_out.shape[0]
        qkv, k_now, v_now, res = pl.pallas_call(
            functools.partial(main_kernel, (q_per_kv, head, pitch, n_tp, n_sp)),
            out_shape=(pltpu.VMEM((kv_local, pitch * (q_per_kv + 2), head), F32), vmem_cache, vmem_cache,
                       pltpu.VMEM((n_seq, d_model), F32)),
            in_specs=[SMEM] + [HBM] * 7,
            out_specs=(VMEM,) * 4,
            scratch_shapes=[
                pltpu.VMEM(hidden.shape, BF16),
                pltpu.VMEM((d_model // 128, 128), BF16),
                pltpu.VMEM((1, n_seq), jnp.int32),
                pltpu.VMEM((n_blk, d_model // n_blk, grp_cols), BF16),
                pltpu.VMEM((n_seq, d_model), BF16),
                pltpu.VMEM((n_seq, grp_cols), F32),
                pltpu.VMEM((d_model // 128, 128), F32),
                pltpu.VMEM((n_sp, n_rows + 8, head), F32),
                pltpu.VMEM((n_sp, n_rows + 8, head), F32),
                pltpu.VMEM((CORES, n_rows, head), F32),
                pltpu.VMEM((1, n_rows, head), F32),
                pltpu.VMEM((CORES * per, depth), BF16),
                pltpu.VMEM((n_tp, depth, cols), BF16),
                pltpu.VMEM((n_tp, CORES * per, cols), F32),
                pltpu.VMEM((n_tp, CORES * per, cols), F32),
                pltpu.VMEM((CORES * per, cols), BF16),
                DMA((3,)), DMA((n_blk,)), DMA((2, n_sp)), DMA((q_per_kv + 2,)), DMA((q_per_kv + 2,)),
                DMA((n_tp,)), DMA,
                DMA((n_sp,)), DMA((n_sp,)), DMA, DMA, DMA((n_tp,)), DMA((n_tp,)),
                DMA((n_tp, nx)), DMA((n_tp, nx)), DMA((n_tp, nx)), DMA((n_tp, nx)),
                DMA((2, n_tp, nx)), DMA((2, n_tp, nx)),
            ],
            compiler_params=pltpu.CompilerParams(
                collective_id=0, has_side_effects=True, vmem_limit_bytes=46 * MIB),
            name='main',
        )(positions, in_hbm(hidden), in_hbm(norm_scale.reshape(d_model // 128, 128)),
          in_hbm(positions.reshape(1, n_seq)), in_hbm(w_qkv), in_hbm(k_cache.reshape(flat)),
          in_hbm(v_cache.reshape(flat)), in_hbm(w_out))

        h_out, k_out, v_out, _, _ = pl.pallas_call(
            functools.partial(write_kernel, (q_per_kv, head, pitch, n_sp)),
            out_shape=(jax.ShapeDtypeStruct(hidden.shape, BF16), hbm_cache, hbm_cache, vmem_cache, vmem_cache),
            in_specs=[SMEM, VMEM, VMEM, VMEM, VMEM],
            out_specs=(HBM, HBM, HBM, VMEM, VMEM),
            input_output_aliases={3: 3, 4: 4},
            scratch_shapes=[pltpu.VMEM(hidden.shape, BF16), DMA((2, n_sp)), DMA((n_seq // 16,))],
            compiler_params=pltpu.CompilerParams(vmem_limit_bytes=4 * MIB),
            name='write',
        )(positions, qkv, res, k_now, v_now)
        return h_out, k_out.reshape(k_cache.shape), v_out.reshape(v_cache.shape)

    return jax.shard_map(
        local_step,
        mesh=mesh,
        in_specs=(P('dp', None), P(None), P(None, 'tp'), P('tp', None), cache_spec, cache_spec, P('dp')),
        out_specs=(P('dp', None), cache_spec, cache_spec),
        check_vma=False,
    )
```

```python
import functools
import math

import jax
import jax.numpy as jnp
from jax import lax
from jax.experimental import pallas as pl
from jax.experimental.pallas import tpu as pltpu
from jax.sharding import PartitionSpec as P

MESH = pl.DeviceIdType.MESH
F32 = jnp.float32
BF16 = jnp.bfloat16
HBM = pl.BlockSpec(memory_space=pltpu.HBM)
VMEM = pl.BlockSpec(memory_space=pltpu.VMEM)
SMEM = pl.BlockSpec(memory_space=pltpu.SMEM)
CORES = 2
CACHE_STEP = 10
MIB = 1024 * 1024


def in_hbm(val):
    return pltpu.with_memory_space_constraint(val, pltpu.HBM)


def ds(start, size, align):
    return pl.ds(pl.multiple_of(start, align), size)


def rcopy(src, dst, send_sem, recv_sem, **where):
    return pltpu.make_async_remote_copy(
        src_ref=src, dst_ref=dst, send_sem=send_sem, recv_sem=recv_sem,
        device_id=where, device_id_type=MESH,
    )


def main_kernel(dims, pos_flat, h_hbm, scale_hbm, pos_hbm, w_ref, k_hbm, v_hbm, wo_ref, out_ref, kbuf, vbuf, res_ref,
                h_ref, scale_ref, pos_ref, wbuf, u_ref, acc, gain, o_ref, rbuf, abuf, attn, lhs, wobuf, pbuf, ybuf, hbuf,
                hsem, wsem, csem, s_part, r_part, wosem, hosem, rs_s, rs_r, ab_s, ab_r, y_s, y_r, a_s, a_r, b_s, b_r,
                d_s, d_r, pos_smem):
    n_seq, d_model = h_ref.shape
    q_per_kv, head, pitch, n_tp, n_sp = dims
    n_blk, blk, grp = wbuf.shape
    groups = out_ref.shape[0]
    heads = groups * q_per_kv
    rows2 = kbuf.shape[1]
    n_grp = rows2 // groups
    nx = n_sp // CORES
    y = lax.axis_index('tp')
    s = lax.axis_index('sp')
    core = lax.rem(s, CORES)
    x = s // CORES
    partner = s + 1 - 2 * core
    n_rows = attn.shape[1]
    per = n_rows // heads
    cols = wobuf.shape[2]
    seqs = CORES * per
    base = s * n_grp

    def yat(d):
        return lax.rem(y + d, n_tp)

    def xat(d):
        return lax.rem(x + d, nx) * CORES + core

    def wload(i):
        return pltpu.make_async_copy(
            w_ref.at[ds(i * blk, blk, blk), ds(core * grp, grp, 128)], wbuf.at[i], wsem.at[i])

    def wcopy(j):
        return pltpu.make_async_copy(
            wo_ref.at[:, ds((core * n_tp + yat(j)) * cols, cols, cols)], wobuf.at[j], wosem.at[j])

    def chunk_of(d):
        return lax.rem(s + d, n_sp)

    def ccopy(d, which):
        src, dst = ((k_hbm, kbuf), (v_hbm, vbuf))[which]
        cut = pl.ds(chunk_of(d) * per, per)
        return pltpu.make_async_copy(src.at[cut], dst.at[cut], csem.at[which, d])

    def owner(t):
        return 1 + (t + n_sp // 2 - 2) % (n_sp - 1)

    hcopy = pltpu.make_async_copy(
        h_hbm.at[ds(x * seqs, seqs, seqs), ds((core * n_tp + y) * cols, cols, cols)], hbuf, hosem)
    far_tp = sorted(range(1, n_tp), key=lambda d: -min(d, n_tp - d))
    far_x = sorted(range(1, nx), key=lambda d: -min(d, nx - d))
    order = far_tp + [0]
    loads = [
        pltpu.make_async_copy(src, dst, hsem.at[i])
        for i, (src, dst) in enumerate(
            ((h_hbm, h_ref), (scale_hbm, scale_ref), (pos_hbm, pos_ref), (pos_flat, pos_smem)))
    ]
    for load in loads:
        load.start()
    for i in range(n_blk):
        wload(i).start()
    barrier = pltpu.get_barrier_semaphore()
    for d in range(1, n_sp):
        pl.semaphore_signal(barrier, inc=1, device_id={'sp': lax.rem(s + d, n_sp)}, device_id_type=MESH)
    for d in range(1, n_tp):
        pl.semaphore_signal(barrier, inc=1, device_id={'tp': yat(d)}, device_id_type=MESH)
    for load in loads:
        load.wait()

    lanes = 128
    zero = jnp.zeros((n_seq, lanes), F32)

    def add_sum(i, tot):
        return tot + h_ref[:, ds(i * lanes, lanes, lanes)].astype(F32)

    mean = jnp.sum(lax.fori_loop(0, d_model // lanes, add_sum, zero, unroll=8), axis=1, keepdims=True) / d_model

    def add_sq(i, tot):
        cent = h_ref[:, ds(i * lanes, lanes, lanes)].astype(F32) - mean
        return tot + cent * cent

    var = jnp.sum(lax.fori_loop(0, d_model // lanes, add_sq, zero, unroll=8), axis=1, keepdims=True) / d_model
    inv = lax.rsqrt(var + 1e-5)

    gain[...] = scale_ref[...].astype(F32)

    def norm(i, carry):
        cut = ds(i * lanes, lanes, lanes)
        cent = h_ref[:, cut].astype(F32) - mean
        u_ref[:, cut] = (cent * inv * gain[pl.ds(i, 1), :]).astype(BF16)
        return carry

    lax.fori_loop(0, d_model // lanes, norm, 0, unroll=8)

    eye = lax.broadcasted_iota(jnp.int32, (n_seq, n_seq), 0) == lax.broadcasted_iota(jnp.int32, (n_seq, n_seq), 1)
    pos_col = jnp.sum(jnp.where(eye, pos_ref[...].astype(F32), 0.0), axis=1, keepdims=True)
    lane = lax.broadcasted_iota(jnp.int32, (n_seq, head), 1)
    half = head // 2
    inv_freq = jnp.exp(lax.rem(lane, half).astype(F32) * (-2.0 * math.log(500000.0) / head))
    angle = pos_col * inv_freq
    cos_t = jnp.cos(angle)
    sin_t = jnp.where(lane < half, -jnp.sin(angle), jnp.sin(angle))

    def psend(j):
        ref = out_ref.at[core, pl.ds(j * pitch, n_seq)]
        return rcopy(ref, ref, s_part.at[j], r_part.at[j], sp=partner)

    acc[...] = jnp.zeros_like(acc)

    def mm(i, carry):
        wload(i).wait()

        @pl.when(i == CACHE_STEP)
        def _():
            for d in [owner(t) for t in range(n_sp - 1)] + [0]:
                ccopy(d, 0).start()
                ccopy(d, 1).start()

        acc[...] += jnp.dot(u_ref[:, ds(i * blk, blk, blk)], wbuf[i], preferred_element_type=F32)
        return carry

    lax.fori_loop(0, n_blk, mm, 0)
    pl.semaphore_wait(barrier, n_sp + n_tp - 2)
    for j in order:
        wcopy(j).start()
    hcopy.start()
    for j in range(q_per_kv + 2):
        val = jnp.clip(acc[:, j * head:(j + 1) * head].astype(BF16), -8.0, 8.0).astype(F32)
        if j < q_per_kv + 1:
            val = (val * cos_t + pltpu.roll(val, half, 1) * sin_t).astype(BF16).astype(F32)
        out_ref[core, j * pitch:j * pitch + n_seq, :] = val
        if j > 0:
            psend(j - 1).start()
    psend(q_per_kv + 1).start()
    colj = lax.broadcasted_iota(jnp.int32, (heads, rows2), 1)
    rown = lax.broadcasted_iota(jnp.int32, (heads, rows2), 0)
    same = lax.rem(colj, groups) == rown // q_per_kv
    eye = lax.broadcasted_iota(jnp.int32, (n_rows, n_rows), 0) == lax.broadcasted_iota(jnp.int32, (n_rows, n_rows), 1)
    for j in range(q_per_kv + 2):
        psend(j).wait_recv()

    def rs(d):
        to = chunk_of(d)
        return rcopy(o_ref.at[d], rbuf.at[d], rs_s.at[d], rs_r.at[d], sp=to)

    def attend(d):
        i = chunk_of(d)
        ccopy(d, 0).wait()
        ccopy(d, 1).wait()
        scores, fresh, vals = [], [], []
        for t in range(per):
            b = i * per + t
            rel = pos_smem[b] - base
            rows = [
                jnp.concatenate([
                    jnp.broadcast_to(out_ref[g, pl.ds(off * pitch + b, 1), :], (q_per_kv, head)) for g in range(groups)
                ], axis=0) for off in (q_per_kv, q_per_kv + 1)
            ]
            q = jnp.concatenate([out_ref[g, pl.ds(b, q_per_kv, stride=pitch), :] for g in range(groups)], axis=0)
            sc = lax.dot_general(q.astype(BF16), kbuf[b], (((1,), (1,)), ((), ())), preferred_element_type=F32)
            ok = jnp.logical_and(same, colj < groups * rel)
            scores.append(jnp.where(ok, sc * (head ** -0.5), -1e30))
            own = jnp.sum(q * rows[0], axis=1, keepdims=True) * (head ** -0.5)
            at = jnp.full((heads, 1), rel, jnp.int32)
            fresh.append(jnp.where(jnp.logical_and(at >= 0, at < n_grp), own, -1e30))
            vals.append(rows[1])
        sc = jnp.concatenate(scores, axis=0)
        own = jnp.concatenate(fresh, axis=0)
        top = jnp.maximum(jnp.max(sc, axis=1, keepdims=True), own)
        wt = jnp.exp(sc - top)
        own = jnp.exp(own - top)
        tot = jnp.sum(wt, axis=1, keepdims=True) + own
        wt = wt.astype(BF16)
        own = own.astype(BF16).astype(F32)
        for t in range(per):
            cut = slice(t * heads, (t + 1) * heads)
            o_ref[d, cut, :] = jnp.dot(
                wt[cut], vbuf[i * per + t], preferred_element_type=F32) + own[cut] * vals[t]
        top_row = jnp.sum(jnp.where(eye, top, 0.0), axis=0, keepdims=True)
        tot_row = jnp.sum(jnp.where(eye, tot, 0.0), axis=0, keepdims=True)
        pad = jnp.zeros((6, n_rows), F32)
        o_ref[d, n_rows:n_rows + 8, :] = jnp.concatenate([top_row, tot_row, pad], axis=0)

    def sweep(t, carry):
        d = owner(t)
        attend(d)
        rs(d).start()
        return carry

    lax.fori_loop(0, n_sp - 1, sweep, 0)
    attend(0)
    parts = [o_ref.at[0]]
    for d in range(1, n_sp):
        rs(d).wait_recv()
        parts.append(rbuf.at[d])
    tops = [p[n_rows:n_rows + 1, :] for p in parts]
    sums = [p[n_rows + 1:n_rows + 2, :] for p in parts]
    top = functools.reduce(jnp.maximum, tops)
    facs = [jnp.exp(t - top) for t in tops]
    tot = functools.reduce(jnp.add, [f * l for f, l in zip(facs, sums)])
    fac = jnp.concatenate([f / tot for f in facs], axis=0)
    pad = jnp.zeros((n_rows - n_sp, n_rows), F32)
    fac = jnp.transpose(jnp.concatenate([fac, pad], axis=0))
    val = parts[0][0:n_rows, :] * fac[:, 0:1]
    for j in range(1, n_sp):
        val = val + parts[j][0:n_rows, :] * fac[:, j:j + 1]
    attn[0] = val

    swap = rcopy(attn.at[0], abuf.at[core], ab_s, ab_r, sp=partner)
    swap.start()
    abuf[core] = val
    swap.wait()
    flat = abuf.reshape(CORES * n_rows, head)
    for n in range(heads):
        lhs[:, n * head:(n + 1) * head] = flat[pl.ds(n, seqs, stride=heads), :].astype(BF16)

    def ysend(d):
        return rcopy(pbuf.at[d], ybuf.at[d], y_s.at[d], y_r.at[d], tp=yat(d))

    def proj(j):
        wcopy(j).wait()
        pbuf[j] = jnp.dot(lhs[...], wobuf[j], preferred_element_type=F32)

    for j in order:
        proj(j)
        if j:
            ysend(j).start()
    hcopy.wait()
    tot = pbuf[0]
    for d in range(1, n_tp):
        ysend(d).wait_recv()
        tot = tot + ybuf[d]
    res_ref[ds(x * seqs, seqs, seqs), ds((core * n_tp + y) * cols, cols, cols)] = hbuf[...].astype(F32) + tot

    def block(dy, dx, part):
        by = lax.rem(y + n_tp - dy, n_tp)
        bx = lax.rem(x + nx - dx, nx)
        return res_ref.at[ds(bx * seqs + part * per, per, per), ds((core * n_tp + by) * cols, cols, cols)]

    sends = []

    def go(dy, dx, part, sems, where, ty, tx):
        ref = block(dy, dx, part)
        cp = rcopy(ref, ref, sems[0].at[ty, tx], sems[1].at[ty, tx], **where)
        cp.start()
        sends.append(cp)

    def fwd(dy, dx, part):
        if part == 0 and dx == 0:
            for e in far_x:
                go(dy, 0, 0, (a_s, a_r), {'sp': xat(e)}, dy, e)
        if part == 1 and dy == 0:
            for e in far_tp:
                go(0, dx, 1, (b_s, b_r), {'tp': yat(e)}, e, dx)
        ref = block(dy, dx, part)
        cp = rcopy(ref, ref, d_s.at[part, dy, dx], d_r.at[part, dy, dx], sp=partner)
        cp.start()
        sends.append(cp)

    for e in far_tp:
        go(0, 0, 0, (a_s, a_r), {'tp': yat(e)}, e, 0)
    for e in far_x:
        go(0, 0, 1, (b_s, b_r), {'sp': xat(e)}, 0, e)
    fwd(0, 0, 0)
    fwd(0, 0, 1)

    def arrive(dy, dx, part):
        ref = block(dy, dx, part)
        r = (a_r, b_r)[part].at[dy, dx]
        q = (a_s, b_s)[part].at[dy, dx]
        rcopy(ref, ref, q, r, sp=partner).wait_recv()
        fwd(dy, dx, part)

    def hops(item):
        dy, dx, part = item
        first = dx == 0 if part == 0 else dy == 0
        return (not first, min(dy, n_tp - dy) + min(dx, nx - dx), dy + dx)

    due = [(dy, dx, part) for dy in range(n_tp) for dx in range(nx) for part in range(2) if dy + dx > 0]
    for dy, dx, part in sorted(due, key=hops):
        arrive(dy, dx, part)
    for part in range(2):
        for dy in range(n_tp):
            for dx in range(nx):
                by = lax.rem(y + n_tp - dy, n_tp)
                bx = lax.rem(x + nx - dx, nx)
                ref = res_ref.at[ds(bx * seqs + part * per, per, per),
                                 ds(((1 - core) * n_tp + by) * cols, cols, cols)]
                rcopy(ref, ref, d_s.at[part, dy, dx], d_r.at[part, dy, dx], sp=partner).wait_recv()
    for cp in sends:
        cp.wait_send()
    for d in range(1, n_sp):
        rs(d).wait_send()
    for d in range(1, n_tp):
        ysend(d).wait_send()
    for j in range(q_per_kv + 2):
        psend(j).wait_send()


def write_kernel(dims, pos_ref, qkv_ref, res_ref, k_ref, v_ref, h_out, ko_ref, vo_ref, kbuf, vbuf, hbuf, osem, hsem):
    q_per_kv, head, pitch, n_ch = dims
    n_seq, rows2, _ = kbuf.shape
    groups = qkv_ref.shape[0]
    n_grp = rows2 // groups
    per = n_seq // n_ch
    base = lax.axis_index('sp') * n_grp
    tile = 8 * groups
    trow = lax.broadcasted_iota(jnp.int32, (tile, head), 0)

    def bulk(i, which):
        src, dst = ((kbuf, ko_ref), (vbuf, vo_ref))[which]
        cut = pl.ds(i * per, per)
        return pltpu.make_async_copy(src.at[cut], dst.at[cut], osem.at[which, i])

    def hwrite(i):
        cut = pl.ds(i * 16, 16)
        return pltpu.make_async_copy(hbuf.at[cut], h_out.at[cut], hsem.at[i])

    def step(i, carry):
        for t in range(per):
            b = i * per + t
            rel = pos_ref[b] - base
            here = jnp.logical_and(rel >= 0, rel < n_grp)
            at = jnp.clip(rel, 0, n_grp - 1)
            cut = ds((at // 8) * tile, tile, tile)
            hit = jnp.logical_and(trow // groups == at % 8, here)
            for src, buf, off in ((k_ref, kbuf, q_per_kv * pitch), (v_ref, vbuf, (q_per_kv + 1) * pitch)):
                new = qkv_ref[0, pl.ds(off + b, 1), :]
                for g in range(1, groups):
                    new = jnp.where(trow % groups == g, qkv_ref[g, pl.ds(off + b, 1), :], new)
                buf[b, cut, :] = jnp.where(hit, new, src[b, cut, :].astype(F32)).astype(BF16)

        @pl.when(i > 0)
        def _():
            bulk(i - 1, 0).start()
            bulk(i - 1, 1).start()

        return carry

    lax.fori_loop(0, n_ch, step, 0)
    bulk(n_ch - 1, 0).start()
    bulk(n_ch - 1, 1).start()
    n_h = n_seq // 16
    for i in range(n_h):
        hbuf[i * 16:(i + 1) * 16, :] = res_ref[i * 16:(i + 1) * 16, :].astype(BF16)
        if i > 0:
            hwrite(i - 1).start()
    hwrite(n_h - 1).start()
    for i in range(n_ch):
        bulk(i, 0).wait()
        bulk(i, 1).wait()
    for i in range(n_h):
        hwrite(i).wait()


def solution(mesh):
    n_tp, n_sp = mesh.shape['tp'], mesh.shape['sp']
    cache_spec = P('dp', 'sp', 'tp', None)
    DMA = pltpu.SemaphoreType.DMA

    def local_step(hidden, norm_scale, w_qkv, w_out, k_cache, v_cache, positions):
        n_seq, seq_local, kv_local, head = k_cache.shape
        d_model = hidden.shape[1]
        q_per_kv = w_qkv.shape[1] // (kv_local * head) - 2
        heads = kv_local * q_per_kv
        grp_cols = (q_per_kv + 2) * head
        n_blk = 16
        pitch = n_seq + 8
        per = n_seq // n_sp
        n_rows = per * heads
        flat = (n_seq, seq_local * kv_local, head)
        vmem_cache = pltpu.VMEM(flat, BF16)
        hbm_cache = jax.ShapeDtypeStruct(flat, BF16)

        nx = n_sp // CORES
        cols = d_model // (CORES * n_tp)
        depth = w_out.shape[0]
        qkv, k_now, v_now, res = pl.pallas_call(
            functools.partial(main_kernel, (q_per_kv, head, pitch, n_tp, n_sp)),
            out_shape=(pltpu.VMEM((kv_local, pitch * (q_per_kv + 2), head), F32), vmem_cache, vmem_cache,
                       pltpu.VMEM((n_seq, d_model), F32)),
            in_specs=[HBM] * 8,
            out_specs=(VMEM,) * 4,
            scratch_shapes=[
                pltpu.VMEM(hidden.shape, BF16),
                pltpu.VMEM((d_model // 128, 128), BF16),
                pltpu.VMEM((1, n_seq), jnp.int32),
                pltpu.VMEM((n_blk, d_model // n_blk, grp_cols), BF16),
                pltpu.VMEM((n_seq, d_model), BF16),
                pltpu.VMEM((n_seq, grp_cols), F32),
                pltpu.VMEM((d_model // 128, 128), F32),
                pltpu.VMEM((n_sp, n_rows + 8, head), F32),
                pltpu.VMEM((n_sp, n_rows + 8, head), F32),
                pltpu.VMEM((CORES, n_rows, head), F32),
                pltpu.VMEM((1, n_rows, head), F32),
                pltpu.VMEM((CORES * per, depth), BF16),
                pltpu.VMEM((n_tp, depth, cols), BF16),
                pltpu.VMEM((n_tp, CORES * per, cols), F32),
                pltpu.VMEM((n_tp, CORES * per, cols), F32),
                pltpu.VMEM((CORES * per, cols), BF16),
                DMA((4,)), DMA((n_blk,)), DMA((2, n_sp)), DMA((q_per_kv + 2,)), DMA((q_per_kv + 2,)),
                DMA((n_tp,)), DMA,
                DMA((n_sp,)), DMA((n_sp,)), DMA, DMA, DMA((n_tp,)), DMA((n_tp,)),
                DMA((n_tp, nx)), DMA((n_tp, nx)), DMA((n_tp, nx)), DMA((n_tp, nx)),
                DMA((2, n_tp, nx)), DMA((2, n_tp, nx)),
                pltpu.SMEM((n_seq,), jnp.int32),
            ],
            compiler_params=pltpu.CompilerParams(
                collective_id=0, has_side_effects=True, vmem_limit_bytes=46 * MIB),
            name='main',
        )(in_hbm(positions), in_hbm(hidden), in_hbm(norm_scale.reshape(d_model // 128, 128)),
          in_hbm(positions.reshape(1, n_seq)), in_hbm(w_qkv), in_hbm(k_cache.reshape(flat)),
          in_hbm(v_cache.reshape(flat)), in_hbm(w_out))

        h_out, k_out, v_out, _, _ = pl.pallas_call(
            functools.partial(write_kernel, (q_per_kv, head, pitch, n_sp)),
            out_shape=(jax.ShapeDtypeStruct(hidden.shape, BF16), hbm_cache, hbm_cache, vmem_cache, vmem_cache),
            in_specs=[SMEM, VMEM, VMEM, VMEM, VMEM],
            out_specs=(HBM, HBM, HBM, VMEM, VMEM),
            input_output_aliases={3: 3, 4: 4},
            scratch_shapes=[pltpu.VMEM(hidden.shape, BF16), DMA((2, n_sp)), DMA((n_seq // 16,))],
            compiler_params=pltpu.CompilerParams(vmem_limit_bytes=4 * MIB),
            name='write',
        )(positions, qkv, res, k_now, v_now)
        return h_out, k_out.reshape(k_cache.shape), v_out.reshape(v_cache.shape)

    return jax.shard_map(
        local_step,
        mesh=mesh,
        in_specs=(P('dp', None), P(None), P(None, 'tp'), P('tp', None), cache_spec, cache_spec, P('dp')),
        out_specs=(P('dp', None), cache_spec, cache_spec),
        check_vma=False,
    )
```

```python
import functools
import math

import jax
import jax.numpy as jnp
from jax import lax
from jax.experimental import pallas as pl
from jax.experimental.pallas import tpu as pltpu
from jax.sharding import PartitionSpec as P

MESH = pl.DeviceIdType.MESH
F32 = jnp.float32
BF16 = jnp.bfloat16
HBM = pl.BlockSpec(memory_space=pltpu.HBM)
VMEM = pl.BlockSpec(memory_space=pltpu.VMEM)
SMEM = pl.BlockSpec(memory_space=pltpu.SMEM)
CORES = 2
CACHE_STEP = 10
MIB = 1024 * 1024


def in_hbm(val):
    return pltpu.with_memory_space_constraint(val, pltpu.HBM)


def ds(start, size, align):
    return pl.ds(pl.multiple_of(start, align), size)


def rcopy(src, dst, send_sem, recv_sem, **where):
    return pltpu.make_async_remote_copy(
        src_ref=src, dst_ref=dst, send_sem=send_sem, recv_sem=recv_sem,
        device_id=where, device_id_type=MESH,
    )


def main_kernel(dims, pos_flat, h_hbm, scale_hbm, pos_hbm, w_ref, k_hbm, v_hbm, wo_ref, out_ref, kbuf, vbuf, res_ref,
                h_ref, scale_ref, pos_ref, wbuf, u_ref, acc, gain, o_ref, cbuf, mix, rbuf, abuf, attn, lhs, wobuf, pbuf, ybuf, hbuf,
                hsem, wsem, csem, s_part, r_part, wosem, hosem, c_s, c_r, rs_s, rs_r, ab_s, ab_r, y_s, y_r, a_s, a_r, b_s, b_r,
                d_s, d_r, pos_smem):
    n_seq, d_model = h_ref.shape
    q_per_kv, head, pitch, n_tp, n_sp = dims
    n_blk, blk, grp = wbuf.shape
    groups = out_ref.shape[0]
    heads = groups * q_per_kv
    rows2 = kbuf.shape[1]
    n_grp = rows2 // groups
    nx = n_sp // CORES
    y = lax.axis_index('tp')
    s = lax.axis_index('sp')
    core = lax.rem(s, CORES)
    x = s // CORES
    partner = s + 1 - 2 * core
    n_rows = attn.shape[1]
    per = n_rows // heads
    cols = wobuf.shape[2]
    seqs = CORES * per
    base = s * n_grp

    def yat(d):
        return lax.rem(y + d, n_tp)

    def xat(d):
        return lax.rem(x + d, nx) * CORES + core

    def wload(i):
        return pltpu.make_async_copy(
            w_ref.at[ds(i * blk, blk, blk), ds(core * grp, grp, 128)], wbuf.at[i], wsem.at[i])

    def wcopy(j):
        return pltpu.make_async_copy(
            wo_ref.at[:, ds((core * n_tp + yat(j)) * cols, cols, cols)], wobuf.at[j], wosem.at[j])

    def chunk_of(d):
        return lax.rem(x + d // CORES, nx) * CORES + (core if d % CORES == 0 else 1 - core)

    def ccopy(d, which):
        src, dst = ((k_hbm, kbuf), (v_hbm, vbuf))[which]
        cut = pl.ds(chunk_of(d) * per, per)
        return pltpu.make_async_copy(src.at[cut], dst.at[cut], csem.at[which, d])

    hcopy = pltpu.make_async_copy(
        h_hbm.at[ds(x * seqs, seqs, seqs), ds((core * n_tp + y) * cols, cols, cols)], hbuf, hosem)
    far_tp = sorted(range(1, n_tp), key=lambda d: -min(d, n_tp - d))
    far_x = sorted(range(1, nx), key=lambda d: -min(d, nx - d))
    order = far_tp + [0]
    chips = far_x + [0]
    loads = [
        pltpu.make_async_copy(src, dst, hsem.at[i])
        for i, (src, dst) in enumerate(
            ((h_hbm, h_ref), (scale_hbm, scale_ref), (pos_hbm, pos_ref), (pos_flat, pos_smem)))
    ]
    for load in loads:
        load.start()
    for i in range(n_blk):
        wload(i).start()
    barrier = pltpu.get_barrier_semaphore()
    pl.semaphore_signal(barrier, inc=1, device_id={'sp': partner}, device_id_type=MESH)
    for d in range(1, nx):
        pl.semaphore_signal(barrier, inc=1, device_id={'sp': xat(d)}, device_id_type=MESH)
    for d in range(1, n_tp):
        pl.semaphore_signal(barrier, inc=1, device_id={'tp': yat(d)}, device_id_type=MESH)
    for load in loads:
        load.wait()

    lanes = 128
    zero = jnp.zeros((n_seq, lanes), F32)

    def add_sum(i, tot):
        return tot + h_ref[:, ds(i * lanes, lanes, lanes)].astype(F32)

    mean = jnp.sum(lax.fori_loop(0, d_model // lanes, add_sum, zero, unroll=8), axis=1, keepdims=True) / d_model

    def add_sq(i, tot):
        cent = h_ref[:, ds(i * lanes, lanes, lanes)].astype(F32) - mean
        return tot + cent * cent

    var = jnp.sum(lax.fori_loop(0, d_model // lanes, add_sq, zero, unroll=8), axis=1, keepdims=True) / d_model
    inv = lax.rsqrt(var + 1e-5)

    gain[...] = scale_ref[...].astype(F32)

    def norm(i, carry):
        cut = ds(i * lanes, lanes, lanes)
        cent = h_ref[:, cut].astype(F32) - mean
        u_ref[:, cut] = (cent * inv * gain[pl.ds(i, 1), :]).astype(BF16)
        return carry

    lax.fori_loop(0, d_model // lanes, norm, 0, unroll=8)

    eye = lax.broadcasted_iota(jnp.int32, (n_seq, n_seq), 0) == lax.broadcasted_iota(jnp.int32, (n_seq, n_seq), 1)
    pos_col = jnp.sum(jnp.where(eye, pos_ref[...].astype(F32), 0.0), axis=1, keepdims=True)
    lane = lax.broadcasted_iota(jnp.int32, (n_seq, head), 1)
    half = head // 2
    inv_freq = jnp.exp(lax.rem(lane, half).astype(F32) * (-2.0 * math.log(500000.0) / head))
    angle = pos_col * inv_freq
    cos_t = jnp.cos(angle)
    sin_t = jnp.where(lane < half, -jnp.sin(angle), jnp.sin(angle))

    def psend(j):
        ref = out_ref.at[core, pl.ds(j * pitch, n_seq)]
        return rcopy(ref, ref, s_part.at[j], r_part.at[j], sp=partner)

    acc[...] = jnp.zeros_like(acc)

    def mm(i, carry):
        wload(i).wait()

        @pl.when(i == CACHE_STEP)
        def _():
            for d in [CORES * e + p for e in chips for p in (1, 0)]:
                ccopy(d, 0).start()
                ccopy(d, 1).start()

        acc[...] += jnp.dot(u_ref[:, ds(i * blk, blk, blk)], wbuf[i], preferred_element_type=F32)
        return carry

    lax.fori_loop(0, n_blk, mm, 0)
    pl.semaphore_wait(barrier, nx + n_tp - 1)
    for j in order:
        wcopy(j).start()
    hcopy.start()
    for j in range(q_per_kv + 2):
        val = jnp.clip(acc[:, j * head:(j + 1) * head].astype(BF16), -8.0, 8.0).astype(F32)
        if j < q_per_kv + 1:
            val = (val * cos_t + pltpu.roll(val, half, 1) * sin_t).astype(BF16).astype(F32)
        out_ref[core, j * pitch:j * pitch + n_seq, :] = val
        if j > 0:
            psend(j - 1).start()
    psend(q_per_kv + 1).start()
    colj = lax.broadcasted_iota(jnp.int32, (heads, rows2), 1)
    rown = lax.broadcasted_iota(jnp.int32, (heads, rows2), 0)
    same = lax.rem(colj, groups) == rown // q_per_kv
    eye = lax.broadcasted_iota(jnp.int32, (n_rows, n_rows), 0) == lax.broadcasted_iota(jnp.int32, (n_rows, n_rows), 1)
    for j in range(q_per_kv + 2):
        psend(j).wait_recv()

    def give(e):
        return rcopy(o_ref.at[CORES * e + 1], cbuf.at[e], c_s.at[e], c_r.at[e], sp=partner)

    def rs(e):
        return rcopy(mix.at[e], rbuf.at[e], rs_s.at[e], rs_r.at[e], sp=xat(e))

    def merge(parts):
        tops = [p[n_rows:n_rows + 1, :] for p in parts]
        sums = [p[n_rows + 1:n_rows + 2, :] for p in parts]
        top = functools.reduce(jnp.maximum, tops)
        facs = [jnp.exp(t - top) for t in tops]
        tot = functools.reduce(jnp.add, [f * l for f, l in zip(facs, sums)])
        return top, tot, facs

    def weigh(parts, facs):
        pad = jnp.zeros((n_rows - len(facs), n_rows), F32)
        fac = jnp.transpose(jnp.concatenate(facs + [pad], axis=0))
        return functools.reduce(
            jnp.add, [p[0:n_rows, :] * fac[:, j:j + 1] for j, p in enumerate(parts)])

    def pair(e):
        give(e).wait_recv()
        parts = [o_ref.at[CORES * e], cbuf.at[e]]
        top, tot, facs = merge(parts)
        mix[e, 0:n_rows, :] = weigh(parts, facs)
        mix[e, n_rows:n_rows + 8, :] = jnp.concatenate([top, tot, jnp.zeros((6, n_rows), F32)], axis=0)
        if e:
            rs(e).start()

    def attend(d):
        i = chunk_of(d)
        ccopy(d, 0).wait()
        ccopy(d, 1).wait()
        scores, fresh, vals = [], [], []
        for t in range(per):
            b = i * per + t
            rel = pos_smem[b] - base
            rows = [
                jnp.concatenate([
                    jnp.broadcast_to(out_ref[g, pl.ds(off * pitch + b, 1), :], (q_per_kv, head)) for g in range(groups)
                ], axis=0) for off in (q_per_kv, q_per_kv + 1)
            ]
            q = jnp.concatenate([out_ref[g, pl.ds(b, q_per_kv, stride=pitch), :] for g in range(groups)], axis=0)
            sc = lax.dot_general(q.astype(BF16), kbuf[b], (((1,), (1,)), ((), ())), preferred_element_type=F32)
            ok = jnp.logical_and(same, colj < groups * rel)
            scores.append(jnp.where(ok, sc * (head ** -0.5), -1e30))
            own = jnp.sum(q * rows[0], axis=1, keepdims=True) * (head ** -0.5)
            at = jnp.full((heads, 1), rel, jnp.int32)
            fresh.append(jnp.where(jnp.logical_and(at >= 0, at < n_grp), own, -1e30))
            vals.append(rows[1])
        sc = jnp.concatenate(scores, axis=0)
        own = jnp.concatenate(fresh, axis=0)
        top = jnp.maximum(jnp.max(sc, axis=1, keepdims=True), own)
        wt = jnp.exp(sc - top)
        own = jnp.exp(own - top)
        tot = jnp.sum(wt, axis=1, keepdims=True) + own
        wt = wt.astype(BF16)
        own = own.astype(BF16).astype(F32)
        for t in range(per):
            cut = slice(t * heads, (t + 1) * heads)
            o_ref[d, cut, :] = jnp.dot(
                wt[cut], vbuf[i * per + t], preferred_element_type=F32) + own[cut] * vals[t]
        top_row = jnp.sum(jnp.where(eye, top, 0.0), axis=0, keepdims=True)
        tot_row = jnp.sum(jnp.where(eye, tot, 0.0), axis=0, keepdims=True)
        pad = jnp.zeros((6, n_rows), F32)
        o_ref[d, n_rows:n_rows + 8, :] = jnp.concatenate([top_row, tot_row, pad], axis=0)

    last = None
    for e in chips:
        attend(CORES * e + 1)
        give(e).start()
        attend(CORES * e)
        if last is not None:
            pair(last)
        last = e
    pair(last)
    parts = [mix.at[0]]
    for e in reversed(far_x):
        rs(e).wait_recv()
        parts.append(rbuf.at[e])
    _, tot, facs = merge(parts)
    val = weigh(parts, [f / tot for f in facs])
    attn[0] = val

    swap = rcopy(attn.at[0], abuf.at[core], ab_s, ab_r, sp=partner)
    swap.start()
    abuf[core] = val
    swap.wait()
    flat = abuf.reshape(CORES * n_rows, head)
    for n in range(heads):
        lhs[:, n * head:(n + 1) * head] = flat[pl.ds(n, seqs, stride=heads), :].astype(BF16)

    def ysend(d):
        return rcopy(pbuf.at[d], ybuf.at[d], y_s.at[d], y_r.at[d], tp=yat(d))

    def proj(j):
        wcopy(j).wait()
        pbuf[j] = jnp.dot(lhs[...], wobuf[j], preferred_element_type=F32)

    for j in order:
        proj(j)
        if j:
            ysend(j).start()
    hcopy.wait()
    tot = pbuf[0]
    for d in range(1, n_tp):
        ysend(d).wait_recv()
        tot = tot + ybuf[d]
    res_ref[ds(x * seqs, seqs, seqs), ds((core * n_tp + y) * cols, cols, cols)] = hbuf[...].astype(F32) + tot

    def block(dy, dx, part):
        by = lax.rem(y + n_tp - dy, n_tp)
        bx = lax.rem(x + nx - dx, nx)
        return res_ref.at[ds(bx * seqs + part * per, per, per), ds((core * n_tp + by) * cols, cols, cols)]

    sends = []

    def go(dy, dx, part, sems, where, ty, tx):
        ref = block(dy, dx, part)
        cp = rcopy(ref, ref, sems[0].at[ty, tx], sems[1].at[ty, tx], **where)
        cp.start()
        sends.append(cp)

    def fwd(dy, dx, part):
        if part == 0 and dx == 0:
            for e in far_x:
                go(dy, 0, 0, (a_s, a_r), {'sp': xat(e)}, dy, e)
        if part == 1 and dy == 0:
            for e in far_tp:
                go(0, dx, 1, (b_s, b_r), {'tp': yat(e)}, e, dx)
        ref = block(dy, dx, part)
        cp = rcopy(ref, ref, d_s.at[part, dy, dx], d_r.at[part, dy, dx], sp=partner)
        cp.start()
        sends.append(cp)

    for e in reversed(far_tp):
        go(0, 0, 0, (a_s, a_r), {'tp': yat(e)}, e, 0)
    for e in reversed(far_x):
        go(0, 0, 1, (b_s, b_r), {'sp': xat(e)}, 0, e)
    fwd(0, 0, 0)
    fwd(0, 0, 1)

    def arrive(dy, dx, part):
        ref = block(dy, dx, part)
        r = (a_r, b_r)[part].at[dy, dx]
        q = (a_s, b_s)[part].at[dy, dx]
        rcopy(ref, ref, q, r, sp=partner).wait_recv()
        fwd(dy, dx, part)

    def hops(item):
        dy, dx, part = item
        first = dx == 0 if part == 0 else dy == 0
        return (not first, min(dy, n_tp - dy) + min(dx, nx - dx), dy + dx)

    due = [(dy, dx, part) for dy in range(n_tp) for dx in range(nx) for part in range(2) if dy + dx > 0]
    for dy, dx, part in sorted(due, key=hops):
        arrive(dy, dx, part)
    for part in range(2):
        for dy in range(n_tp):
            for dx in range(nx):
                by = lax.rem(y + n_tp - dy, n_tp)
                bx = lax.rem(x + nx - dx, nx)
                ref = res_ref.at[ds(bx * seqs + part * per, per, per),
                                 ds(((1 - core) * n_tp + by) * cols, cols, cols)]
                rcopy(ref, ref, d_s.at[part, dy, dx], d_r.at[part, dy, dx], sp=partner).wait_recv()
    for cp in sends:
        cp.wait_send()
    for e in range(1, nx):
        rs(e).wait_send()
    for e in range(nx):
        give(e).wait_send()
    for d in range(1, n_tp):
        ysend(d).wait_send()
    for j in range(q_per_kv + 2):
        psend(j).wait_send()


def write_kernel(dims, pos_ref, qkv_ref, res_ref, k_ref, v_ref, h_out, ko_ref, vo_ref, kbuf, vbuf, hbuf, osem, hsem):
    q_per_kv, head, pitch, n_ch = dims
    n_seq, rows2, _ = kbuf.shape
    groups = qkv_ref.shape[0]
    n_grp = rows2 // groups
    per = n_seq // n_ch
    base = lax.axis_index('sp') * n_grp
    tile = 8 * groups
    trow = lax.broadcasted_iota(jnp.int32, (tile, head), 0)

    def bulk(i, which):
        src, dst = ((kbuf, ko_ref), (vbuf, vo_ref))[which]
        cut = pl.ds(i * per, per)
        return pltpu.make_async_copy(src.at[cut], dst.at[cut], osem.at[which, i])

    def hwrite(i):
        cut = pl.ds(i * 16, 16)
        return pltpu.make_async_copy(hbuf.at[cut], h_out.at[cut], hsem.at[i])

    def step(i, carry):
        for t in range(per):
            b = i * per + t
            rel = pos_ref[b] - base
            here = jnp.logical_and(rel >= 0, rel < n_grp)
            at = jnp.clip(rel, 0, n_grp - 1)
            cut = ds((at // 8) * tile, tile, tile)
            hit = jnp.logical_and(trow // groups == at % 8, here)
            for src, buf, off in ((k_ref, kbuf, q_per_kv * pitch), (v_ref, vbuf, (q_per_kv + 1) * pitch)):
                new = qkv_ref[0, pl.ds(off + b, 1), :]
                for g in range(1, groups):
                    new = jnp.where(trow % groups == g, qkv_ref[g, pl.ds(off + b, 1), :], new)
                buf[b, cut, :] = jnp.where(hit, new, src[b, cut, :].astype(F32)).astype(BF16)

        @pl.when(i > 0)
        def _():
            bulk(i - 1, 0).start()
            bulk(i - 1, 1).start()

        return carry

    lax.fori_loop(0, n_ch, step, 0)
    bulk(n_ch - 1, 0).start()
    bulk(n_ch - 1, 1).start()
    n_h = n_seq // 16
    for i in range(n_h):
        hbuf[i * 16:(i + 1) * 16, :] = res_ref[i * 16:(i + 1) * 16, :].astype(BF16)
        if i > 0:
            hwrite(i - 1).start()
    hwrite(n_h - 1).start()
    for i in range(n_ch):
        bulk(i, 0).wait()
        bulk(i, 1).wait()
    for i in range(n_h):
        hwrite(i).wait()


def solution(mesh):
    n_tp, n_sp = mesh.shape['tp'], mesh.shape['sp']
    cache_spec = P('dp', 'sp', 'tp', None)
    DMA = pltpu.SemaphoreType.DMA

    def local_step(hidden, norm_scale, w_qkv, w_out, k_cache, v_cache, positions):
        n_seq, seq_local, kv_local, head = k_cache.shape
        d_model = hidden.shape[1]
        q_per_kv = w_qkv.shape[1] // (kv_local * head) - 2
        heads = kv_local * q_per_kv
        grp_cols = (q_per_kv + 2) * head
        n_blk = 16
        pitch = n_seq + 8
        per = n_seq // n_sp
        n_rows = per * heads
        flat = (n_seq, seq_local * kv_local, head)
        vmem_cache = pltpu.VMEM(flat, BF16)
        hbm_cache = jax.ShapeDtypeStruct(flat, BF16)

        nx = n_sp // CORES
        cols = d_model // (CORES * n_tp)
        depth = w_out.shape[0]
        qkv, k_now, v_now, res = pl.pallas_call(
            functools.partial(main_kernel, (q_per_kv, head, pitch, n_tp, n_sp)),
            out_shape=(pltpu.VMEM((kv_local, pitch * (q_per_kv + 2), head), F32), vmem_cache, vmem_cache,
                       pltpu.VMEM((n_seq, d_model), F32)),
            in_specs=[HBM] * 8,
            out_specs=(VMEM,) * 4,
            scratch_shapes=[
                pltpu.VMEM(hidden.shape, BF16),
                pltpu.VMEM((d_model // 128, 128), BF16),
                pltpu.VMEM((1, n_seq), jnp.int32),
                pltpu.VMEM((n_blk, d_model // n_blk, grp_cols), BF16),
                pltpu.VMEM((n_seq, d_model), BF16),
                pltpu.VMEM((n_seq, grp_cols), F32),
                pltpu.VMEM((d_model // 128, 128), F32),
                pltpu.VMEM((n_sp, n_rows + 8, head), F32),
                pltpu.VMEM((nx, n_rows + 8, head), F32),
                pltpu.VMEM((nx, n_rows + 8, head), F32),
                pltpu.VMEM((nx, n_rows + 8, head), F32),
                pltpu.VMEM((CORES, n_rows, head), F32),
                pltpu.VMEM((1, n_rows, head), F32),
                pltpu.VMEM((CORES * per, depth), BF16),
                pltpu.VMEM((n_tp, depth, cols), BF16),
                pltpu.VMEM((n_tp, CORES * per, cols), F32),
                pltpu.VMEM((n_tp, CORES * per, cols), F32),
                pltpu.VMEM((CORES * per, cols), BF16),
                DMA((4,)), DMA((n_blk,)), DMA((2, n_sp)), DMA((q_per_kv + 2,)), DMA((q_per_kv + 2,)),
                DMA((n_tp,)), DMA,
                DMA((nx,)), DMA((nx,)), DMA((nx,)), DMA((nx,)), DMA, DMA, DMA((n_tp,)), DMA((n_tp,)),
                DMA((n_tp, nx)), DMA((n_tp, nx)), DMA((n_tp, nx)), DMA((n_tp, nx)),
                DMA((2, n_tp, nx)), DMA((2, n_tp, nx)),
                pltpu.SMEM((n_seq,), jnp.int32),
            ],
            compiler_params=pltpu.CompilerParams(
                collective_id=0, has_side_effects=True, vmem_limit_bytes=46 * MIB),
            name='main',
        )(in_hbm(positions), in_hbm(hidden), in_hbm(norm_scale.reshape(d_model // 128, 128)),
          in_hbm(positions.reshape(1, n_seq)), in_hbm(w_qkv), in_hbm(k_cache.reshape(flat)),
          in_hbm(v_cache.reshape(flat)), in_hbm(w_out))

        h_out, k_out, v_out, _, _ = pl.pallas_call(
            functools.partial(write_kernel, (q_per_kv, head, pitch, n_sp)),
            out_shape=(jax.ShapeDtypeStruct(hidden.shape, BF16), hbm_cache, hbm_cache, vmem_cache, vmem_cache),
            in_specs=[SMEM, VMEM, VMEM, VMEM, VMEM],
            out_specs=(HBM, HBM, HBM, VMEM, VMEM),
            input_output_aliases={3: 3, 4: 4},
            scratch_shapes=[pltpu.VMEM(hidden.shape, BF16), DMA((2, n_sp)), DMA((n_seq // 16,))],
            compiler_params=pltpu.CompilerParams(vmem_limit_bytes=4 * MIB),
            name='write',
        )(positions, qkv, res, k_now, v_now)
        return h_out, k_out.reshape(k_cache.shape), v_out.reshape(v_cache.shape)

    return jax.shard_map(
        local_step,
        mesh=mesh,
        in_specs=(P('dp', None), P(None), P(None, 'tp'), P('tp', None), cache_spec, cache_spec, P('dp')),
        out_specs=(P('dp', None), cache_spec, cache_spec),
        check_vma=False,
    )
```

```python
import functools
import math

import jax
import jax.numpy as jnp
from jax import lax
from jax.experimental import pallas as pl
from jax.experimental.pallas import tpu as pltpu
from jax.sharding import PartitionSpec as P

MESH = pl.DeviceIdType.MESH
F32 = jnp.float32
BF16 = jnp.bfloat16
HBM = pl.BlockSpec(memory_space=pltpu.HBM)
VMEM = pl.BlockSpec(memory_space=pltpu.VMEM)
SMEM = pl.BlockSpec(memory_space=pltpu.SMEM)
CORES = 2
RING_HEADS = 1
CACHE_STEP = 10
MIB = 1024 * 1024


def in_hbm(val):
    return pltpu.with_memory_space_constraint(val, pltpu.HBM)


def ds(start, size, align):
    return pl.ds(pl.multiple_of(start, align), size)


def rcopy(src, dst, send_sem, recv_sem, **where):
    return pltpu.make_async_remote_copy(
        src_ref=src, dst_ref=dst, send_sem=send_sem, recv_sem=recv_sem,
        device_id=where, device_id_type=MESH,
    )


def main_kernel(dims, pos_flat, h_hbm, scale_hbm, pos_hbm, w_ref, k_hbm, v_hbm, wo_ref, out_ref, kbuf, vbuf, res_ref,
                h_ref, scale_ref, pos_ref, wbuf, u_ref, acc, gain, wring, o_ref, cbuf, mix, rbuf, abuf, attn, lhs, wobuf, pbuf, ybuf, hbuf,
                hsem, wsem, csem, s_part, r_part, wosem, hosem, c_s, c_r, rs_s, rs_r, ab_s, ab_r, y_s, y_r, a_s, a_r, b_s, b_r,
                d_s, d_r, pos_smem, rsem, s_ring, r_ring):
    n_seq, d_model = h_ref.shape
    q_per_kv, head, pitch, n_tp, n_sp = dims
    n_blk, blk, lcols = wbuf.shape
    n_rblk, rblk, rcols = wring.shape
    rh = rcols // head
    grp = (q_per_kv + 2) * head
    groups = out_ref.shape[0]
    heads = groups * q_per_kv
    rows2 = kbuf.shape[1]
    n_grp = rows2 // groups
    nx = n_sp // CORES
    y = lax.axis_index('tp')
    s = lax.axis_index('sp')
    core = lax.rem(s, CORES)
    x = s // CORES
    partner = s + 1 - 2 * core
    n_rows = attn.shape[1]
    per = n_rows // heads
    cols = wobuf.shape[2]
    seqs = CORES * per
    base = s * n_grp

    def yat(d):
        return lax.rem(y + d, n_tp)

    def xat(d):
        return lax.rem(x + d, nx) * CORES + core

    def wload(i):
        return pltpu.make_async_copy(
            w_ref.at[ds(i * blk, blk, blk), ds(core * grp + nx * rcols, lcols, 128)], wbuf.at[i], wsem.at[i])

    def rload(i):
        return pltpu.make_async_copy(
            w_ref.at[pl.ds(i * rblk, rblk), ds(core * grp + x * rcols, rcols, 128)], wring.at[i], rsem.at[i])

    def wcopy(j):
        return pltpu.make_async_copy(
            wo_ref.at[:, ds((core * n_tp + yat(j)) * cols, cols, cols)], wobuf.at[j], wosem.at[j])

    def chunk_of(d):
        return lax.rem(x + d // CORES, nx) * CORES + (core if d % CORES == 0 else 1 - core)

    def ccopy(d, which):
        src, dst = ((k_hbm, kbuf), (v_hbm, vbuf))[which]
        cut = pl.ds(chunk_of(d) * per, per)
        return pltpu.make_async_copy(src.at[cut], dst.at[cut], csem.at[which, d])

    hcopy = pltpu.make_async_copy(
        h_hbm.at[ds(x * seqs, seqs, seqs), ds((core * n_tp + y) * cols, cols, cols)], hbuf, hosem)
    far_tp = sorted(range(1, n_tp), key=lambda d: -min(d, n_tp - d))
    far_x = sorted(range(1, nx), key=lambda d: -min(d, nx - d))
    order = far_tp + [0]
    chips = far_x + [0]
    loads = [
        pltpu.make_async_copy(src, dst, hsem.at[i])
        for i, (src, dst) in enumerate(
            ((h_hbm, h_ref), (scale_hbm, scale_ref), (pos_hbm, pos_ref), (pos_flat, pos_smem)))
    ]
    for load in loads:
        load.start()
    for i in range(n_rblk):
        rload(i).start()
    for i in range(n_blk):
        wload(i).start()
    barrier = pltpu.get_barrier_semaphore()
    pl.semaphore_signal(barrier, inc=1, device_id={'sp': partner}, device_id_type=MESH)
    for d in range(1, nx):
        pl.semaphore_signal(barrier, inc=1, device_id={'sp': xat(d)}, device_id_type=MESH)
    for d in range(1, n_tp):
        pl.semaphore_signal(barrier, inc=1, device_id={'tp': yat(d)}, device_id_type=MESH)
    for load in loads:
        load.wait()

    lanes = 128
    zero = jnp.zeros((n_seq, lanes), F32)

    def add_sum(i, tot):
        return tot + h_ref[:, ds(i * lanes, lanes, lanes)].astype(F32)

    mean = jnp.sum(lax.fori_loop(0, d_model // lanes, add_sum, zero, unroll=8), axis=1, keepdims=True) / d_model

    def add_sq(i, tot):
        cent = h_ref[:, ds(i * lanes, lanes, lanes)].astype(F32) - mean
        return tot + cent * cent

    var = jnp.sum(lax.fori_loop(0, d_model // lanes, add_sq, zero, unroll=8), axis=1, keepdims=True) / d_model
    inv = lax.rsqrt(var + 1e-5)

    gain[...] = scale_ref[...].astype(F32)

    def norm(i, carry):
        cut = ds(i * lanes, lanes, lanes)
        cent = h_ref[:, cut].astype(F32) - mean
        u_ref[:, cut] = (cent * inv * gain[pl.ds(i, 1), :]).astype(BF16)
        return carry

    lax.fori_loop(0, d_model // lanes, norm, 0, unroll=8)

    eye = lax.broadcasted_iota(jnp.int32, (n_seq, n_seq), 0) == lax.broadcasted_iota(jnp.int32, (n_seq, n_seq), 1)
    pos_col = jnp.sum(jnp.where(eye, pos_ref[...].astype(F32), 0.0), axis=1, keepdims=True)
    lane = lax.broadcasted_iota(jnp.int32, (n_seq, head), 1)
    half = head // 2
    inv_freq = jnp.exp(lax.rem(lane, half).astype(F32) * (-2.0 * math.log(500000.0) / head))
    angle = pos_col * inv_freq
    cos_t = jnp.cos(angle)
    sin_t = jnp.where(lane < half, -jnp.sin(angle), jnp.sin(angle))

    def finish(val, rotate):
        val = jnp.clip(val.astype(BF16), -8.0, 8.0).astype(F32)
        if rotate:
            val = (val * cos_t + pltpu.roll(val, half, 1) * sin_t).astype(BF16).astype(F32)
        return val

    def slab(cx):
        return out_ref.at[core, ds(cx * rh * pitch, (rh - 1) * pitch + n_seq, 8)]

    def rsend(e):
        return rcopy(slab(x), slab(x), s_ring.at[e], r_ring.at[e], sp=xat(e))

    n_local = lcols // head

    def psend(d):
        ref = slab(lax.rem(x + nx - d, nx)) if d < nx else out_ref.at[core, pl.ds((nx * rh + d - nx) * pitch, n_seq)]
        return rcopy(ref, ref, s_part.at[d], r_part.at[d], sp=partner)

    tot = None
    for i in range(n_rblk):
        rload(i).wait()
        prod = jnp.dot(u_ref[:, i * rblk:(i + 1) * rblk], wring[i], preferred_element_type=F32)
        tot = prod if tot is None else tot + prod
    for t in range(rh):
        out_ref[core, ds((x * rh + t) * pitch, n_seq, 8), :] = finish(tot[:, t * head:(t + 1) * head], True)
    pl.semaphore_wait(barrier, nx + n_tp - 1)
    for e in far_x:
        rsend(e).start()
    psend(0).start()

    acc[...] = jnp.zeros_like(acc)

    def mm(i, carry):
        wload(i).wait()

        @pl.when(i == CACHE_STEP)
        def _():
            for d in [CORES * e + p for e in chips for p in (1, 0)]:
                ccopy(d, 0).start()
                ccopy(d, 1).start()

        acc[...] += jnp.dot(u_ref[:, ds(i * blk, blk, blk)], wbuf[i], preferred_element_type=F32)
        return carry

    lax.fori_loop(0, n_blk, mm, 0)
    for j in order:
        wcopy(j).start()
    hcopy.start()
    for t in range(n_local):
        at = nx * rh + t
        out_ref[core, at * pitch:at * pitch + n_seq, :] = finish(
            acc[:, t * head:(t + 1) * head], at < q_per_kv + 1)
        if t > 0:
            psend(nx + t - 1).start()
    psend(nx + n_local - 1).start()
    for e in reversed(far_x):
        rsend(e).wait_recv()
        psend(e).start()

    colj = lax.broadcasted_iota(jnp.int32, (heads, rows2), 1)
    rown = lax.broadcasted_iota(jnp.int32, (heads, rows2), 0)
    same = lax.rem(colj, groups) == rown // q_per_kv
    eye = lax.broadcasted_iota(jnp.int32, (n_rows, n_rows), 0) == lax.broadcasted_iota(jnp.int32, (n_rows, n_rows), 1)
    for d in range(nx + n_local):
        psend(d).wait_recv()

    def give(e):
        return rcopy(o_ref.at[CORES * e + 1], cbuf.at[e], c_s.at[e], c_r.at[e], sp=partner)

    def rs(e):
        return rcopy(mix.at[e], rbuf.at[e], rs_s.at[e], rs_r.at[e], sp=xat(e))

    def merge(parts):
        tops = [p[n_rows:n_rows + 1, :] for p in parts]
        sums = [p[n_rows + 1:n_rows + 2, :] for p in parts]
        top = functools.reduce(jnp.maximum, tops)
        facs = [jnp.exp(t - top) for t in tops]
        tot = functools.reduce(jnp.add, [f * l for f, l in zip(facs, sums)])
        return top, tot, facs

    def weigh(parts, facs):
        pad = jnp.zeros((n_rows - len(facs), n_rows), F32)
        fac = jnp.transpose(jnp.concatenate(facs + [pad], axis=0))
        return functools.reduce(
            jnp.add, [p[0:n_rows, :] * fac[:, j:j + 1] for j, p in enumerate(parts)])

    def pair(e):
        give(e).wait_recv()
        parts = [o_ref.at[CORES * e], cbuf.at[e]]
        top, tot, facs = merge(parts)
        mix[e, 0:n_rows, :] = weigh(parts, facs)
        mix[e, n_rows:n_rows + 8, :] = jnp.concatenate([top, tot, jnp.zeros((6, n_rows), F32)], axis=0)
        if e:
            rs(e).start()

    def attend(d):
        i = chunk_of(d)
        ccopy(d, 0).wait()
        ccopy(d, 1).wait()
        scores, fresh, vals = [], [], []
        for t in range(per):
            b = i * per + t
            rel = pos_smem[b] - base
            rows = [
                jnp.concatenate([
                    jnp.broadcast_to(out_ref[g, pl.ds(off * pitch + b, 1), :], (q_per_kv, head)) for g in range(groups)
                ], axis=0) for off in (q_per_kv, q_per_kv + 1)
            ]
            q = jnp.concatenate([out_ref[g, pl.ds(b, q_per_kv, stride=pitch), :] for g in range(groups)], axis=0)
            sc = lax.dot_general(q.astype(BF16), kbuf[b], (((1,), (1,)), ((), ())), preferred_element_type=F32)
            ok = jnp.logical_and(same, colj < groups * rel)
            scores.append(jnp.where(ok, sc * (head ** -0.5), -1e30))
            own = jnp.sum(q * rows[0], axis=1, keepdims=True) * (head ** -0.5)
            at = jnp.full((heads, 1), rel, jnp.int32)
            fresh.append(jnp.where(jnp.logical_and(at >= 0, at < n_grp), own, -1e30))
            vals.append(rows[1])
        sc = jnp.concatenate(scores, axis=0)
        own = jnp.concatenate(fresh, axis=0)
        top = jnp.maximum(jnp.max(sc, axis=1, keepdims=True), own)
        wt = jnp.exp(sc - top)
        own = jnp.exp(own - top)
        tot = jnp.sum(wt, axis=1, keepdims=True) + own
        wt = wt.astype(BF16)
        own = own.astype(BF16).astype(F32)
        for t in range(per):
            cut = slice(t * heads, (t + 1) * heads)
            o_ref[d, cut, :] = jnp.dot(
                wt[cut], vbuf[i * per + t], preferred_element_type=F32) + own[cut] * vals[t]
        top_row = jnp.sum(jnp.where(eye, top, 0.0), axis=0, keepdims=True)
        tot_row = jnp.sum(jnp.where(eye, tot, 0.0), axis=0, keepdims=True)
        pad = jnp.zeros((6, n_rows), F32)
        o_ref[d, n_rows:n_rows + 8, :] = jnp.concatenate([top_row, tot_row, pad], axis=0)

    last = None
    for e in chips:
        attend(CORES * e + 1)
        give(e).start()
        attend(CORES * e)
        if last is not None:
            pair(last)
        last = e
    pair(last)
    parts = [mix.at[0]]
    for e in reversed(far_x):
        rs(e).wait_recv()
        parts.append(rbuf.at[e])
    _, tot, facs = merge(parts)
    val = weigh(parts, [f / tot for f in facs])
    attn[0] = val

    swap = rcopy(attn.at[0], abuf.at[core], ab_s, ab_r, sp=partner)
    swap.start()
    abuf[core] = val
    swap.wait()
    flat = abuf.reshape(CORES * n_rows, head)
    for n in range(heads):
        lhs[:, n * head:(n + 1) * head] = flat[pl.ds(n, seqs, stride=heads), :].astype(BF16)

    def ysend(d):
        return rcopy(pbuf.at[d], ybuf.at[d], y_s.at[d], y_r.at[d], tp=yat(d))

    def proj(j):
        wcopy(j).wait()
        pbuf[j] = jnp.dot(lhs[...], wobuf[j], preferred_element_type=F32)

    for j in order:
        proj(j)
        if j:
            ysend(j).start()
    hcopy.wait()
    tot = pbuf[0]
    for d in range(1, n_tp):
        ysend(d).wait_recv()
        tot = tot + ybuf[d]
    res_ref[ds(x * seqs, seqs, seqs), ds((core * n_tp + y) * cols, cols, cols)] = hbuf[...].astype(F32) + tot

    def block(dy, dx, part):
        by = lax.rem(y + n_tp - dy, n_tp)
        bx = lax.rem(x + nx - dx, nx)
        return res_ref.at[ds(bx * seqs + part * per, per, per), ds((core * n_tp + by) * cols, cols, cols)]

    sends = []

    def go(dy, dx, part, sems, where, ty, tx):
        ref = block(dy, dx, part)
        cp = rcopy(ref, ref, sems[0].at[ty, tx], sems[1].at[ty, tx], **where)
        cp.start()
        sends.append(cp)

    def fwd(dy, dx, part):
        if part == 0 and dx == 0:
            for e in far_x:
                go(dy, 0, 0, (a_s, a_r), {'sp': xat(e)}, dy, e)
        if part == 1 and dy == 0:
            for e in far_tp:
                go(0, dx, 1, (b_s, b_r), {'tp': yat(e)}, e, dx)
        ref = block(dy, dx, part)
        cp = rcopy(ref, ref, d_s.at[part, dy, dx], d_r.at[part, dy, dx], sp=partner)
        cp.start()
        sends.append(cp)

    for e in reversed(far_tp):
        go(0, 0, 0, (a_s, a_r), {'tp': yat(e)}, e, 0)
    for e in reversed(far_x):
        go(0, 0, 1, (b_s, b_r), {'sp': xat(e)}, 0, e)
    fwd(0, 0, 0)
    fwd(0, 0, 1)

    def arrive(dy, dx, part):
        ref = block(dy, dx, part)
        r = (a_r, b_r)[part].at[dy, dx]
        q = (a_s, b_s)[part].at[dy, dx]
        rcopy(ref, ref, q, r, sp=partner).wait_recv()
        fwd(dy, dx, part)

    def hops(item):
        dy, dx, part = item
        first = dx == 0 if part == 0 else dy == 0
        return (not first, min(dy, n_tp - dy) + min(dx, nx - dx), dy + dx)

    due = [(dy, dx, part) for dy in range(n_tp) for dx in range(nx) for part in range(2) if dy + dx > 0]
    for dy, dx, part in sorted(due, key=hops):
        arrive(dy, dx, part)
    for part in range(2):
        for dy in range(n_tp):
            for dx in range(nx):
                by = lax.rem(y + n_tp - dy, n_tp)
                bx = lax.rem(x + nx - dx, nx)
                ref = res_ref.at[ds(bx * seqs + part * per, per, per),
                                 ds(((1 - core) * n_tp + by) * cols, cols, cols)]
                rcopy(ref, ref, d_s.at[part, dy, dx], d_r.at[part, dy, dx], sp=partner).wait_recv()
    for cp in sends:
        cp.wait_send()
    for e in range(1, nx):
        rs(e).wait_send()
    for e in range(nx):
        give(e).wait_send()
    for d in range(1, n_tp):
        ysend(d).wait_send()
    for d in range(nx + n_local):
        psend(d).wait_send()
    for e in range(1, nx):
        rsend(e).wait_send()


def write_kernel(dims, pos_ref, qkv_ref, res_ref, k_ref, v_ref, h_out, ko_ref, vo_ref, kbuf, vbuf, hbuf, osem, hsem):
    q_per_kv, head, pitch, n_ch = dims
    n_seq, rows2, _ = kbuf.shape
    groups = qkv_ref.shape[0]
    n_grp = rows2 // groups
    per = n_seq // n_ch
    base = lax.axis_index('sp') * n_grp
    tile = 8 * groups
    trow = lax.broadcasted_iota(jnp.int32, (tile, head), 0)

    def bulk(i, which):
        src, dst = ((kbuf, ko_ref), (vbuf, vo_ref))[which]
        cut = pl.ds(i * per, per)
        return pltpu.make_async_copy(src.at[cut], dst.at[cut], osem.at[which, i])

    def hwrite(i):
        cut = pl.ds(i * 16, 16)
        return pltpu.make_async_copy(hbuf.at[cut], h_out.at[cut], hsem.at[i])

    def step(i, carry):
        for t in range(per):
            b = i * per + t
            rel = pos_ref[b] - base
            here = jnp.logical_and(rel >= 0, rel < n_grp)
            at = jnp.clip(rel, 0, n_grp - 1)
            cut = ds((at // 8) * tile, tile, tile)
            hit = jnp.logical_and(trow // groups == at % 8, here)
            for src, buf, off in ((k_ref, kbuf, q_per_kv * pitch), (v_ref, vbuf, (q_per_kv + 1) * pitch)):
                new = qkv_ref[0, pl.ds(off + b, 1), :]
                for g in range(1, groups):
                    new = jnp.where(trow % groups == g, qkv_ref[g, pl.ds(off + b, 1), :], new)
                buf[b, cut, :] = jnp.where(hit, new, src[b, cut, :].astype(F32)).astype(BF16)

        @pl.when(i > 0)
        def _():
            bulk(i - 1, 0).start()
            bulk(i - 1, 1).start()

        return carry

    lax.fori_loop(0, n_ch, step, 0)
    bulk(n_ch - 1, 0).start()
    bulk(n_ch - 1, 1).start()
    n_h = n_seq // 16
    for i in range(n_h):
        hbuf[i * 16:(i + 1) * 16, :] = res_ref[i * 16:(i + 1) * 16, :].astype(BF16)
        if i > 0:
            hwrite(i - 1).start()
    hwrite(n_h - 1).start()
    for i in range(n_ch):
        bulk(i, 0).wait()
        bulk(i, 1).wait()
    for i in range(n_h):
        hwrite(i).wait()


def solution(mesh):
    n_tp, n_sp = mesh.shape['tp'], mesh.shape['sp']
    cache_spec = P('dp', 'sp', 'tp', None)
    DMA = pltpu.SemaphoreType.DMA

    def local_step(hidden, norm_scale, w_qkv, w_out, k_cache, v_cache, positions):
        n_seq, seq_local, kv_local, head = k_cache.shape
        d_model = hidden.shape[1]
        q_per_kv = w_qkv.shape[1] // (kv_local * head) - 2
        heads = kv_local * q_per_kv
        grp_cols = (q_per_kv + 2) * head
        n_blk, n_rblk = 16, 2
        ring_cols = RING_HEADS * head
        local_cols = grp_cols - (n_sp // CORES) * ring_cols
        pitch = n_seq + 8
        per = n_seq // n_sp
        n_rows = per * heads
        flat = (n_seq, seq_local * kv_local, head)
        vmem_cache = pltpu.VMEM(flat, BF16)
        hbm_cache = jax.ShapeDtypeStruct(flat, BF16)

        nx = n_sp // CORES
        cols = d_model // (CORES * n_tp)
        depth = w_out.shape[0]
        qkv, k_now, v_now, res = pl.pallas_call(
            functools.partial(main_kernel, (q_per_kv, head, pitch, n_tp, n_sp)),
            out_shape=(pltpu.VMEM((kv_local, pitch * (q_per_kv + 2), head), F32), vmem_cache, vmem_cache,
                       pltpu.VMEM((n_seq, d_model), F32)),
            in_specs=[HBM] * 8,
            out_specs=(VMEM,) * 4,
            scratch_shapes=[
                pltpu.VMEM(hidden.shape, BF16),
                pltpu.VMEM((d_model // 128, 128), BF16),
                pltpu.VMEM((1, n_seq), jnp.int32),
                pltpu.VMEM((n_blk, d_model // n_blk, local_cols), BF16),
                pltpu.VMEM((n_seq, d_model), BF16),
                pltpu.VMEM((n_seq, local_cols), F32),
                pltpu.VMEM((d_model // 128, 128), F32),
                pltpu.VMEM((n_rblk, d_model // n_rblk, ring_cols), BF16),
                pltpu.VMEM((n_sp, n_rows + 8, head), F32),
                pltpu.VMEM((nx, n_rows + 8, head), F32),
                pltpu.VMEM((nx, n_rows + 8, head), F32),
                pltpu.VMEM((nx, n_rows + 8, head), F32),
                pltpu.VMEM((CORES, n_rows, head), F32),
                pltpu.VMEM((1, n_rows, head), F32),
                pltpu.VMEM((CORES * per, depth), BF16),
                pltpu.VMEM((n_tp, depth, cols), BF16),
                pltpu.VMEM((n_tp, CORES * per, cols), F32),
                pltpu.VMEM((n_tp, CORES * per, cols), F32),
                pltpu.VMEM((CORES * per, cols), BF16),
                DMA((4,)), DMA((n_blk,)), DMA((2, n_sp)), DMA((q_per_kv + 2,)), DMA((q_per_kv + 2,)),
                DMA((n_tp,)), DMA,
                DMA((nx,)), DMA((nx,)), DMA((nx,)), DMA((nx,)), DMA, DMA, DMA((n_tp,)), DMA((n_tp,)),
                DMA((n_tp, nx)), DMA((n_tp, nx)), DMA((n_tp, nx)), DMA((n_tp, nx)),
                DMA((2, n_tp, nx)), DMA((2, n_tp, nx)),
                pltpu.SMEM((n_seq,), jnp.int32),
                DMA((n_rblk,)), DMA((nx,)), DMA((nx,)),
            ],
            compiler_params=pltpu.CompilerParams(
                collective_id=0, has_side_effects=True, vmem_limit_bytes=46 * MIB),
            name='main',
        )(in_hbm(positions), in_hbm(hidden), in_hbm(norm_scale.reshape(d_model // 128, 128)),
          in_hbm(positions.reshape(1, n_seq)), in_hbm(w_qkv), in_hbm(k_cache.reshape(flat)),
          in_hbm(v_cache.reshape(flat)), in_hbm(w_out))

        h_out, k_out, v_out, _, _ = pl.pallas_call(
            functools.partial(write_kernel, (q_per_kv, head, pitch, n_sp)),
            out_shape=(jax.ShapeDtypeStruct(hidden.shape, BF16), hbm_cache, hbm_cache, vmem_cache, vmem_cache),
            in_specs=[SMEM, VMEM, VMEM, VMEM, VMEM],
            out_specs=(HBM, HBM, HBM, VMEM, VMEM),
            input_output_aliases={3: 3, 4: 4},
            scratch_shapes=[pltpu.VMEM(hidden.shape, BF16), DMA((2, n_sp)), DMA((n_seq // 16,))],
            compiler_params=pltpu.CompilerParams(vmem_limit_bytes=4 * MIB),
            name='write',
        )(positions, qkv, res, k_now, v_now)
        return h_out, k_out.reshape(k_cache.shape), v_out.reshape(v_cache.shape)

    return jax.shard_map(
        local_step,
        mesh=mesh,
        in_specs=(P('dp', None), P(None), P(None, 'tp'), P('tp', None), cache_spec, cache_spec, P('dp')),
        out_specs=(P('dp', None), cache_spec, cache_spec),
        check_vma=False,
    )
```

```python
import functools
import math

import jax
import jax.numpy as jnp
from jax import lax
from jax.experimental import pallas as pl
from jax.experimental.pallas import tpu as pltpu
from jax.sharding import PartitionSpec as P

MESH = pl.DeviceIdType.MESH
F32 = jnp.float32
BF16 = jnp.bfloat16
HBM = pl.BlockSpec(memory_space=pltpu.HBM)
VMEM = pl.BlockSpec(memory_space=pltpu.VMEM)
SMEM = pl.BlockSpec(memory_space=pltpu.SMEM)
CORES = 2
RING_HEADS = 1
CACHE_STEP = 12
WINDOW = 5
MIB = 1024 * 1024


def in_hbm(val):
    return pltpu.with_memory_space_constraint(val, pltpu.HBM)


def ds(start, size, align):
    return pl.ds(pl.multiple_of(start, align), size)


def rcopy(src, dst, send_sem, recv_sem, **where):
    return pltpu.make_async_remote_copy(
        src_ref=src, dst_ref=dst, send_sem=send_sem, recv_sem=recv_sem,
        device_id=where, device_id_type=MESH,
    )


def main_kernel(dims, pos_flat, h_hbm, scale_hbm, pos_hbm, w_ref, k_hbm, v_hbm, wo_ref, out_ref, kbuf, vbuf, res_ref,
                h_ref, scale_ref, pos_ref, wbuf, u_ref, acc, gain, wring, o_ref, cbuf, mix, rbuf, abuf, attn, lhs, wobuf, pbuf, ybuf, hbuf,
                hsem, wsem, csem, s_part, r_part, wosem, hosem, c_s, c_r, rs_s, rs_r, ab_s, ab_r, y_s, y_r, a_s, a_r, b_s, b_r,
                d_s, d_r, pos_smem, rsem, s_ring, r_ring):
    n_seq, d_model = h_ref.shape
    q_per_kv, head, pitch, n_tp, n_sp = dims
    n_blk, blk, lcols = wbuf.shape
    n_rblk, rblk, rcols = wring.shape
    rh = rcols // head
    grp = (q_per_kv + 2) * head
    groups = out_ref.shape[0]
    heads = groups * q_per_kv
    rows2 = kbuf.shape[1]
    n_grp = rows2 // groups
    nx = n_sp // CORES
    y = lax.axis_index('tp')
    s = lax.axis_index('sp')
    core = lax.rem(s, CORES)
    x = s // CORES
    partner = s + 1 - 2 * core
    n_rows = attn.shape[1]
    per = n_rows // heads
    cols = wobuf.shape[2]
    seqs = CORES * per
    base = s * n_grp

    def yat(d):
        return lax.rem(y + d, n_tp)

    def xat(d):
        return lax.rem(x + d, nx) * CORES + core

    def wload(i):
        return pltpu.make_async_copy(
            w_ref.at[ds(i * blk, blk, blk), ds(core * grp + nx * rcols, lcols, 128)], wbuf.at[i], wsem.at[i])

    def rload(i):
        return pltpu.make_async_copy(
            w_ref.at[pl.ds(i * rblk, rblk), ds(core * grp + x * rcols, rcols, 128)], wring.at[i], rsem.at[i])

    def wcopy(j):
        return pltpu.make_async_copy(
            wo_ref.at[:, ds((core * n_tp + yat(j)) * cols, cols, cols)], wobuf.at[j], wosem.at[j])

    def chunk_of(d):
        return lax.rem(x + d // CORES, nx) * CORES + (core if d % CORES == 0 else 1 - core)

    def ccopy(d, which):
        src, dst = ((k_hbm, kbuf), (v_hbm, vbuf))[which]
        cut = pl.ds(chunk_of(d) * per, per)
        return pltpu.make_async_copy(src.at[cut], dst.at[cut], csem.at[which, d])

    def cache_load(e):
        for p in (1, 0):
            ccopy(CORES * e + p, 0).start()
            ccopy(CORES * e + p, 1).start()

    hcopy = pltpu.make_async_copy(
        h_hbm.at[ds(x * seqs, seqs, seqs), ds((core * n_tp + y) * cols, cols, cols)], hbuf, hosem)
    far_tp = sorted(range(1, n_tp), key=lambda d: -min(d, n_tp - d))
    far_x = sorted(range(1, nx), key=lambda d: -min(d, nx - d))
    order = far_tp + [0]
    chips = far_x + [0]
    loads = [
        pltpu.make_async_copy(src, dst, hsem.at[i])
        for i, (src, dst) in enumerate(
            ((h_hbm, h_ref), (scale_hbm, scale_ref), (pos_hbm, pos_ref), (pos_flat, pos_smem)))
    ]
    for load in loads:
        load.start()
    for i in range(n_rblk):
        rload(i).start()
    barrier = pltpu.get_barrier_semaphore()
    pl.semaphore_signal(barrier, inc=1, device_id={'sp': partner}, device_id_type=MESH)
    for d in range(1, nx):
        pl.semaphore_signal(barrier, inc=1, device_id={'sp': xat(d)}, device_id_type=MESH)
    for d in range(1, n_tp):
        pl.semaphore_signal(barrier, inc=1, device_id={'tp': yat(d)}, device_id_type=MESH)
    for load in loads:
        load.wait()
    for i in range(WINDOW):
        wload(i).start()

    lanes = 128
    zero = jnp.zeros((n_seq, lanes), F32)

    def add_sum(i, tot):
        return tot + h_ref[:, ds(i * lanes, lanes, lanes)].astype(F32)

    mean = jnp.sum(lax.fori_loop(0, d_model // lanes, add_sum, zero, unroll=8), axis=1, keepdims=True) / d_model

    def add_sq(i, tot):
        cent = h_ref[:, ds(i * lanes, lanes, lanes)].astype(F32) - mean
        return tot + cent * cent

    var = jnp.sum(lax.fori_loop(0, d_model // lanes, add_sq, zero, unroll=8), axis=1, keepdims=True) / d_model
    inv = lax.rsqrt(var + 1e-5)

    gain[...] = scale_ref[...].astype(F32)

    def norm(i, carry):
        cut = ds(i * lanes, lanes, lanes)
        cent = h_ref[:, cut].astype(F32) - mean
        u_ref[:, cut] = (cent * inv * gain[pl.ds(i, 1), :]).astype(BF16)
        return carry

    lax.fori_loop(0, d_model // lanes, norm, 0, unroll=8)

    eye = lax.broadcasted_iota(jnp.int32, (n_seq, n_seq), 0) == lax.broadcasted_iota(jnp.int32, (n_seq, n_seq), 1)
    pos_col = jnp.sum(jnp.where(eye, pos_ref[...].astype(F32), 0.0), axis=1, keepdims=True)
    lane = lax.broadcasted_iota(jnp.int32, (n_seq, head), 1)
    half = head // 2
    inv_freq = jnp.exp(lax.rem(lane, half).astype(F32) * (-2.0 * math.log(500000.0) / head))
    angle = pos_col * inv_freq
    cos_t = jnp.cos(angle)
    sin_t = jnp.where(lane < half, -jnp.sin(angle), jnp.sin(angle))

    def finish(val, rotate):
        val = jnp.clip(val.astype(BF16), -8.0, 8.0).astype(F32)
        if rotate:
            val = (val * cos_t + pltpu.roll(val, half, 1) * sin_t).astype(BF16).astype(F32)
        return val

    def slab(cx):
        return out_ref.at[core, ds(cx * rh * pitch, (rh - 1) * pitch + n_seq, 8)]

    def rsend(e):
        return rcopy(slab(x), slab(x), s_ring.at[e], r_ring.at[e], sp=xat(e))

    n_local = lcols // head

    def psend(d):
        ref = slab(lax.rem(x + nx - d, nx)) if d < nx else out_ref.at[core, pl.ds((nx * rh + d - nx) * pitch, n_seq)]
        return rcopy(ref, ref, s_part.at[d], r_part.at[d], sp=partner)

    tot = None
    for i in range(n_rblk):
        rload(i).wait()
        prod = jnp.dot(u_ref[:, i * rblk:(i + 1) * rblk], wring[i], preferred_element_type=F32)
        tot = prod if tot is None else tot + prod
    for t in range(rh):
        out_ref[core, ds((x * rh + t) * pitch, n_seq, 8), :] = finish(tot[:, t * head:(t + 1) * head], True)
    pl.semaphore_wait(barrier, nx + n_tp - 1)
    for e in far_x:
        rsend(e).start()
    psend(0).start()

    acc[...] = jnp.zeros_like(acc)

    def mm(i, carry):
        wload(i).wait()

        @pl.when(i + WINDOW < n_blk)
        def _():
            wload(i + WINDOW).start()

        @pl.when(i == CACHE_STEP)
        def _():
            cache_load(chips[0])

        acc[...] += jnp.dot(u_ref[:, ds(i * blk, blk, blk)], wbuf[i], preferred_element_type=F32)
        return carry

    lax.fori_loop(0, n_blk, mm, 0)
    for e in chips[1:]:
        cache_load(e)
    hcopy.start()
    for t in range(n_local):
        at = nx * rh + t
        out_ref[core, at * pitch:at * pitch + n_seq, :] = finish(
            acc[:, t * head:(t + 1) * head], at < q_per_kv + 1)
        if t > 0:
            psend(nx + t - 1).start()
    psend(nx + n_local - 1).start()
    for e in reversed(far_x):
        rsend(e).wait_recv()
        psend(e).start()

    colj = lax.broadcasted_iota(jnp.int32, (heads, rows2), 1)
    rown = lax.broadcasted_iota(jnp.int32, (heads, rows2), 0)
    same = lax.rem(colj, groups) == rown // q_per_kv
    eye = lax.broadcasted_iota(jnp.int32, (n_rows, n_rows), 0) == lax.broadcasted_iota(jnp.int32, (n_rows, n_rows), 1)
    for d in range(nx + n_local):
        psend(d).wait_recv()

    def give(e):
        return rcopy(o_ref.at[CORES * e + 1], cbuf.at[e], c_s.at[e], c_r.at[e], sp=partner)

    def rs(e):
        return rcopy(mix.at[e], rbuf.at[e], rs_s.at[e], rs_r.at[e], sp=xat(e))

    def merge(parts):
        tops = [p[n_rows:n_rows + 1, :] for p in parts]
        sums = [p[n_rows + 1:n_rows + 2, :] for p in parts]
        top = functools.reduce(jnp.maximum, tops)
        facs = [jnp.exp(t - top) for t in tops]
        tot = functools.reduce(jnp.add, [f * l for f, l in zip(facs, sums)])
        return top, tot, facs

    def weigh(parts, facs):
        pad = jnp.zeros((n_rows - len(facs), n_rows), F32)
        fac = jnp.transpose(jnp.concatenate(facs + [pad], axis=0))
        return functools.reduce(
            jnp.add, [p[0:n_rows, :] * fac[:, j:j + 1] for j, p in enumerate(parts)])

    def pair(e):
        give(e).wait_recv()
        parts = [o_ref.at[CORES * e], cbuf.at[e]]
        top, tot, facs = merge(parts)
        mix[e, 0:n_rows, :] = weigh(parts, facs)
        mix[e, n_rows:n_rows + 8, :] = jnp.concatenate([top, tot, jnp.zeros((6, n_rows), F32)], axis=0)
        if e:
            rs(e).start()

    def attend(d):
        i = chunk_of(d)
        ccopy(d, 0).wait()
        ccopy(d, 1).wait()
        scores, fresh, vals = [], [], []
        for t in range(per):
            b = i * per + t
            rel = pos_smem[b] - base
            rows = [
                jnp.concatenate([
                    jnp.broadcast_to(out_ref[g, pl.ds(off * pitch + b, 1), :], (q_per_kv, head)) for g in range(groups)
                ], axis=0) for off in (q_per_kv, q_per_kv + 1)
            ]
            q = jnp.concatenate([out_ref[g, pl.ds(b, q_per_kv, stride=pitch), :] for g in range(groups)], axis=0)
            sc = lax.dot_general(q.astype(BF16), kbuf[b], (((1,), (1,)), ((), ())), preferred_element_type=F32)
            ok = jnp.logical_and(same, colj < groups * rel)
            scores.append(jnp.where(ok, sc * (head ** -0.5), -1e30))
            own = jnp.sum(q * rows[0], axis=1, keepdims=True) * (head ** -0.5)
            at = jnp.full((heads, 1), rel, jnp.int32)
            fresh.append(jnp.where(jnp.logical_and(at >= 0, at < n_grp), own, -1e30))
            vals.append(rows[1])
        sc = jnp.concatenate(scores, axis=0)
        own = jnp.concatenate(fresh, axis=0)
        top = jnp.maximum(jnp.max(sc, axis=1, keepdims=True), own)
        wt = jnp.exp(sc - top)
        own = jnp.exp(own - top)
        tot = jnp.sum(wt, axis=1, keepdims=True) + own
        wt = wt.astype(BF16)
        own = own.astype(BF16).astype(F32)
        for t in range(per):
            cut = slice(t * heads, (t + 1) * heads)
            o_ref[d, cut, :] = jnp.dot(
                wt[cut], vbuf[i * per + t], preferred_element_type=F32) + own[cut] * vals[t]
        top_row = jnp.sum(jnp.where(eye, top, 0.0), axis=0, keepdims=True)
        tot_row = jnp.sum(jnp.where(eye, tot, 0.0), axis=0, keepdims=True)
        pad = jnp.zeros((6, n_rows), F32)
        o_ref[d, n_rows:n_rows + 8, :] = jnp.concatenate([top_row, tot_row, pad], axis=0)

    last = None
    for t, e in enumerate(chips):
        if t == nx // 2:
            for j in order[:n_tp // 2]:
                wcopy(j).start()
        attend(CORES * e + 1)
        give(e).start()
        attend(CORES * e)
        if last is not None:
            pair(last)
        last = e
    for j in order[n_tp // 2:]:
        wcopy(j).start()
    pair(last)
    parts = [mix.at[0]]
    for e in reversed(far_x):
        rs(e).wait_recv()
        parts.append(rbuf.at[e])
    _, tot, facs = merge(parts)
    val = weigh(parts, [f / tot for f in facs])
    attn[0] = val

    swap = rcopy(attn.at[0], abuf.at[core], ab_s, ab_r, sp=partner)
    swap.start()
    abuf[core] = val
    swap.wait()
    flat = abuf.reshape(CORES * n_rows, head)
    for n in range(heads):
        lhs[:, n * head:(n + 1) * head] = flat[pl.ds(n, seqs, stride=heads), :].astype(BF16)

    def ysend(d):
        return rcopy(pbuf.at[d], ybuf.at[d], y_s.at[d], y_r.at[d], tp=yat(d))

    def proj(j):
        wcopy(j).wait()
        pbuf[j] = jnp.dot(lhs[...], wobuf[j], preferred_element_type=F32)

    for j in order:
        proj(j)
        if j:
            ysend(j).start()
    hcopy.wait()
    tot = pbuf[0]
    for d in range(1, n_tp):
        ysend(d).wait_recv()
        tot = tot + ybuf[d]
    res_ref[ds(x * seqs, seqs, seqs), ds((core * n_tp + y) * cols, cols, cols)] = hbuf[...].astype(F32) + tot

    def block(dy, dx, part):
        by = lax.rem(y + n_tp - dy, n_tp)
        bx = lax.rem(x + nx - dx, nx)
        return res_ref.at[ds(bx * seqs + part * per, per, per), ds((core * n_tp + by) * cols, cols, cols)]

    sends = []

    def go(dy, dx, part, sems, where, ty, tx):
        ref = block(dy, dx, part)
        cp = rcopy(ref, ref, sems[0].at[ty, tx], sems[1].at[ty, tx], **where)
        cp.start()
        sends.append(cp)

    def fwd(dy, dx, part):
        if part == 0 and dx == 0:
            for e in far_x:
                go(dy, 0, 0, (a_s, a_r), {'sp': xat(e)}, dy, e)
        if part == 1 and dy == 0:
            for e in far_tp:
                go(0, dx, 1, (b_s, b_r), {'tp': yat(e)}, e, dx)
        ref = block(dy, dx, part)
        cp = rcopy(ref, ref, d_s.at[part, dy, dx], d_r.at[part, dy, dx], sp=partner)
        cp.start()
        sends.append(cp)

    for e in reversed(far_tp):
        go(0, 0, 0, (a_s, a_r), {'tp': yat(e)}, e, 0)
    for e in reversed(far_x):
        go(0, 0, 1, (b_s, b_r), {'sp': xat(e)}, 0, e)
    fwd(0, 0, 0)
    fwd(0, 0, 1)

    def arrive(dy, dx, part):
        ref = block(dy, dx, part)
        r = (a_r, b_r)[part].at[dy, dx]
        q = (a_s, b_s)[part].at[dy, dx]
        rcopy(ref, ref, q, r, sp=partner).wait_recv()
        fwd(dy, dx, part)

    def hops(item):
        dy, dx, part = item
        first = dx == 0 if part == 0 else dy == 0
        return (not first, min(dy, n_tp - dy) + min(dx, nx - dx), dy + dx)

    due = [(dy, dx, part) for dy in range(n_tp) for dx in range(nx) for part in range(2) if dy + dx > 0]
    for dy, dx, part in sorted(due, key=hops):
        arrive(dy, dx, part)
    for part in range(2):
        for dy in range(n_tp):
            for dx in range(nx):
                by = lax.rem(y + n_tp - dy, n_tp)
                bx = lax.rem(x + nx - dx, nx)
                ref = res_ref.at[ds(bx * seqs + part * per, per, per),
                                 ds(((1 - core) * n_tp + by) * cols, cols, cols)]
                rcopy(ref, ref, d_s.at[part, dy, dx], d_r.at[part, dy, dx], sp=partner).wait_recv()
    for cp in sends:
        cp.wait_send()
    for e in range(1, nx):
        rs(e).wait_send()
    for e in range(nx):
        give(e).wait_send()
    for d in range(1, n_tp):
        ysend(d).wait_send()
    for d in range(nx + n_local):
        psend(d).wait_send()
    for e in range(1, nx):
        rsend(e).wait_send()


def write_kernel(dims, pos_ref, qkv_ref, res_ref, k_ref, v_ref, h_out, ko_ref, vo_ref, kbuf, vbuf, hbuf, osem, hsem):
    q_per_kv, head, pitch, n_ch = dims
    n_seq, rows2, _ = kbuf.shape
    groups = qkv_ref.shape[0]
    n_grp = rows2 // groups
    per = n_seq // n_ch
    base = lax.axis_index('sp') * n_grp
    tile = 8 * groups
    trow = lax.broadcasted_iota(jnp.int32, (tile, head), 0)

    def bulk(i, which):
        src, dst = ((kbuf, ko_ref), (vbuf, vo_ref))[which]
        cut = pl.ds(i * per, per)
        return pltpu.make_async_copy(src.at[cut], dst.at[cut], osem.at[which, i])

    def hwrite(i):
        cut = pl.ds(i * 16, 16)
        return pltpu.make_async_copy(hbuf.at[cut], h_out.at[cut], hsem.at[i])

    def step(i, carry):
        for t in range(per):
            b = i * per + t
            rel = pos_ref[b] - base
            here = jnp.logical_and(rel >= 0, rel < n_grp)
            at = jnp.clip(rel, 0, n_grp - 1)
            cut = ds((at // 8) * tile, tile, tile)
            hit = jnp.logical_and(trow // groups == at % 8, here)
            for src, buf, off in ((k_ref, kbuf, q_per_kv * pitch), (v_ref, vbuf, (q_per_kv + 1) * pitch)):
                new = qkv_ref[0, pl.ds(off + b, 1), :]
                for g in range(1, groups):
                    new = jnp.where(trow % groups == g, qkv_ref[g, pl.ds(off + b, 1), :], new)
                buf[b, cut, :] = jnp.where(hit, new, src[b, cut, :].astype(F32)).astype(BF16)

        @pl.when(i > 0)
        def _():
            bulk(i - 1, 0).start()
            bulk(i - 1, 1).start()

        return carry

    lax.fori_loop(0, n_ch, step, 0)
    bulk(n_ch - 1, 0).start()
    bulk(n_ch - 1, 1).start()
    n_h = n_seq // 16
    for i in range(n_h):
        hbuf[i * 16:(i + 1) * 16, :] = res_ref[i * 16:(i + 1) * 16, :].astype(BF16)
        if i > 0:
            hwrite(i - 1).start()
    hwrite(n_h - 1).start()
    for i in range(n_ch):
        bulk(i, 0).wait()
        bulk(i, 1).wait()
    for i in range(n_h):
        hwrite(i).wait()


def solution(mesh):
    n_tp, n_sp = mesh.shape['tp'], mesh.shape['sp']
    cache_spec = P('dp', 'sp', 'tp', None)
    DMA = pltpu.SemaphoreType.DMA

    def local_step(hidden, norm_scale, w_qkv, w_out, k_cache, v_cache, positions):
        n_seq, seq_local, kv_local, head = k_cache.shape
        d_model = hidden.shape[1]
        q_per_kv = w_qkv.shape[1] // (kv_local * head) - 2
        heads = kv_local * q_per_kv
        grp_cols = (q_per_kv + 2) * head
        n_blk, n_rblk = 16, 2
        ring_cols = RING_HEADS * head
        local_cols = grp_cols - (n_sp // CORES) * ring_cols
        pitch = n_seq + 8
        per = n_seq // n_sp
        n_rows = per * heads
        flat = (n_seq, seq_local * kv_local, head)
        vmem_cache = pltpu.VMEM(flat, BF16)
        hbm_cache = jax.ShapeDtypeStruct(flat, BF16)

        nx = n_sp // CORES
        cols = d_model // (CORES * n_tp)
        depth = w_out.shape[0]
        qkv, k_now, v_now, res = pl.pallas_call(
            functools.partial(main_kernel, (q_per_kv, head, pitch, n_tp, n_sp)),
            out_shape=(pltpu.VMEM((kv_local, pitch * (q_per_kv + 2), head), F32), vmem_cache, vmem_cache,
                       pltpu.VMEM((n_seq, d_model), F32)),
            in_specs=[HBM] * 8,
            out_specs=(VMEM,) * 4,
            scratch_shapes=[
                pltpu.VMEM(hidden.shape, BF16),
                pltpu.VMEM((d_model // 128, 128), BF16),
                pltpu.VMEM((1, n_seq), jnp.int32),
                pltpu.VMEM((n_blk, d_model // n_blk, local_cols), BF16),
                pltpu.VMEM((n_seq, d_model), BF16),
                pltpu.VMEM((n_seq, local_cols), F32),
                pltpu.VMEM((d_model // 128, 128), F32),
                pltpu.VMEM((n_rblk, d_model // n_rblk, ring_cols), BF16),
                pltpu.VMEM((n_sp, n_rows + 8, head), F32),
                pltpu.VMEM((nx, n_rows + 8, head), F32),
                pltpu.VMEM((nx, n_rows + 8, head), F32),
                pltpu.VMEM((nx, n_rows + 8, head), F32),
                pltpu.VMEM((CORES, n_rows, head), F32),
                pltpu.VMEM((1, n_rows, head), F32),
                pltpu.VMEM((CORES * per, depth), BF16),
                pltpu.VMEM((n_tp, depth, cols), BF16),
                pltpu.VMEM((n_tp, CORES * per, cols), F32),
                pltpu.VMEM((n_tp, CORES * per, cols), F32),
                pltpu.VMEM((CORES * per, cols), BF16),
                DMA((4,)), DMA((n_blk,)), DMA((2, n_sp)), DMA((q_per_kv + 2,)), DMA((q_per_kv + 2,)),
                DMA((n_tp,)), DMA,
                DMA((nx,)), DMA((nx,)), DMA((nx,)), DMA((nx,)), DMA, DMA, DMA((n_tp,)), DMA((n_tp,)),
                DMA((n_tp, nx)), DMA((n_tp, nx)), DMA((n_tp, nx)), DMA((n_tp, nx)),
                DMA((2, n_tp, nx)), DMA((2, n_tp, nx)),
                pltpu.SMEM((n_seq,), jnp.int32),
                DMA((n_rblk,)), DMA((nx,)), DMA((nx,)),
            ],
            compiler_params=pltpu.CompilerParams(
                collective_id=0, has_side_effects=True, vmem_limit_bytes=46 * MIB),
            name='main',
        )(in_hbm(positions), in_hbm(hidden), in_hbm(norm_scale.reshape(d_model // 128, 128)),
          in_hbm(positions.reshape(1, n_seq)), in_hbm(w_qkv), in_hbm(k_cache.reshape(flat)),
          in_hbm(v_cache.reshape(flat)), in_hbm(w_out))

        h_out, k_out, v_out, _, _ = pl.pallas_call(
            functools.partial(write_kernel, (q_per_kv, head, pitch, n_sp)),
            out_shape=(jax.ShapeDtypeStruct(hidden.shape, BF16), hbm_cache, hbm_cache, vmem_cache, vmem_cache),
            in_specs=[SMEM, VMEM, VMEM, VMEM, VMEM],
            out_specs=(HBM, HBM, HBM, VMEM, VMEM),
            input_output_aliases={3: 3, 4: 4},
            scratch_shapes=[pltpu.VMEM(hidden.shape, BF16), DMA((2, n_sp)), DMA((n_seq // 16,))],
            compiler_params=pltpu.CompilerParams(vmem_limit_bytes=4 * MIB),
            name='write',
        )(positions, qkv, res, k_now, v_now)
        return h_out, k_out.reshape(k_cache.shape), v_out.reshape(v_cache.shape)

    return jax.shard_map(
        local_step,
        mesh=mesh,
        in_specs=(P('dp', None), P(None), P(None, 'tp'), P('tp', None), cache_spec, cache_spec, P('dp')),
        out_specs=(P('dp', None), cache_spec, cache_spec),
        check_vma=False,
    )
```

```python
import functools
import math

import jax
import jax.numpy as jnp
from jax import lax
from jax.experimental import pallas as pl
from jax.experimental.pallas import tpu as pltpu
from jax.sharding import PartitionSpec as P

MESH = pl.DeviceIdType.MESH
F32 = jnp.float32
BF16 = jnp.bfloat16
HBM = pl.BlockSpec(memory_space=pltpu.HBM)
VMEM = pl.BlockSpec(memory_space=pltpu.VMEM)
SMEM = pl.BlockSpec(memory_space=pltpu.SMEM)
CORES = 2
RING_HEADS = 1
CACHE_STEP = 12
WINDOW = 5
H_PARTS = 4
WO_PARTS = 2
MIB = 1024 * 1024


def in_hbm(val):
    return pltpu.with_memory_space_constraint(val, pltpu.HBM)


def ds(start, size, align):
    return pl.ds(pl.multiple_of(start, align), size)


def rcopy(src, dst, send_sem, recv_sem, **where):
    return pltpu.make_async_remote_copy(
        src_ref=src, dst_ref=dst, send_sem=send_sem, recv_sem=recv_sem,
        device_id=where, device_id_type=MESH,
    )


def main_kernel(dims, pos_flat, h_hbm, scale_hbm, pos_hbm, w_ref, k_hbm, v_hbm, wo_ref, out_ref, kbuf, vbuf, res_ref,
                h_ref, scale_ref, pos_ref, wbuf, u_ref, acc, gain, wring, o_ref, cbuf, mix, rbuf, abuf, attn, lhs, wobuf, pbuf, ybuf, hbuf,
                hsem, wsem, csem, s_part, r_part, wosem, hosem, c_s, c_r, rs_s, rs_r, ab_s, ab_r, y_s, y_r, a_s, a_r, b_s, b_r,
                d_s, d_r, pos_smem, rsem, s_ring, r_ring):
    n_seq, d_model = h_ref.shape
    q_per_kv, head, pitch, n_tp, n_sp = dims
    n_blk, blk, lcols = wbuf.shape
    n_rblk, rblk, rcols = wring.shape
    rh = rcols // head
    grp = (q_per_kv + 2) * head
    groups = out_ref.shape[0]
    heads = groups * q_per_kv
    rows2 = kbuf.shape[1]
    n_grp = rows2 // groups
    nx = n_sp // CORES
    y = lax.axis_index('tp')
    s = lax.axis_index('sp')
    core = lax.rem(s, CORES)
    x = s // CORES
    partner = s + 1 - 2 * core
    n_rows = attn.shape[1]
    per = n_rows // heads
    cols = wobuf.shape[2]
    seqs = CORES * per
    base = s * n_grp

    def yat(d):
        return lax.rem(y + d, n_tp)

    def xat(d):
        return lax.rem(x + d, nx) * CORES + core

    def wload(i):
        return pltpu.make_async_copy(
            w_ref.at[ds(i * blk, blk, blk), ds(core * grp + nx * rcols, lcols, 128)], wbuf.at[i], wsem.at[i])

    def rload(i):
        return pltpu.make_async_copy(
            w_ref.at[pl.ds(i * rblk, rblk), ds(core * grp + x * rcols, rcols, 128)], wring.at[i], rsem.at[i])

    def wcopy(j, part):
        rows = wobuf.shape[1] // WO_PARTS
        cut = pl.ds(part * rows, rows)
        return pltpu.make_async_copy(
            wo_ref.at[cut, ds((core * n_tp + yat(j)) * cols, cols, cols)], wobuf.at[j, cut], wosem.at[j, part])

    def out_load(n):
        for _ in range(min(n, len(todo))):
            j = todo.pop(0)
            for part in range(WO_PARTS):
                wcopy(j, part).start()

    def chunk_of(d):
        return lax.rem(x + d // CORES, nx) * CORES + (core if d % CORES == 0 else 1 - core)

    def ccopy(d, which):
        src, dst = ((k_hbm, kbuf), (v_hbm, vbuf))[which]
        cut = pl.ds(chunk_of(d) * per, per)
        return pltpu.make_async_copy(src.at[cut], dst.at[cut], csem.at[which, d])

    def cache_load(e):
        for p in (1, 0):
            ccopy(CORES * e + p, 0).start()
            ccopy(CORES * e + p, 1).start()

    hcopy = pltpu.make_async_copy(
        h_hbm.at[ds(x * seqs, seqs, seqs), ds((core * n_tp + y) * cols, cols, cols)], hbuf, hosem)
    far_tp = sorted(range(1, n_tp), key=lambda d: -min(d, n_tp - d))
    far_x = sorted(range(1, nx), key=lambda d: -min(d, nx - d))
    order = far_tp + [0]
    chips = far_x + [0]
    todo = list(order)
    cuts = [pl.ds(i * (d_model // H_PARTS), d_model // H_PARTS) for i in range(H_PARTS)]
    loads = [
        pltpu.make_async_copy(src, dst, hsem.at[i])
        for i, (src, dst) in enumerate(
            [(h_hbm.at[:, cut], h_ref.at[:, cut]) for cut in cuts]
            + [(scale_hbm, scale_ref), (pos_hbm, pos_ref), (pos_flat, pos_smem)])
    ]
    for load in loads:
        load.start()
    for i in range(n_rblk):
        rload(i).start()
    barrier = pltpu.get_barrier_semaphore()
    pl.semaphore_signal(barrier, inc=1, device_id={'sp': partner}, device_id_type=MESH)
    for d in range(1, nx):
        pl.semaphore_signal(barrier, inc=1, device_id={'sp': xat(d)}, device_id_type=MESH)
    for d in range(1, n_tp):
        pl.semaphore_signal(barrier, inc=1, device_id={'tp': yat(d)}, device_id_type=MESH)
    for load in loads:
        load.wait()
    for i in range(WINDOW):
        wload(i).start()

    lanes = 128
    zero = jnp.zeros((n_seq, lanes), F32)

    def add_sum(i, tot):
        return tot + h_ref[:, ds(i * lanes, lanes, lanes)].astype(F32)

    mean = jnp.sum(lax.fori_loop(0, d_model // lanes, add_sum, zero, unroll=8), axis=1, keepdims=True) / d_model

    def add_sq(i, tot):
        cent = h_ref[:, ds(i * lanes, lanes, lanes)].astype(F32) - mean
        return tot + cent * cent

    var = jnp.sum(lax.fori_loop(0, d_model // lanes, add_sq, zero, unroll=8), axis=1, keepdims=True) / d_model
    inv = lax.rsqrt(var + 1e-5)

    gain[...] = scale_ref[...].astype(F32)

    def norm(i, carry):
        cut = ds(i * lanes, lanes, lanes)
        cent = h_ref[:, cut].astype(F32) - mean
        u_ref[:, cut] = (cent * inv * gain[pl.ds(i, 1), :]).astype(BF16)
        return carry

    lax.fori_loop(0, d_model // lanes, norm, 0, unroll=8)

    eye = lax.broadcasted_iota(jnp.int32, (n_seq, n_seq), 0) == lax.broadcasted_iota(jnp.int32, (n_seq, n_seq), 1)
    pos_col = jnp.sum(jnp.where(eye, pos_ref[...].astype(F32), 0.0), axis=1, keepdims=True)
    lane = lax.broadcasted_iota(jnp.int32, (n_seq, head), 1)
    half = head // 2
    inv_freq = jnp.exp(lax.rem(lane, half).astype(F32) * (-2.0 * math.log(500000.0) / head))
    angle = pos_col * inv_freq
    cos_t = jnp.cos(angle)
    sin_t = jnp.where(lane < half, -jnp.sin(angle), jnp.sin(angle))

    def finish(val, rotate):
        val = jnp.clip(val.astype(BF16), -8.0, 8.0).astype(F32)
        if rotate:
            val = (val * cos_t + pltpu.roll(val, half, 1) * sin_t).astype(BF16).astype(F32)
        return val

    def slab(cx):
        return out_ref.at[core, ds(cx * rh * pitch, (rh - 1) * pitch + n_seq, 8)]

    def rsend(e):
        return rcopy(slab(x), slab(x), s_ring.at[e], r_ring.at[e], sp=xat(e))

    n_local = lcols // head

    def psend(d):
        ref = slab(lax.rem(x + nx - d, nx)) if d < nx else out_ref.at[core, pl.ds((nx * rh + d - nx) * pitch, n_seq)]
        return rcopy(ref, ref, s_part.at[d], r_part.at[d], sp=partner)

    tot = None
    for i in range(n_rblk):
        rload(i).wait()
        prod = jnp.dot(u_ref[:, i * rblk:(i + 1) * rblk], wring[i], preferred_element_type=F32)
        tot = prod if tot is None else tot + prod
    for t in range(rh):
        out_ref[core, ds((x * rh + t) * pitch, n_seq, 8), :] = finish(tot[:, t * head:(t + 1) * head], True)
    pl.semaphore_wait(barrier, nx + n_tp - 1)
    for e in far_x:
        rsend(e).start()
    psend(0).start()

    acc[...] = jnp.zeros_like(acc)

    def mm(i, carry):
        wload(i).wait()

        @pl.when(i + WINDOW < n_blk)
        def _():
            wload(i + WINDOW).start()

        @pl.when(i == CACHE_STEP)
        def _():
            cache_load(chips[0])

        acc[...] += jnp.dot(u_ref[:, ds(i * blk, blk, blk)], wbuf[i], preferred_element_type=F32)
        return carry

    lax.fori_loop(0, n_blk, mm, 0)
    for e in chips[1:]:
        cache_load(e)
    hcopy.start()
    for t in range(n_local):
        at = nx * rh + t
        out_ref[core, at * pitch:at * pitch + n_seq, :] = finish(
            acc[:, t * head:(t + 1) * head], at < q_per_kv + 1)
        if t > 0:
            psend(nx + t - 1).start()
    psend(nx + n_local - 1).start()
    for e in reversed(far_x):
        rsend(e).wait_recv()
        psend(e).start()

    colj = lax.broadcasted_iota(jnp.int32, (heads, rows2), 1)
    rown = lax.broadcasted_iota(jnp.int32, (heads, rows2), 0)
    same = lax.rem(colj, groups) == rown // q_per_kv
    eye = lax.broadcasted_iota(jnp.int32, (n_rows, n_rows), 0) == lax.broadcasted_iota(jnp.int32, (n_rows, n_rows), 1)
    for d in range(nx + n_local):
        psend(d).wait_recv()

    def give(e):
        return rcopy(o_ref.at[CORES * e + 1], cbuf.at[e], c_s.at[e], c_r.at[e], sp=partner)

    def rs(e):
        return rcopy(mix.at[e], rbuf.at[e], rs_s.at[e], rs_r.at[e], sp=xat(e))

    def merge(parts):
        tops = [p[n_rows:n_rows + 1, :] for p in parts]
        sums = [p[n_rows + 1:n_rows + 2, :] for p in parts]
        top = functools.reduce(jnp.maximum, tops)
        facs = [jnp.exp(t - top) for t in tops]
        tot = functools.reduce(jnp.add, [f * l for f, l in zip(facs, sums)])
        return top, tot, facs

    def weigh(parts, facs):
        pad = jnp.zeros((n_rows - len(facs), n_rows), F32)
        fac = jnp.transpose(jnp.concatenate(facs + [pad], axis=0))
        return functools.reduce(
            jnp.add, [p[0:n_rows, :] * fac[:, j:j + 1] for j, p in enumerate(parts)])

    def pair(e):
        give(e).wait_recv()
        parts = [o_ref.at[CORES * e], cbuf.at[e]]
        top, tot, facs = merge(parts)
        mix[e, 0:n_rows, :] = weigh(parts, facs)
        mix[e, n_rows:n_rows + 8, :] = jnp.concatenate([top, tot, jnp.zeros((6, n_rows), F32)], axis=0)
        if e:
            rs(e).start()

    def attend(d):
        i = chunk_of(d)
        ccopy(d, 0).wait()
        ccopy(d, 1).wait()
        scores, fresh, vals = [], [], []
        for t in range(per):
            b = i * per + t
            rel = pos_smem[b] - base
            rows = [
                jnp.concatenate([
                    jnp.broadcast_to(out_ref[g, pl.ds(off * pitch + b, 1), :], (q_per_kv, head)) for g in range(groups)
                ], axis=0) for off in (q_per_kv, q_per_kv + 1)
            ]
            q = jnp.concatenate([out_ref[g, pl.ds(b, q_per_kv, stride=pitch), :] for g in range(groups)], axis=0)
            sc = lax.dot_general(q.astype(BF16), kbuf[b], (((1,), (1,)), ((), ())), preferred_element_type=F32)
            ok = jnp.logical_and(same, colj < groups * rel)
            scores.append(jnp.where(ok, sc * (head ** -0.5), -1e30))
            own = jnp.sum(q * rows[0], axis=1, keepdims=True) * (head ** -0.5)
            at = jnp.full((heads, 1), rel, jnp.int32)
            fresh.append(jnp.where(jnp.logical_and(at >= 0, at < n_grp), own, -1e30))
            vals.append(rows[1])
        sc = jnp.concatenate(scores, axis=0)
        own = jnp.concatenate(fresh, axis=0)
        top = jnp.maximum(jnp.max(sc, axis=1, keepdims=True), own)
        wt = jnp.exp(sc - top)
        own = jnp.exp(own - top)
        tot = jnp.sum(wt, axis=1, keepdims=True) + own
        wt = wt.astype(BF16)
        own = own.astype(BF16).astype(F32)
        for t in range(per):
            cut = slice(t * heads, (t + 1) * heads)
            o_ref[d, cut, :] = jnp.dot(
                wt[cut], vbuf[i * per + t], preferred_element_type=F32) + own[cut] * vals[t]
        top_row = jnp.sum(jnp.where(eye, top, 0.0), axis=0, keepdims=True)
        tot_row = jnp.sum(jnp.where(eye, tot, 0.0), axis=0, keepdims=True)
        pad = jnp.zeros((6, n_rows), F32)
        o_ref[d, n_rows:n_rows + 8, :] = jnp.concatenate([top_row, tot_row, pad], axis=0)

    last = None
    for t, e in enumerate(chips):
        if t >= nx // 2:
            out_load(1)
        attend(CORES * e + 1)
        give(e).start()
        attend(CORES * e)
        if last is not None:
            pair(last)
        last = e
    out_load(1)
    pair(last)
    parts = [mix.at[0]]
    for e in reversed(far_x):
        rs(e).wait_recv()
        parts.append(rbuf.at[e])
    out_load(len(todo))
    _, tot, facs = merge(parts)
    val = weigh(parts, [f / tot for f in facs])
    attn[0] = val

    swap = rcopy(attn.at[0], abuf.at[core], ab_s, ab_r, sp=partner)
    swap.start()
    abuf[core] = val
    swap.wait()
    flat = abuf.reshape(CORES * n_rows, head)
    for n in range(heads):
        lhs[:, n * head:(n + 1) * head] = flat[pl.ds(n, seqs, stride=heads), :].astype(BF16)

    def ysend(d):
        return rcopy(pbuf.at[d], ybuf.at[d], y_s.at[d], y_r.at[d], tp=yat(d))

    def proj(j):
        for part in range(WO_PARTS):
            wcopy(j, part).wait()
        pbuf[j] = jnp.dot(lhs[...], wobuf[j], preferred_element_type=F32)

    for j in order:
        proj(j)
        if j:
            ysend(j).start()
    hcopy.wait()
    tot = pbuf[0]
    for d in range(1, n_tp):
        ysend(d).wait_recv()
        tot = tot + ybuf[d]
    res_ref[ds(x * seqs, seqs, seqs), ds((core * n_tp + y) * cols, cols, cols)] = hbuf[...].astype(F32) + tot

    def block(dy, dx, part):
        by = lax.rem(y + n_tp - dy, n_tp)
        bx = lax.rem(x + nx - dx, nx)
        return res_ref.at[ds(bx * seqs + part * per, per, per), ds((core * n_tp + by) * cols, cols, cols)]

    sends = []

    def go(dy, dx, part, sems, where, ty, tx):
        ref = block(dy, dx, part)
        cp = rcopy(ref, ref, sems[0].at[ty, tx], sems[1].at[ty, tx], **where)
        cp.start()
        sends.append(cp)

    def fwd(dy, dx, part):
        if part == 0 and dx == 0:
            for e in far_x:
                go(dy, 0, 0, (a_s, a_r), {'sp': xat(e)}, dy, e)
        if part == 1 and dy == 0:
            for e in far_tp:
                go(0, dx, 1, (b_s, b_r), {'tp': yat(e)}, e, dx)
        ref = block(dy, dx, part)
        cp = rcopy(ref, ref, d_s.at[part, dy, dx], d_r.at[part, dy, dx], sp=partner)
        cp.start()
        sends.append(cp)

    for e in reversed(far_tp):
        go(0, 0, 0, (a_s, a_r), {'tp': yat(e)}, e, 0)
    for e in reversed(far_x):
        go(0, 0, 1, (b_s, b_r), {'sp': xat(e)}, 0, e)
    fwd(0, 0, 0)
    fwd(0, 0, 1)

    def arrive(dy, dx, part):
        ref = block(dy, dx, part)
        r = (a_r, b_r)[part].at[dy, dx]
        q = (a_s, b_s)[part].at[dy, dx]
        rcopy(ref, ref, q, r, sp=partner).wait_recv()
        fwd(dy, dx, part)

    def hops(item):
        dy, dx, part = item
        first = dx == 0 if part == 0 else dy == 0
        return (not first, min(dy, n_tp - dy) + min(dx, nx - dx), dy + dx)

    due = [(dy, dx, part) for dy in range(n_tp) for dx in range(nx) for part in range(2) if dy + dx > 0]
    for dy, dx, part in sorted(due, key=hops):
        arrive(dy, dx, part)
    for part in range(2):
        for dy in range(n_tp):
            for dx in range(nx):
                by = lax.rem(y + n_tp - dy, n_tp)
                bx = lax.rem(x + nx - dx, nx)
                ref = res_ref.at[ds(bx * seqs + part * per, per, per),
                                 ds(((1 - core) * n_tp + by) * cols, cols, cols)]
                rcopy(ref, ref, d_s.at[part, dy, dx], d_r.at[part, dy, dx], sp=partner).wait_recv()
    for cp in sends:
        cp.wait_send()
    for e in range(1, nx):
        rs(e).wait_send()
    for e in range(nx):
        give(e).wait_send()
    for d in range(1, n_tp):
        ysend(d).wait_send()
    for d in range(nx + n_local):
        psend(d).wait_send()
    for e in range(1, nx):
        rsend(e).wait_send()


def write_kernel(dims, pos_ref, qkv_ref, res_ref, k_ref, v_ref, h_out, ko_ref, vo_ref, kbuf, vbuf, hbuf, osem, hsem):
    q_per_kv, head, pitch, n_ch = dims
    n_seq, rows2, _ = kbuf.shape
    groups = qkv_ref.shape[0]
    n_grp = rows2 // groups
    per = n_seq // n_ch
    base = lax.axis_index('sp') * n_grp
    tile = 8 * groups
    trow = lax.broadcasted_iota(jnp.int32, (tile, head), 0)

    def bulk(i, which):
        src, dst = ((kbuf, ko_ref), (vbuf, vo_ref))[which]
        cut = pl.ds(i * per, per)
        return pltpu.make_async_copy(src.at[cut], dst.at[cut], osem.at[which, i])

    def hwrite(i):
        cut = pl.ds(i * 16, 16)
        return pltpu.make_async_copy(hbuf.at[cut], h_out.at[cut], hsem.at[i])

    def step(i, carry):
        for t in range(per):
            b = i * per + t
            rel = pos_ref[b] - base
            here = jnp.logical_and(rel >= 0, rel < n_grp)
            at = jnp.clip(rel, 0, n_grp - 1)
            cut = ds((at // 8) * tile, tile, tile)
            hit = jnp.logical_and(trow // groups == at % 8, here)
            for src, buf, off in ((k_ref, kbuf, q_per_kv * pitch), (v_ref, vbuf, (q_per_kv + 1) * pitch)):
                new = qkv_ref[0, pl.ds(off + b, 1), :]
                for g in range(1, groups):
                    new = jnp.where(trow % groups == g, qkv_ref[g, pl.ds(off + b, 1), :], new)
                buf[b, cut, :] = jnp.where(hit, new, src[b, cut, :].astype(F32)).astype(BF16)

        @pl.when(i > 0)
        def _():
            bulk(i - 1, 0).start()
            bulk(i - 1, 1).start()

        return carry

    lax.fori_loop(0, n_ch, step, 0)
    bulk(n_ch - 1, 0).start()
    bulk(n_ch - 1, 1).start()
    n_h = n_seq // 16
    for i in range(n_h):
        hbuf[i * 16:(i + 1) * 16, :] = res_ref[i * 16:(i + 1) * 16, :].astype(BF16)
        if i > 0:
            hwrite(i - 1).start()
    hwrite(n_h - 1).start()
    for i in range(n_ch):
        bulk(i, 0).wait()
        bulk(i, 1).wait()
    for i in range(n_h):
        hwrite(i).wait()


def solution(mesh):
    n_tp, n_sp = mesh.shape['tp'], mesh.shape['sp']
    cache_spec = P('dp', 'sp', 'tp', None)
    DMA = pltpu.SemaphoreType.DMA

    def local_step(hidden, norm_scale, w_qkv, w_out, k_cache, v_cache, positions):
        n_seq, seq_local, kv_local, head = k_cache.shape
        d_model = hidden.shape[1]
        q_per_kv = w_qkv.shape[1] // (kv_local * head) - 2
        heads = kv_local * q_per_kv
        grp_cols = (q_per_kv + 2) * head
        n_blk, n_rblk = 16, 2
        ring_cols = RING_HEADS * head
        local_cols = grp_cols - (n_sp // CORES) * ring_cols
        pitch = n_seq + 8
        per = n_seq // n_sp
        n_rows = per * heads
        flat = (n_seq, seq_local * kv_local, head)
        vmem_cache = pltpu.VMEM(flat, BF16)
        hbm_cache = jax.ShapeDtypeStruct(flat, BF16)

        nx = n_sp // CORES
        cols = d_model // (CORES * n_tp)
        depth = w_out.shape[0]
        qkv, k_now, v_now, res = pl.pallas_call(
            functools.partial(main_kernel, (q_per_kv, head, pitch, n_tp, n_sp)),
            out_shape=(pltpu.VMEM((kv_local, pitch * (q_per_kv + 2), head), F32), vmem_cache, vmem_cache,
                       pltpu.VMEM((n_seq, d_model), F32)),
            in_specs=[HBM] * 8,
            out_specs=(VMEM,) * 4,
            scratch_shapes=[
                pltpu.VMEM(hidden.shape, BF16),
                pltpu.VMEM((d_model // 128, 128), BF16),
                pltpu.VMEM((1, n_seq), jnp.int32),
                pltpu.VMEM((n_blk, d_model // n_blk, local_cols), BF16),
                pltpu.VMEM((n_seq, d_model), BF16),
                pltpu.VMEM((n_seq, local_cols), F32),
                pltpu.VMEM((d_model // 128, 128), F32),
                pltpu.VMEM((n_rblk, d_model // n_rblk, ring_cols), BF16),
                pltpu.VMEM((n_sp, n_rows + 8, head), F32),
                pltpu.VMEM((nx, n_rows + 8, head), F32),
                pltpu.VMEM((nx, n_rows + 8, head), F32),
                pltpu.VMEM((nx, n_rows + 8, head), F32),
                pltpu.VMEM((CORES, n_rows, head), F32),
                pltpu.VMEM((1, n_rows, head), F32),
                pltpu.VMEM((CORES * per, depth), BF16),
                pltpu.VMEM((n_tp, depth, cols), BF16),
                pltpu.VMEM((n_tp, CORES * per, cols), F32),
                pltpu.VMEM((n_tp, CORES * per, cols), F32),
                pltpu.VMEM((CORES * per, cols), BF16),
                DMA((H_PARTS + 3,)), DMA((n_blk,)), DMA((2, n_sp)), DMA((q_per_kv + 2,)), DMA((q_per_kv + 2,)),
                DMA((n_tp, WO_PARTS)), DMA,
                DMA((nx,)), DMA((nx,)), DMA((nx,)), DMA((nx,)), DMA, DMA, DMA((n_tp,)), DMA((n_tp,)),
                DMA((n_tp, nx)), DMA((n_tp, nx)), DMA((n_tp, nx)), DMA((n_tp, nx)),
                DMA((2, n_tp, nx)), DMA((2, n_tp, nx)),
                pltpu.SMEM((n_seq,), jnp.int32),
                DMA((n_rblk,)), DMA((nx,)), DMA((nx,)),
            ],
            compiler_params=pltpu.CompilerParams(
                collective_id=0, has_side_effects=True, vmem_limit_bytes=46 * MIB),
            name='main',
        )(in_hbm(positions), in_hbm(hidden), in_hbm(norm_scale.reshape(d_model // 128, 128)),
          in_hbm(positions.reshape(1, n_seq)), in_hbm(w_qkv), in_hbm(k_cache.reshape(flat)),
          in_hbm(v_cache.reshape(flat)), in_hbm(w_out))

        h_out, k_out, v_out, _, _ = pl.pallas_call(
            functools.partial(write_kernel, (q_per_kv, head, pitch, n_sp)),
            out_shape=(jax.ShapeDtypeStruct(hidden.shape, BF16), hbm_cache, hbm_cache, vmem_cache, vmem_cache),
            in_specs=[SMEM, VMEM, VMEM, VMEM, VMEM],
            out_specs=(HBM, HBM, HBM, VMEM, VMEM),
            input_output_aliases={3: 3, 4: 4},
            scratch_shapes=[pltpu.VMEM(hidden.shape, BF16), DMA((2, n_sp)), DMA((n_seq // 16,))],
            compiler_params=pltpu.CompilerParams(vmem_limit_bytes=4 * MIB),
            name='write',
        )(positions, qkv, res, k_now, v_now)
        return h_out, k_out.reshape(k_cache.shape), v_out.reshape(v_cache.shape)

    return jax.shard_map(
        local_step,
        mesh=mesh,
        in_specs=(P('dp', None), P(None), P(None, 'tp'), P('tp', None), cache_spec, cache_spec, P('dp')),
        out_specs=(P('dp', None), cache_spec, cache_spec),
        check_vma=False,
    )
```
